32 devices in a mesh: dp: 2 (over x), row: 4 (over z), col: 4 (over y, core).
Axes of the slice: x: 2, y: 2, z: 4, core: 2. Of those that a mesh axis runs over, the one named last changes fastest.
Arguments:
- layer_input: bfloat16 [2048, 2048], P(('dp', 'col'), 'row'), may hold values from -6 to 6
- cotangent: bfloat16 [2048, 2048], P(('dp', 'col'), 'row'), may hold values from -6 to 6
- w_query: bfloat16 [2048, 2048], P('row', 'col'), may hold values from -0.125 to 0.125
- key_matrix: bfloat16 [2048, 1024], P('row', 'col'), may hold values from -0.125 to 0.125
- value_matrix: bfloat16 [2048, 1024], P('row', 'col'), may hold values from -0.125 to 0.125
- w_output: bfloat16 [2048, 2048], P('col', 'row'), may hold values from -1 to 1
- w_gate: bfloat16 [2048, 6144], P('row', 'col'), may hold values from -0.125 to 0.125
- w_up: bfloat16 [2048, 6144], P('row', 'col'), may hold values from -0.125 to 0.125
- w_down: bfloat16 [6144, 2048], P('col', 'row'), may hold values from -0.078125 to 0.078125
- attn_gain: float32 [2048], P('row'), may hold values from 0.5 to 1.5
- mlp_gain: float32 [2048], P('row'), may hold values from 0.5 to 1.5
- query_gain: float32 [128], replicated, may hold values from 0.5 to 1.5
- key_gain: float32 [128], replicated, may hold values from 0.5 to 1.5
- segment_ids: int32 [8, 256], P(('dp', 'row')), may hold values from 0 to 3, never falling along the last dimension, each value on 1 to 128 neighbouring positions
Outputs:
- block_out: bfloat16 [2048, 2048], P(('dp', 'col'), 'row')
- input_grad: float32 [2048, 2048], P(('dp', 'col'), 'row')
- grad_query: float32 [2048, 2048], P('row', 'col')
- grad_key: float32 [2048, 1024], P('row', 'col')
- grad_value: float32 [2048, 1024], P('row', 'col')
- grad_output: float32 [2048, 2048], P('col', 'row')
- grad_gate: float32 [2048, 6144], P('row', 'col')
- grad_up: float32 [2048, 6144], P('row', 'col')
- grad_down: float32 [6144, 2048], P('col', 'row')
- gain_attn: float32 [2048], replicated
- gain_mlp: float32 [2048], replicated
- gain_query: float32 [128], replicated
- gain_key: float32 [128], replicated
The draws below stay inside these ranges and needn't reach their ends.
All inputs are finite; a program needn't handle non-finite values.
Results may differ from the reference program's by a relative error of at most 0.015.
Values may be sent and summed in bfloat16 or wider, within the bound.
A program may use at most 128 MiB of HBM per device.

```python
import math
import jax
import jax.numpy as jnp
import numpy as np
from jax import lax

MODEL_WIDTH = 2048
QUERY_HEADS = 16
KEY_VALUE_HEADS = 8
HEAD_SIZE = 128
FEEDFWD_UNITS = 6144
PACKED_LENGTH = 256
TOKENS = 2048
SEQS = 8


def level_of(stream_key, extent, pieces, least, top_value):
    def one(axis_at, parts):
        steps = jax.random.uniform(jax.random.fold_in(jax.random.fold_in(stream_key, 6), axis_at), (parts,), jnp.float32, least / len(pieces), top_value / len(pieces))
        return jnp.repeat(jnp.exp(steps), extent[axis_at] // parts).reshape((-1,) + (1,) * (len(extent) - axis_at - 1))

    factor_of = one(*pieces[0])
    for cut in pieces[1:]:
        factor_of = factor_of * one(*cut)
    return factor_of


def length_profile(amount, total, most, skew):
    portions = [(1 << 20) // math.isqrt(standing ** skew) + 1 for standing in range(2, amount + 1)]
    spare, counts = total - most - (amount - 1), [1] * (amount - 1)
    while spare > 0:
        movable = [i for i in range(amount - 1) if counts[i] < most]
        pool, left = sum([portions[i] for i in movable]), spare
        for i in movable:
            more = min(most - counts[i], max(1, left * portions[i] // pool), spare)
            counts[i] = counts[i] + more
            spare = spare - more
    return np.array([most] + counts)


def ragged_sizes(own_key, amount, total, bound, lean):
    if amount == 2:
        one = jax.random.randint(own_key, (), max(1, total - bound), min(bound, total - 1) + 1)
        return jnp.stack([one, total - one])
    sizes = jnp.asarray(length_profile(amount, total, bound, lean), jnp.int32)
    twos = (amount - 1) // 2
    source_of, sink = sizes[1:1 + 2 * twos:2], sizes[2:2 + 2 * twos:2]
    slack = jnp.minimum(source_of - 1, bound - sink)
    moved = jax.random.randint(jax.random.fold_in(own_key, 1), (twos,), 0, 1 << 20) % (slack + 1)
    sizes = sizes.at[1:1 + 2 * twos:2].set(source_of - moved).at[2:2 + 2 * twos:2].set(sink + moved)
    return sizes[jax.random.permutation(jax.random.fold_in(own_key, 2), amount)]


def noise(stream_key, shape, deviation, limit, cuts=(), held_as=jnp.bfloat16):
    array = deviation * jax.random.normal(stream_key, shape, jnp.float32)
    if cuts:
        array = array * level_of(stream_key, shape, cuts, -0.22, 0.18)
    return jnp.clip(array, -limit, limit).astype(held_as)


def setup_inputs(seed: int = 0) -> dict:
    key_list = jax.random.split(jax.random.key(seed), 15)
    layer_input = noise(key_list[0], (TOKENS, MODEL_WIDTH), 1.0, 6.0, ((0, 8), (1, 4)))
    cotangent = noise(key_list[1], (TOKENS, MODEL_WIDTH), 1.0, 6.0, ((0, 8), (1, 4)))
    w_query = noise(key_list[2], (MODEL_WIDTH, QUERY_HEADS * HEAD_SIZE), MODEL_WIDTH ** -0.5, 0.125, ((0, 4), (1, 4)))
    key_matrix = noise(key_list[3], (MODEL_WIDTH, KEY_VALUE_HEADS * HEAD_SIZE), MODEL_WIDTH ** -0.5, 0.125, ((0, 4), (1, 4)))
    value_matrix = noise(key_list[4], (MODEL_WIDTH, KEY_VALUE_HEADS * HEAD_SIZE), MODEL_WIDTH ** -0.5, 0.125, ((0, 4), (1, 4)))
    w_output = noise(key_list[5], (QUERY_HEADS * HEAD_SIZE, MODEL_WIDTH), (QUERY_HEADS * HEAD_SIZE // 64) ** -0.5, 1.0, ((0, 4), (1, 4)))
    w_gate = noise(key_list[6], (MODEL_WIDTH, FEEDFWD_UNITS), MODEL_WIDTH ** -0.5, 0.125, ((0, 4), (1, 4)))
    w_up = noise(key_list[7], (MODEL_WIDTH, FEEDFWD_UNITS), MODEL_WIDTH ** -0.5, 0.125, ((0, 4), (1, 4)))
    w_down = noise(key_list[8], (FEEDFWD_UNITS, MODEL_WIDTH), FEEDFWD_UNITS ** -0.5, 0.078125, ((0, 4), (1, 4)))
    attn_gain = jnp.clip(1.0 + 0.1 * jax.random.normal(key_list[9], (MODEL_WIDTH,), jnp.float32), 0.5, 1.5)
    mlp_gain = jnp.clip(1.0 + 0.1 * jax.random.normal(key_list[10], (MODEL_WIDTH,), jnp.float32), 0.5, 1.5)
    query_gain = jnp.clip(1.0 + 0.1 * jax.random.normal(key_list[11], (HEAD_SIZE,), jnp.float32), 0.5, 1.5)
    key_gain = jnp.clip(1.0 + 0.1 * jax.random.normal(key_list[12], (HEAD_SIZE,), jnp.float32), 0.5, 1.5)
    segment_ids = jax.vmap(lambda own: jnp.searchsorted(jnp.cumsum(ragged_sizes(own, 4, PACKED_LENGTH, PACKED_LENGTH // 2, 0)), jnp.arange(PACKED_LENGTH), side="right"))(jax.random.split(key_list[13], SEQS)).reshape((SEQS, PACKED_LENGTH)).astype(jnp.int32)
    return {"layer_input": layer_input, "cotangent": cotangent, "w_query": w_query, "key_matrix": key_matrix, "value_matrix": value_matrix, "w_output": w_output, "w_gate": w_gate, "w_up": w_up, "w_down": w_down, "attn_gain": attn_gain, "mlp_gain": mlp_gain, "query_gain": query_gain, "key_gain": key_gain, "segment_ids": segment_ids}


EPSILON = 1e-06
THETA = 1000000.0

def positions_of(segment):
    length = segment.shape[0]
    index = jnp.arange(length, dtype=jnp.int32)
    change = jnp.concatenate([jnp.ones((1,), jnp.int32), (segment[1:] != segment[:-1]).astype(jnp.int32)])
    starts = lax.cummax(jnp.where(change > 0, index, jnp.zeros_like(index)), axis=0)
    return index - starts

def rope_tables(segment, width):
    half = width // 2
    inverse = jnp.power(THETA, -(jnp.arange(half, dtype=jnp.float32) * (2.0 / width)))
    angle = positions_of(segment).astype(jnp.float32)[:, None] * inverse[None, :]
    return (jnp.cos(angle), jnp.sin(angle))

def rotate(field, cosine, sine):
    half = field.shape[-1] // 2
    first = field[..., :half]
    second = field[..., half:]
    cos_b = cosine[:, None, :]
    sin_b = sine[:, None, :]
    return jnp.concatenate([first * cos_b - second * sin_b, second * cos_b + first * sin_b], axis=-1)

def unrotate(grad, cosine, sine):
    half = grad.shape[-1] // 2
    first = grad[..., :half]
    second = grad[..., half:]
    cos_b = cosine[:, None, :]
    sin_b = sine[:, None, :]
    return jnp.concatenate([first * cos_b + second * sin_b, second * cos_b - first * sin_b], axis=-1)

def head_norm(field, gain):
    scale = lax.rsqrt(lax.optimization_barrier(jnp.mean(field * field, axis=-1, keepdims=True)) + EPSILON)
    unit = field * scale
    return (unit * gain, unit, scale)

def head_norm_back(grad, unit, scale, gain):
    inner = grad * gain
    back = scale * (inner - unit * lax.optimization_barrier(jnp.mean(inner * unit, axis=-1, keepdims=True)))
    return (back, lax.optimization_barrier(jnp.sum(grad * unit, axis=(0, 1))))

def mix(form, left, right):
    return jnp.einsum(form, left.astype(jnp.float32), right.astype(jnp.float32))

def score_mask(segment, start, block):
    length = segment.shape[0]
    query_index = start + jnp.arange(block, dtype=jnp.int32)
    key_index = jnp.arange(length, dtype=jnp.int32)
    query_seg = lax.dynamic_slice_in_dim(segment, start, block, 0)
    return (query_seg[:, None] == segment[None, :]) & (key_index[None, :] <= query_index[:, None])

def attend(query, key_rows, value_rows, segment):
    length, heads, width = query.shape
    groups = key_rows.shape[1]
    group_factor = heads // groups
    block = min(512, length)
    blocks = length // block
    scale = width ** (-0.5)
    grouped = query.reshape(blocks, block, groups, group_factor, width)
    starts = jnp.arange(blocks, dtype=jnp.int32) * block

    def one_block(item):
        query_block, start = item
        scores = mix('qgrd,kgd->grqk', query_block, key_rows) * scale
        allowed = score_mask(segment, start, block)
        scores = jnp.where(allowed[None, None], scores, -1e+30)
        top = lax.optimization_barrier(jnp.max(scores, axis=-1, keepdims=True))
        weights = jnp.exp(scores - top)
        total = lax.optimization_barrier(jnp.sum(weights, axis=-1, keepdims=True))
        probs = (weights / total).astype(jnp.bfloat16)
        result = mix('grqk,kgd->qgrd', probs, value_rows)
        return (result.astype(jnp.bfloat16), (top + jnp.log(total))[..., 0])
    results, log_total = lax.map(one_block, (grouped, starts))
    return (results.reshape(length, heads * width), log_total)

def attend_back(query, key_rows, value_rows, segment, mixed, grad_mixed, log_total):
    length, heads, width = query.shape
    groups = key_rows.shape[1]
    group_factor = heads // groups
    block = min(512, length)
    blocks = length // block
    scale = width ** (-0.5)
    delta = lax.optimization_barrier(jnp.sum(grad_mixed.astype(jnp.float32).reshape(length, heads, width) * mixed.astype(jnp.float32).reshape(length, heads, width), axis=-1))
    delta = jnp.transpose(delta.reshape(blocks, block, groups, group_factor), (0, 2, 3, 1))
    grouped = query.reshape(blocks, block, groups, group_factor, width)
    grouped_grad = grad_mixed.reshape(blocks, block, groups, group_factor, width)
    starts = jnp.arange(blocks, dtype=jnp.int32) * block

    def one_block(carry, item):
        grad_keys, value_gradients = carry
        query_block, grad_block, total_block, delta_block, start = item
        scores = mix('qgrd,kgd->grqk', query_block, key_rows) * scale
        allowed = score_mask(segment, start, block)
        scores = jnp.where(allowed[None, None], scores, -1e+30)
        probs = jnp.exp(scores - total_block[..., None])
        value_gradients = value_gradients + mix('grqk,qgrd->kgd', probs.astype(jnp.bfloat16), grad_block)
        grad_probs = mix('qgrd,kgd->grqk', grad_block, value_rows)
        grad_scores = (probs * (grad_probs - delta_block[..., None])).astype(jnp.bfloat16)
        grad_query = mix('grqk,kgd->qgrd', grad_scores, key_rows) * scale
        grad_keys = grad_keys + mix('grqk,qgrd->kgd', grad_scores, query_block) * scale
        return ((grad_keys, value_gradients), grad_query)
    empty = jnp.zeros((length, groups, width), jnp.float32)
    (grad_keys, value_gradients), grad_query = lax.scan(one_block, (empty, empty), (grouped, grouped_grad, log_total, delta, starts))
    return (grad_query.reshape(length, heads, width), grad_keys, value_gradients)

def silu_parts(gate):
    sigma = jax.nn.sigmoid(gate)
    return (gate * sigma, sigma * (1.0 + gate * (1.0 - sigma)))

def matrix_result(left, right):
    return jnp.dot(left, right, preferred_element_type=jnp.float32)

def product_flip(left, right):
    return lax.dot_general(left, right, (((1,), (1,)), ((), ())), preferred_element_type=jnp.float32)

def weight_term(left, right):
    return lax.dot_general(left, right, (((0,), (0,)), ((), ())), preferred_element_type=jnp.float32)

def reference(layer_input, cotangent, w_query, key_matrix, value_matrix, w_output, w_gate, w_up, w_down, attn_gain, mlp_gain, query_gain, key_gain, segment_ids):
    inputs_all = layer_input.reshape(SEQS, PACKED_LENGTH, MODEL_WIDTH)
    cotan_all = cotangent.reshape(SEQS, PACKED_LENGTH, MODEL_WIDTH)

    def one_sequence(totals, item):
        tokens, cotan, segment = item
        cosine, sine = rope_tables(segment, HEAD_SIZE)
        inputs = tokens.astype(jnp.float32)
        scale_in = lax.rsqrt(lax.optimization_barrier(jnp.mean(inputs * inputs, axis=-1, keepdims=True)) + EPSILON)
        unit_in = inputs * scale_in
        normalized_input = (unit_in * attn_gain).astype(jnp.bfloat16)
        query = matrix_result(normalized_input, w_query).reshape(PACKED_LENGTH, QUERY_HEADS, HEAD_SIZE)
        key_rows = matrix_result(normalized_input, key_matrix).reshape(PACKED_LENGTH, KEY_VALUE_HEADS, HEAD_SIZE)
        value_rows = matrix_result(normalized_input, value_matrix).astype(jnp.bfloat16).reshape(PACKED_LENGTH, KEY_VALUE_HEADS, HEAD_SIZE)
        query_norm, query_unit, query_scale = head_norm(query, query_gain)
        key_norm, key_unit, key_scale = head_norm(key_rows, key_gain)
        query_rot = rotate(query_norm, cosine, sine).astype(jnp.bfloat16)
        key_rot = rotate(key_norm, cosine, sine).astype(jnp.bfloat16)
        mixed, log_total = attend(query_rot, key_rot, value_rows, segment)
        hidden = inputs + matrix_result(mixed, w_output)
        scale_mid = lax.rsqrt(lax.optimization_barrier(jnp.mean(hidden * hidden, axis=-1, keepdims=True)) + EPSILON)
        unit_mid = hidden * scale_mid
        normed_mid = (unit_mid * mlp_gain).astype(jnp.bfloat16)
        gate = matrix_result(normed_mid, w_gate)
        upward = matrix_result(normed_mid, w_up)
        silu, slope = silu_parts(gate)
        active = (silu * upward).astype(jnp.bfloat16)
        block_out = (hidden + matrix_result(active, w_down)).astype(jnp.bfloat16)
        grad_active = product_flip(cotan, w_down)
        grad_down = weight_term(active, cotan)
        grad_gate_in = (grad_active * upward * slope).astype(jnp.bfloat16)
        grad_up_in = (grad_active * silu).astype(jnp.bfloat16)
        grad_mid = product_flip(grad_gate_in, w_gate) + product_flip(grad_up_in, w_up)
        grad_gate = weight_term(normed_mid, grad_gate_in)
        grad_up = weight_term(normed_mid, grad_up_in)
        inner_mid = grad_mid * mlp_gain
        gain_mlp = lax.optimization_barrier(jnp.sum(grad_mid * unit_mid, axis=0))
        grad_hidden = cotan.astype(jnp.float32) + scale_mid * (inner_mid - unit_mid * lax.optimization_barrier(jnp.mean(inner_mid * unit_mid, axis=-1, keepdims=True)))
        grad_attn = grad_hidden.astype(jnp.bfloat16)
        grad_mixed = product_flip(grad_attn, w_output).astype(jnp.bfloat16)
        grad_output = weight_term(mixed, grad_attn)
        grad_query_rot, grad_key_rot, value_gradients = attend_back(query_rot, key_rot, value_rows, segment, mixed, grad_mixed, log_total)
        grad_query_raw, gain_query = head_norm_back(unrotate(grad_query_rot, cosine, sine), query_unit, query_scale, query_gain)
        unrotated_key_gradient, gain_key = head_norm_back(unrotate(grad_key_rot, cosine, sine), key_unit, key_scale, key_gain)
        grad_query_b = grad_query_raw.reshape(PACKED_LENGTH, QUERY_HEADS * HEAD_SIZE).astype(jnp.bfloat16)
        key_gradient_copy = unrotated_key_gradient.reshape(PACKED_LENGTH, KEY_VALUE_HEADS * HEAD_SIZE).astype(jnp.bfloat16)
        value_gradient_copy = value_gradients.reshape(PACKED_LENGTH, KEY_VALUE_HEADS * HEAD_SIZE).astype(jnp.bfloat16)
        grad_in_norm = product_flip(grad_query_b, w_query) + product_flip(key_gradient_copy, key_matrix) + product_flip(value_gradient_copy, value_matrix)
        grad_query = weight_term(normalized_input, grad_query_b)
        grad_key = weight_term(normalized_input, key_gradient_copy)
        grad_value = weight_term(normalized_input, value_gradient_copy)
        inner_in = grad_in_norm * attn_gain
        gain_attn = lax.optimization_barrier(jnp.sum(grad_in_norm * unit_in, axis=0))
        input_grad = grad_hidden + scale_in * (inner_in - unit_in * lax.optimization_barrier(jnp.mean(inner_in * unit_in, axis=-1, keepdims=True)))
        terms = (grad_query, grad_key, grad_value, grad_output, grad_gate, grad_up, grad_down, gain_attn, gain_mlp, gain_query, gain_key)
        totals = tuple((total + term for total, term in zip(totals, terms)))
        return (totals, (block_out, input_grad))
    zero_filled = (jnp.zeros((MODEL_WIDTH, QUERY_HEADS * HEAD_SIZE), jnp.float32), jnp.zeros((MODEL_WIDTH, KEY_VALUE_HEADS * HEAD_SIZE), jnp.float32), jnp.zeros((MODEL_WIDTH, KEY_VALUE_HEADS * HEAD_SIZE), jnp.float32), jnp.zeros((QUERY_HEADS * HEAD_SIZE, MODEL_WIDTH), jnp.float32), jnp.zeros((MODEL_WIDTH, FEEDFWD_UNITS), jnp.float32), jnp.zeros((MODEL_WIDTH, FEEDFWD_UNITS), jnp.float32), jnp.zeros((FEEDFWD_UNITS, MODEL_WIDTH), jnp.float32), jnp.zeros((MODEL_WIDTH,), jnp.float32), jnp.zeros((MODEL_WIDTH,), jnp.float32), jnp.zeros((HEAD_SIZE,), jnp.float32), jnp.zeros((HEAD_SIZE,), jnp.float32))
    totals, (outputs, grads_in) = lax.scan(one_sequence, zero_filled, (inputs_all, cotan_all, segment_ids))
    return (outputs.reshape(SEQS * PACKED_LENGTH, MODEL_WIDTH), grads_in.reshape(SEQS * PACKED_LENGTH, MODEL_WIDTH), totals[0], totals[1], totals[2], totals[3], totals[4], totals[5], totals[6], totals[7], totals[8], totals[9], totals[10])
```

```python
import functools

import jax
import jax.numpy as jnp
from jax import lax
from jax.experimental import pallas as pl
from jax.experimental.pallas import tpu as pltpu
from jax.sharding import PartitionSpec as P

MODEL_WIDTH = 2048
HEAD_SIZE = 128
EPSILON = 1e-06
THETA = 1000000.0
ROWS = 4
COLS = 4
MESH = pl.DeviceIdType.MESH
VMEM = pltpu.VMEM
DMA = pltpu.SemaphoreType.DMA
BF16 = jnp.bfloat16
F32 = jnp.float32


def remote(src, dst, send, recv, device):
    return pltpu.make_async_remote_copy(
        src_ref=src,
        dst_ref=dst,
        send_sem=send,
        recv_sem=recv,
        device_id=device,
        device_id_type=MESH,
    )


class Here:
    def __init__(self):
        self.dp = lax.axis_index("dp")
        self.z = lax.axis_index("row")
        self.c = lax.axis_index("col")
        self.core = self.c % 2
        self.c_core = self.c + 1 - 2 * self.core
        self.c_y = (self.c + 2) % COLS
        self.up = (self.dp, self.z + 1, self.c)
        self.down = (self.dp, self.z - 1, self.c)
        self.over_y = (self.dp, self.z, self.c_y)
        self.over_core = (self.dp, self.z, self.c_core)

    def peers(self):
        for dz in range(ROWS):
            for dc in range(COLS):
                if dz or dc:
                    z, c = (self.z + dz) % ROWS, (self.c + dc) % COLS
                    yield dz * COLS + dc, z, c


def meet(here, use_z, use_c, everyone):
    barrier = pltpu.get_barrier_semaphore()

    def signal(device):
        pl.semaphore_signal(barrier, inc=1, device_id=device, device_id_type=MESH)

    if everyone:
        for _, z, c in here.peers():
            signal((here.dp, z, c))
        pl.semaphore_wait(barrier, ROWS * COLS - 1)
        return
    count = 0
    if use_c:
        signal(here.over_y)
        signal(here.over_core)
        count = 2
    if use_z:
        pl.when(here.z < ROWS - 1)(lambda: signal(here.up))
        pl.when(here.z > 0)(lambda: signal(here.down))
        inner = (here.z % 3 + 2) // 3
        pl.semaphore_wait(barrier, count + 1 + inner)
    else:
        pl.semaphore_wait(barrier, count)


def gather_kernel(use_z, use_c, place, with_stat, *refs):
    here = Here()
    z, c = here.z, here.c
    if with_stat:
        x_ref, st_ref, o_ref, so_ref, *sems = refs
        s_send, s_recv = sems[-2:]
    else:
        x_ref, o_ref, *sems = refs
    up_send, down_send, z_recv, y_send, y_recv, c_send, c_recv = sems[:7]
    meet(here, use_z, use_c, with_stat)

    def slot(zz, cc):
        return o_ref.at[place(zz, cc)]

    def to_up(src, zz, d):
        return remote(src, slot(zz, c), up_send.at[d], z_recv.at[zz], here.up)

    def to_down(src, zz, d):
        return remote(src, slot(zz, c), down_send.at[d], z_recv.at[zz], here.down)

    def to_y(src, zz):
        return remote(src, slot(zz, c), y_send.at[zz], y_recv.at[zz], here.over_y)

    def to_core(src, zz, cc, half):
        k = half * ROWS + zz
        return remote(src, slot(zz, cc), c_send.at[k], c_recv.at[k], here.over_core)

    def arrived(zz, cc, sem):
        remote(slot(zz, cc), slot(zz, cc), y_send.at[0], sem, here.over_y).wait_recv()

    pending = []

    def send(cond, make):
        if cond is None:
            make().start()
        else:
            pl.when(cond)(lambda: make().start())
        pending.append((cond, make))

    top = z < ROWS - 1
    low = z > 0
    if use_z:
        send(top, lambda: to_up(x_ref, z, 0))
        send(low, lambda: to_down(x_ref, z, 0))
    if use_c:
        send(None, lambda: to_y(x_ref, z))
        send(None, lambda: to_core(x_ref, z, c, 0))
    if with_stat:
        me = z * COLS + c
        for k, zz, cc in here.peers():
            remote(
                st_ref, so_ref.at[me], s_send.at[k], s_recv.at[me], (here.dp, zz, cc)
            ).start()
        so_ref[me] = st_ref[...]
    o_ref[place(z, c)] = x_ref[...]

    def from_y(zz):
        arrived(zz, here.c_y, y_recv.at[zz])
        send_now = to_core(slot(zz, here.c_y), zz, here.c_y, 1)
        send_now.start()

    if use_z:
        for d in range(1, ROWS):
            below, above = z - d, z + d
            has_below, has_above = below >= 0, above < ROWS

            def step_below(below=below, d=d):
                arrived(below, c, z_recv.at[below])
                pl.when(top)(lambda: to_up(slot(below, c), below, d).start())
                if use_c:
                    to_y(slot(below, c), below).start()
                    to_core(slot(below, c), below, c, 0).start()

            def step_above(above=above, d=d):
                arrived(above, c, z_recv.at[above])
                pl.when(low)(lambda: to_down(slot(above, c), above, d).start())
                if use_c:
                    to_y(slot(above, c), above).start()
                    to_core(slot(above, c), above, c, 0).start()

            pl.when(has_below)(step_below)
            pl.when(has_above)(step_above)
            if use_c:
                if d == 1:
                    from_y(z)
                else:
                    pl.when(z - (d - 1) >= 0)(lambda d=d: from_y(z - (d - 1)))
                    pl.when(z + (d - 1) < ROWS)(lambda d=d: from_y(z + (d - 1)))
        if use_c:
            d = ROWS
            pl.when(z - (d - 1) >= 0)(lambda: from_y(z - (ROWS - 1)))
            pl.when(z + (d - 1) < ROWS)(lambda: from_y(z + (ROWS - 1)))
    else:
        from_y(z)

    for cond, make in pending:
        if cond is None:
            make().wait_send()
        else:
            pl.when(cond)(lambda make=make: make().wait_send())
    if use_z:
        for d in range(1, ROWS):
            below, above = z - d, z + d
            pl.when((below >= 0) & top)(
                lambda below=below, d=d: to_up(slot(below, c), below, d).wait_send()
            )
            pl.when((above < ROWS) & low)(
                lambda above=above, d=d: to_down(slot(above, c), above, d).wait_send()
            )
    if use_c:
        steps = ROWS if use_z else 1
        for d in range(steps):
            zz = (z + d) % ROWS
            if d:
                to_y(slot(zz, c), zz).wait_send()
                to_core(slot(zz, c), zz, c, 0).wait_send()
            to_core(slot(zz, here.c_y), zz, here.c_y, 1).wait_send()
            arrived(zz, here.c_core, c_recv.at[zz])
            arrived(zz, (here.c_core + 2) % COLS, c_recv.at[ROWS + zz])
    if with_stat:
        for k, zz, cc in here.peers():
            source = zz * COLS + cc
            copy = remote(
                st_ref, so_ref.at[source], s_send.at[k], s_recv.at[source], (here.dp, zz, cc)
            )
            copy.wait_send()
            copy.wait_recv()


def tokens_by_row(n):
    return lambda zz, cc: (pl.ds(pl.multiple_of(zz * n, n), n), slice(None))


def tokens_by_col(n):
    return lambda zz, cc: (pl.ds(pl.multiple_of(cc * n, n), n), slice(None))


def whole_plane(n, w):
    return lambda zz, cc: (
        pl.ds(pl.multiple_of(cc * n, n), n),
        pl.ds(pl.multiple_of(zz * w, w), w),
    )


def vm(n):
    return [pl.BlockSpec(memory_space=VMEM)] * n


def gather(x, use_z, use_c, call, stat=None):
    n, w = x.shape
    if use_z and use_c:
        place, shape = whole_plane(n, w), (n * COLS, w * ROWS)
    elif use_z:
        place, shape = tokens_by_row(n), (n * ROWS, w)
    else:
        place, shape = tokens_by_col(n), (n * COLS, w)
    outs = [jax.ShapeDtypeStruct(shape, x.dtype)]
    scratch = [DMA((ROWS,))] * 5 + [DMA((2 * ROWS,))] * 2
    args = [x]
    if stat is not None:
        outs.append(jax.ShapeDtypeStruct((ROWS * COLS,) + stat.shape, stat.dtype))
        scratch += [DMA((ROWS * COLS,))] * 2
        args.append(stat)
    result = pl.pallas_call(
        functools.partial(gather_kernel, use_z, use_c, place, stat is not None),
        out_shape=outs,
        in_specs=vm(len(args)),
        out_specs=vm(len(outs)),
        scratch_shapes=scratch,
        compiler_params=pltpu.CompilerParams(collective_id=call, has_side_effects=True),
        name=f"gather_{call}",
    )(*args)
    return result if stat is not None else result[0]


def scatter_kernel(use_z, use_c, place, stat_to, n_stat, *refs):
    here = Here()
    z, c = here.z, here.c
    blocks = ROWS if use_z else 1
    p_ref, *refs = refs
    if n_stat:
        st_ref, o_ref, so_ref, *refs = refs
        s_send, s_recv = refs[-2:]
        refs = refs[:-2]
    else:
        o_ref, *refs = refs
    if use_c:
        c_buf, t_buf, y_buf, c_send, c_recv, y_send, y_recv, *refs = refs
    if use_z:
        z_out, z_in_up, z_in_down, z_send, up_recv, down_recv = refs
    meet(here, use_z, use_c, n_stat > 0)

    mirrored = z // 2
    inner = (z % 3 + 2) // 3

    def order(i):
        ends, middle = (3, 2, 1, 0)[i], (3, 0, 2, 1)[i]
        g = ends + inner * (middle - ends)
        return g + mirrored * (3 - 2 * g)

    def dest(i):
        return order(i) if use_z else z

    def load(ref):
        return ref[...].astype(F32)

    def core_copy(j, i):
        other = here.c_core
        cc = (other + 2) % COLS if j == 0 else other
        k = j * blocks + i
        return remote(
            p_ref.at[place(dest(i), cc)], c_buf.at[k], c_send.at[k], c_recv.at[k], here.over_core
        )

    def y_copy(i):
        return remote(t_buf.at[i], y_buf.at[i], y_send.at[i], y_recv.at[i], here.over_y)

    if use_c:
        for j in range(2):
            for i in range(blocks):
                core_copy(j, i).start()
    if n_stat:
        sends, receives = stat_to(here)

        def stat_copy(k, slot, device, block):
            return remote(
                st_ref.at[block], so_ref.at[slot], s_send.at[k], s_recv.at[slot], device
            )

        for k, slot, device, block, own in sends:

            def keep(block=block, slot=slot):
                so_ref[slot] = st_ref[block]

            def go(k=k, slot=slot, device=device, block=block):
                stat_copy(k, slot, device, block).start()

            if own is None:
                go()
            elif own is True:
                keep()
            else:
                pl.when(own)(keep)
                pl.when(jnp.logical_not(own))(go)
    if use_c:
        for i in range(blocks):
            core_copy(0, i).wait_recv()
            t_buf[i] = (
                load(p_ref.at[place(dest(i), here.c_y)]) + load(c_buf.at[i])
            ).astype(BF16)
            y_copy(i).start()

    def up_copy(i, zz):
        return remote(z_out.at[i], z_in_up.at[zz], z_send.at[i], up_recv.at[zz], here.up)

    def down_copy(i, zz):
        return remote(z_out.at[i], z_in_down.at[zz], z_send.at[i], down_recv.at[zz], here.down)

    for i in range(blocks):
        zz = dest(i)
        local = load(p_ref.at[place(zz, c)])
        if use_c:
            core_copy(1, i).wait_recv()
            y_copy(i).wait_recv()
            local = local + load(c_buf.at[blocks + i]) + load(y_buf.at[i])
        if not use_z:
            o_ref[...] = local.astype(o_ref.dtype)
        elif i < ROWS - 1:
            z_out[i] = local.astype(BF16)

            def go_up(i=i, zz=zz):
                @pl.when(z > 0)
                def _():
                    up_copy(i, zz).wait_recv()
                    z_out[i] = (load(z_out.at[i]) + load(z_in_up.at[zz])).astype(BF16)

                up_copy(i, zz).start()

            def go_down(i=i, zz=zz):
                @pl.when(z < ROWS - 1)
                def _():
                    down_copy(i, zz).wait_recv()
                    z_out[i] = (load(z_out.at[i]) + load(z_in_down.at[zz])).astype(BF16)

                down_copy(i, zz).start()

            pl.when(zz > z)(go_up)
            pl.when(zz < z)(go_down)
        else:
            o_ref[...] = local.astype(o_ref.dtype)

            @pl.when(z > 0)
            def _():
                up_copy(0, z).wait_recv()
                o_ref[...] = (load(o_ref) + load(z_in_up.at[z])).astype(o_ref.dtype)

            @pl.when(z < ROWS - 1)
            def _():
                down_copy(0, z).wait_recv()
                o_ref[...] = (load(o_ref) + load(z_in_down.at[z])).astype(o_ref.dtype)

    if use_c:
        for i in range(blocks):
            core_copy(0, i).wait_send()
            core_copy(1, i).wait_send()
            y_copy(i).wait_send()
    if use_z:
        for i in range(ROWS - 1):
            up_copy(i, 0).wait_send()
    if n_stat:
        for k, slot, device, block, own in sends:
            if own is not True:
                done = functools.partial(stat_copy, k, slot, device, block)
                if own is None:
                    done().wait_send()
                else:
                    pl.when(jnp.logical_not(own))(lambda done=done: done().wait_send())
        for slot, own in receives:
            got = functools.partial(stat_copy, 0, slot, here.over_core, 0)
            if own is None:
                got().wait_recv()
            else:
                pl.when(jnp.logical_not(own))(lambda got=got: got().wait_recv())


def row_stats(here):
    others = [(d, (here.z + d) % ROWS) for d in range(1, ROWS)]
    sends = [(0, here.z, None, here.z, True)]
    sends += [(d, here.z, (here.dp, zz, here.c), zz, None) for d, zz in others]
    return sends, [(zz, None) for _, zz in others]


def plane_stats(here):
    me = here.z * COLS + here.c
    sends = [(0, me, None, here.c, True)]
    sends += [(k, me, (here.dp, zz, cc), cc, None) for k, zz, cc in here.peers()]
    return sends, [(zz * COLS + cc, None) for _, zz, cc in here.peers()]


def owner_stats(here):
    own = here.c == here.z
    sends = [(0, here.c, (here.dp, here.z, here.z), 0, own)]
    sends += [
        (d, here.c, (here.dp, (here.z + d) % ROWS, here.z), 0, None) for d in range(1, ROWS)
    ]
    receives = [(here.c, own)] + [((here.c + d) % COLS, None) for d in range(1, COLS)]
    return sends, receives


def scatter_sum(p, use_z, use_c, call, stat=None, stat_to=None, dtype=F32):
    rows, cols = p.shape
    if use_z and use_c:
        n, w = rows // COLS, cols // ROWS
        place = whole_plane(n, w)
    elif use_z:
        n, w = rows // ROWS, cols
        place = tokens_by_row(n)
    else:
        n, w = rows // COLS, cols
        place = tokens_by_col(n)
    blocks = ROWS if use_z else 1
    outs = [jax.ShapeDtypeStruct((n, w), dtype)]
    scratch = []
    if use_c:
        scratch += [
            VMEM((2 * blocks, n, w), BF16),
            VMEM((blocks, n, w), BF16),
            VMEM((blocks, n, w), BF16),
            DMA((2 * blocks,)),
            DMA((2 * blocks,)),
            DMA((blocks,)),
            DMA((blocks,)),
        ]
    if use_z:
        scratch += [
            VMEM((ROWS - 1, n, w), BF16),
            VMEM((ROWS, n, w), BF16),
            VMEM((ROWS, n, w), BF16),
            DMA((ROWS,)),
            DMA((ROWS,)),
            DMA((ROWS,)),
        ]
    args = [p]
    n_stat = 0
    if stat is not None:
        n_stat = ROWS * COLS if stat_to is plane_stats else ROWS
        outs.append(jax.ShapeDtypeStruct((n_stat,) + stat.shape[1:], stat.dtype))
        scratch += [DMA((n_stat,))] * 2
        args.append(stat)
    result = pl.pallas_call(
        functools.partial(scatter_kernel, use_z, use_c, place, stat_to, n_stat),
        out_shape=outs,
        in_specs=vm(len(args)),
        out_specs=vm(len(outs)),
        scratch_shapes=scratch,
        compiler_params=pltpu.CompilerParams(collective_id=call, has_side_effects=True),
        name=f"scatter_{call}",
    )(*args)
    return result if stat is not None else result[0]


def positions_of(segment):
    length = segment.shape[0]
    index = jnp.arange(length, dtype=jnp.int32)
    change = jnp.concatenate(
        [jnp.ones((1,), jnp.int32), (segment[1:] != segment[:-1]).astype(jnp.int32)]
    )
    starts = lax.cummax(jnp.where(change > 0, index, jnp.zeros_like(index)), axis=0)
    return index - starts


def rope_tables(segment, width):
    half = width // 2
    inverse = jnp.power(THETA, -(jnp.arange(half, dtype=F32) * (2.0 / width)))
    angle = positions_of(segment).astype(F32)[:, None] * inverse[None, :]
    return (jnp.cos(angle), jnp.sin(angle))


def rotate(field, cosine, sine):
    half = field.shape[-1] // 2
    first, second = field[..., :half], field[..., half:]
    cos_b, sin_b = cosine[:, None, :], sine[:, None, :]
    return jnp.concatenate(
        [first * cos_b - second * sin_b, second * cos_b + first * sin_b], axis=-1
    )


def unrotate(grad, cosine, sine):
    return rotate(grad, cosine, -sine)


def head_norm(field, gain):
    scale = lax.rsqrt(jnp.mean(field * field, axis=-1, keepdims=True) + EPSILON)
    unit = field * scale
    return (unit * gain, unit, scale)


def head_norm_back(grad, unit, scale, gain):
    inner = grad * gain
    back = scale * (inner - unit * jnp.mean(inner * unit, axis=-1, keepdims=True))
    return (back, jnp.sum(grad * unit, axis=(0, 1)))


def mix(form, left, right):
    return jnp.einsum(form, left, right, preferred_element_type=F32)


def allowed_of(segment):
    index = jnp.arange(segment.shape[0], dtype=jnp.int32)
    return (segment[:, None] == segment[None, :]) & (index[None, :] <= index[:, None])


def attend(query, key_rows, value_rows, allowed):
    length, heads, width = query.shape
    groups = key_rows.shape[1]
    grouped = query.reshape(length, groups, heads // groups, width)
    scores = mix("qgrd,kgd->grqk", grouped, key_rows) * width ** (-0.5)
    scores = jnp.where(allowed[None, None], scores, -1e30)
    top = jnp.max(scores, axis=-1, keepdims=True)
    weights = jnp.exp(scores - top)
    total = jnp.sum(weights, axis=-1, keepdims=True)
    probs = (weights / total).astype(BF16)
    result = mix("grqk,kgd->qgrd", probs, value_rows)
    return (result.astype(BF16).reshape(length, heads * width), (top + jnp.log(total))[..., 0])


def attend_back(query, key_rows, value_rows, allowed, mixed, grad_mixed, log_total):
    length, heads, width = query.shape
    groups = key_rows.shape[1]
    shape = (length, groups, heads // groups, width)
    scale = width ** (-0.5)
    delta = jnp.sum(
        grad_mixed.astype(F32).reshape(shape) * mixed.astype(F32).reshape(shape), axis=-1
    )
    delta = jnp.transpose(delta, (1, 2, 0))
    grouped, grad = query.reshape(shape), grad_mixed.reshape(shape)
    scores = mix("qgrd,kgd->grqk", grouped, key_rows) * scale
    scores = jnp.where(allowed[None, None], scores, -1e30)
    probs = jnp.exp(scores - log_total[..., None])
    grad_values = mix("grqk,qgrd->kgd", probs.astype(BF16), grad)
    grad_probs = mix("qgrd,kgd->grqk", grad, value_rows)
    grad_scores = (probs * (grad_probs - delta[..., None])).astype(BF16)
    grad_query = mix("grqk,kgd->qgrd", grad_scores, key_rows) * scale
    grad_keys = mix("grqk,qgrd->kgd", grad_scores, grouped) * scale
    return (grad_query.reshape(length, heads, width), grad_keys, grad_values)


def silu_parts(gate):
    sigma = jax.nn.sigmoid(gate)
    return (gate * sigma, sigma * (1.0 + gate * (1.0 - sigma)))


def dot(left, right, flipped=False):
    return lax.dot_general(
        left, right, (((1,), (1 if flipped else 0,)), ((), ())), preferred_element_type=F32
    )


def weight_term(left, right):
    return lax.dot_general(left, right, (((0,), (0,)), ((), ())), preferred_element_type=F32)


def packed(vector):
    return vector.reshape(-1, 2, HEAD_SIZE)


def over_rows(blocks, axis):
    z = lax.axis_index("row")
    block = lambda at: lax.dynamic_index_in_dim(blocks, at, 0, keepdims=False)
    got = [(z, block(z))]
    for shift in range(1, ROWS):
        ring = [(i, (i + shift) % ROWS) for i in range(ROWS)]
        got.append(((z - shift) % ROWS, lax.ppermute(block((z + shift) % ROWS), "row", ring)))
    size = blocks.shape[1:][axis]
    shape = list(blocks.shape[1:])
    shape[axis] *= ROWS
    out = jnp.zeros(shape, blocks.dtype)
    for at, piece in got:
        out = lax.dynamic_update_slice_in_dim(out, piece, at * size, axis)
    return out


def swap_dp(value):
    return lax.ppermute(value, "dp", [(0, 1), (1, 0)])


def both_halves(half, axis, dp):
    x = lax.axis_index("dp")
    other = swap_dp(half)
    stacked = jnp.stack([half, other], axis)
    return jnp.where(x == 0, stacked, jnp.flip(stacked, axis))


def spread_weight(blocks, axis, dp):
    if dp != 2:
        return over_rows(blocks, axis)
    n, w = blocks.shape[1:]
    x = lax.axis_index("dp")
    half = lax.dynamic_slice_in_dim(blocks, x * (n // 2), n // 2, 1)
    part = over_rows(half, axis)
    if axis == 0:
        part = part.reshape(ROWS, n // 2, w)
        return both_halves(part, 1, dp).reshape(ROWS * n, w)
    return both_halves(part, 0, dp).reshape(n, ROWS * w)


def sum_dp(value, dp):
    value = value.astype(BF16)
    if dp != 2:
        return lax.psum(value, "dp").astype(F32)
    return value.astype(F32) + swap_dp(value).astype(F32)


def collect_gradient(blocks, axis, dp):
    blocks = blocks.astype(BF16)
    if dp != 2:
        return over_rows(lax.psum(blocks, "dp"), axis)
    n, w = blocks.shape[1:]
    x = lax.axis_index("dp")
    half = lambda at: lax.dynamic_slice_in_dim(blocks, at * (n // 2), n // 2, 1)
    part = (half(x).astype(F32) + swap_dp(half(1 - x)).astype(F32)).astype(BF16)
    part = over_rows(part, axis)
    if axis == 0:
        return both_halves(part.reshape(ROWS, n // 2, w), 1, dp).reshape(ROWS * n, w)
    return both_halves(part, 0, dp).reshape(n, ROWS * w)


def per_device(
    dp,
    layer_input,
    cotangent,
    w_query,
    key_matrix,
    value_matrix,
    w_output,
    w_gate,
    w_up,
    w_down,
    attn_gain,
    mlp_gain,
    query_gain,
    key_gain,
    segment_ids,
):
    segment = segment_ids[0]
    length = segment.shape[0]
    feats = layer_input.shape[1]
    query_width = w_query.shape[1]
    key_width = key_matrix.shape[1]
    ff_local = w_gate.shape[1]
    units = ff_local // ROWS
    heads = lambda field: field.reshape(length, -1, HEAD_SIZE)

    in_rows = gather(layer_input, False, True, 0)
    split_cols = lambda w: jnp.transpose(w.reshape(feats, ROWS, units), (1, 0, 2))
    w_pair = spread_weight(
        jnp.concatenate([split_cols(w_gate), split_cols(w_up)], axis=2), 0, dp
    )
    w_low = spread_weight(w_down.reshape(ROWS, units, feats), 1, dp)

    cosine, sine = rope_tables(segment, HEAD_SIZE)
    allowed = allowed_of(segment)
    w_joint = jnp.concatenate([w_query, key_matrix, value_matrix], axis=1)
    inputs = layer_input.astype(F32)
    in_rows_f = in_rows.astype(F32)
    in_gained = (in_rows_f * attn_gain).astype(BF16)
    in_stat = packed(jnp.sum(in_rows_f * in_rows_f, axis=-1))
    joint, in_stats = scatter_sum(
        dot(in_gained, w_joint).astype(BF16), True, False, 1, in_stat, row_stats
    )
    scale_in = lax.rsqrt(jnp.sum(in_stats, axis=0).reshape(length, 1) / MODEL_WIDTH + EPSILON)
    joint = joint * scale_in
    query = heads(joint[:, :query_width])
    keys = heads(joint[:, query_width : query_width + key_width])
    values = heads(joint[:, query_width + key_width :].astype(BF16))
    query_norm, query_unit, query_scale = head_norm(query, query_gain)
    key_norm, key_unit, key_scale = head_norm(keys, key_gain)
    query_rot = rotate(query_norm, cosine, sine).astype(BF16)
    key_rot = rotate(key_norm, cosine, sine).astype(BF16)
    mixed, log_total = attend(query_rot, key_rot, values, allowed)
    mix_rows = gather(mixed, True, False, 2)
    hidden = inputs + scatter_sum(dot(mix_rows, w_output).astype(BF16), False, True, 3)

    cot_rows = gather(cotangent, True, True, 4)
    grad_active = dot(cot_rows, w_low, True)

    mid_gained = (hidden * mlp_gain).astype(BF16)
    mid_rows, mid_stats = gather(
        mid_gained, True, True, 5, jnp.sum(hidden * hidden, axis=-1).reshape(2, HEAD_SIZE)
    )
    tokens = mid_rows.shape[0]
    mid_sum = jnp.sum(mid_stats.reshape(ROWS, COLS, length), axis=0).reshape(tokens, 1)
    scale_mid = lax.rsqrt(mid_sum / MODEL_WIDTH + EPSILON)
    pair = dot(mid_rows, w_pair) * scale_mid
    gate, upward = pair[:, :units], pair[:, units:]
    silu, slope = silu_parts(gate)
    active = (silu * upward).astype(BF16)
    grad_gated = grad_active * scale_mid
    grad_pair_in = jnp.concatenate(
        [(grad_gated * upward * slope).astype(BF16), (grad_gated * silu).astype(BF16)], axis=1
    )
    mid_inner = jnp.sum(grad_pair_in.astype(F32) * pair, axis=-1, keepdims=True)
    grad_mid, mid_inners = scatter_sum(
        dot(grad_pair_in, w_pair, True).astype(BF16),
        True,
        True,
        6,
        packed(mid_inner * scale_mid),
        plane_stats,
    )
    grad_pair = weight_term(mid_rows, grad_pair_in)
    grad_low = weight_term(active, cot_rows)
    mid_coef = jnp.sum(mid_inners, axis=0).reshape(length, 1) / MODEL_WIDTH
    gain_mid = jnp.sum(grad_mid * hidden, axis=0)
    grad_hidden = cotangent.astype(F32) + grad_mid * mlp_gain - hidden * mid_coef
    grad_attn = grad_hidden.astype(BF16)

    attn_rows = gather(grad_attn, False, True, 7)
    grad_mixed = scatter_sum(
        dot(attn_rows, w_output, True).astype(BF16), True, False, 8, dtype=BF16
    )
    grad_output = weight_term(mix_rows, attn_rows)
    grad_query_rot, grad_key_rot, grad_values = attend_back(
        query_rot, key_rot, values, allowed, mixed, grad_mixed, log_total
    )
    grad_query_raw, gain_query = head_norm_back(
        unrotate(grad_query_rot, cosine, sine), query_unit, query_scale, query_gain
    )
    grad_key_raw, gain_key = head_norm_back(
        unrotate(grad_key_rot, cosine, sine), key_unit, key_scale, key_gain
    )
    flat = lambda field: field.reshape(length, -1)
    grad_joint_in = (
        jnp.concatenate([flat(grad_query_raw), flat(grad_key_raw), flat(grad_values)], axis=1)
        * scale_in
    ).astype(BF16)
    in_inner = jnp.sum(grad_joint_in.astype(F32) * joint, axis=-1, keepdims=True) * scale_in
    joint_rows = gather(grad_joint_in, True, False, 9)
    grad_in, in_inners = scatter_sum(
        dot(joint_rows, w_joint, True).astype(BF16), False, True, 10, packed(in_inner), owner_stats
    )
    grad_joint = weight_term(in_gained, joint_rows)
    in_coef = jnp.sum(in_inners, axis=0).reshape(length, 1) / MODEL_WIDTH
    input_grad = grad_hidden + grad_in * attn_gain - inputs * in_coef
    gain_in = jnp.sum(grad_in * inputs, axis=0)

    block = scatter_sum(dot(active, w_low).astype(BF16), True, True, 11)
    block_out = (hidden + block).astype(BF16)

    grad_pair = collect_gradient(grad_pair.reshape(ROWS, feats, 2 * units), 1, dp)
    grad_pair = grad_pair.reshape(feats, ROWS, 2, units).astype(F32)
    grad_low = jnp.transpose(grad_low.reshape(units, ROWS, feats), (1, 0, 2))
    grad_down = collect_gradient(grad_low, 0, dp).astype(F32)
    grad_joint = sum_dp(grad_joint, dp)
    grad_output = sum_dp(grad_output, dp)

    offset = lax.axis_index("row") * feats
    place = lambda part: lax.dynamic_update_slice(
        jnp.zeros((MODEL_WIDTH,), F32), part, (offset,)
    )
    gain_attn, gain_mlp, gain_q, gain_k = lax.psum(
        (place(gain_in), place(gain_mid), gain_query, gain_key), ("dp", "row", "col")
    )
    return (
        block_out,
        input_grad,
        grad_joint[:, :query_width],
        grad_joint[:, query_width : query_width + key_width],
        grad_joint[:, query_width + key_width :],
        grad_output,
        grad_pair[:, :, 0].reshape(feats, ff_local),
        grad_pair[:, :, 1].reshape(feats, ff_local),
        grad_down,
        gain_attn,
        gain_mlp,
        gain_q,
        gain_k,
    )


def solution(mesh):
    tokens, weights, flipped = P(("dp", "col"), "row"), P("row", "col"), P("col", "row")
    features, copied = P("row"), P()
    return jax.shard_map(
        functools.partial(per_device, mesh.shape["dp"]),
        mesh=mesh,
        in_specs=(
            (tokens, tokens)
            + (weights,) * 3
            + (flipped, weights, weights, flipped)
            + (features, features, copied, copied, P(("dp", "row"), None))
        ),
        out_specs=(tokens, tokens)
        + (weights,) * 3
        + (flipped, weights, weights, flipped)
        + (copied,) * 4,
        check_vma=False,
    )
```

```python
import functools
from types import SimpleNamespace

import jax
import jax.numpy as jnp
from jax import lax
from jax.experimental import pallas as pl
from jax.experimental.pallas import tpu as pltpu
from jax.sharding import PartitionSpec as P

MODEL_WIDTH = 2048
HEAD_SIZE = 128
EPSILON = 1e-06
THETA = 1000000.0
ROWS = 4
COLS = 4
STEP = 32
MESH = pl.DeviceIdType.MESH
VMEM = pltpu.VMEM
DMA = pltpu.SemaphoreType.DMA
BF16 = jnp.bfloat16
F32 = jnp.float32


def remote(src, dst, send, recv, device):
    return pltpu.make_async_remote_copy(
        src_ref=src,
        dst_ref=dst,
        send_sem=send,
        recv_sem=recv,
        device_id=device,
        device_id_type=MESH,
    )


class Here:
    def __init__(self, n_dp):
        self.n_dp = n_dp
        self.dp = lax.axis_index("dp")
        self.z = lax.axis_index("row")
        self.c = lax.axis_index("col")
        self.core = self.c % 2
        self.c_core = self.c + 1 - 2 * self.core
        self.c_y = (self.c + 2) % COLS
        self.inner = (self.z % 3 + 2) // 3
        self.up = (self.dp, self.z + 1, self.c)
        self.down = (self.dp, self.z - 1, self.c)
        self.over_y = (self.dp, self.z, self.c_y)
        self.over_core = (self.dp, self.z, self.c_core)
        self.over_dp = (1 - self.dp, self.z, self.c)

    def group(self, d):
        return ((self.dp + d) % self.n_dp, self.z, self.c)

    def peers(self):
        for dz in range(ROWS):
            for dc in range(COLS):
                if dz or dc:
                    yield dz * COLS + dc, (self.z + dz) % ROWS, (self.c + dc) % COLS

    def others(self):
        for d in range(1, ROWS):
            yield d, (self.z + d) % ROWS, (self.z - d + ROWS) % ROWS

    def row(self, z):
        return (self.dp, z, self.c)


def meet(here, kinds):
    barrier = pltpu.get_barrier_semaphore()

    def signal(device):
        pl.semaphore_signal(barrier, inc=1, device_id=device, device_id_type=MESH)

    count = 0
    if "dp" in kinds:
        for d in range(1, here.n_dp):
            signal(here.group(d))
        count += here.n_dp - 1
    if "plane" in kinds:
        for _, z, c in here.peers():
            signal((here.dp, z, c))
        count += ROWS * COLS - 1
    else:
        if "col" in kinds:
            signal(here.over_y)
            signal(here.over_core)
            count += 2
        if "rows" in kinds:
            for _, z, _ in here.others():
                signal(here.row(z))
            count += ROWS - 1
        elif "line" in kinds:
            pl.when(here.z < ROWS - 1)(lambda: signal(here.up))
            pl.when(here.z > 0)(lambda: signal(here.down))
            count = count + 1 + here.inner
    pl.semaphore_wait(barrier, count)


class Part:
    def __init__(self, args, outs, scratch, kinds, steps):
        self.args, self.outs, self.scratch = args, outs, scratch
        self.kinds, self.steps = kinds, steps


def run_parts(n_dp, call, *parts):
    counts = [(len(p.args), len(p.outs), len(p.scratch)) for p in parts]
    n_in, n_out = sum(c[0] for c in counts), sum(c[1] for c in counts)
    kinds = set().union(*[p.kinds for p in parts])

    def kernel(*refs):
        here = Here(n_dp)
        ins, outs, scratch = refs[:n_in], refs[n_in : n_in + n_out], refs[n_in + n_out :]
        meet(here, kinds)
        live = []
        for part, (a, o, s) in zip(parts, counts):
            live.append(part.steps(here, ins[:a], outs[:o], scratch[:s]))
            ins, outs, scratch = ins[a:], outs[o:], scratch[s:]
        while live:
            live = [g for g in live if next(g, "end") != "end"]

    vmem = pl.BlockSpec(memory_space=VMEM)
    results = pl.pallas_call(
        kernel,
        out_shape=[o for p in parts for o in p.outs],
        in_specs=[vmem] * n_in,
        out_specs=[vmem] * n_out,
        scratch_shapes=[s for p in parts for s in p.scratch],
        compiler_params=pltpu.CompilerParams(
            collective_id=call, has_side_effects=True, vmem_limit_bytes=60 << 20
        ),
        name=f"stage_{call}",
    )(*[x for p in parts for x in p.args])
    split = []
    for _, o, _ in counts:
        split.append(results[:o])
        results = results[o:]
    return split


def chunked(n, fn):
    step = min(STEP, n)

    def body(i, _):
        fn(pl.multiple_of(i * step, step), step)
        return 0

    lax.fori_loop(0, n // step, body, 0)


def at(place, r, step):
    rows, cols = place
    return pl.ds(rows.start + r, step), cols


def tokens_by_row(n):
    return lambda zz, cc: (pl.ds(pl.multiple_of(zz * n, n), n), slice(None))


def tokens_by_col(n):
    return lambda zz, cc: (pl.ds(pl.multiple_of(cc * n, n), n), slice(None))


def whole_plane(n, w):
    return lambda zz, cc: (
        pl.ds(pl.multiple_of(cc * n, n), n),
        pl.ds(pl.multiple_of(zz * w, w), w),
    )


def gather(x, use_z, use_c, stat=None):
    n, w = x.shape
    if use_z and use_c:
        place, shape = whole_plane(n, w), (n * COLS, w * ROWS)
    elif use_z:
        place, shape = tokens_by_row(n), (n * ROWS, w)
    else:
        place, shape = tokens_by_col(n), (n * COLS, w)
    with_stat = stat is not None
    args, outs = [x], [jax.ShapeDtypeStruct(shape, x.dtype)]
    scratch = [DMA((ROWS,))] * 5 + [DMA((2 * ROWS,))] * 2
    kinds = ({"line"} if use_z else set()) | ({"col"} if use_c else set())
    if with_stat:
        args.append(stat)
        outs.append(jax.ShapeDtypeStruct((ROWS * COLS,) + stat.shape, stat.dtype))
        scratch += [DMA((ROWS * COLS,))] * 2
        kinds.add("plane")

    def steps(here, ins, outs, sems):
        z, c = here.z, here.c
        x_ref, o_ref = ins[0], outs[0]
        up_send, down_send, z_recv, y_send, y_recv, c_send, c_recv = sems[:7]

        def slot(zz, cc):
            return o_ref.at[place(zz, cc)]

        def to_up(src, zz, d):
            return remote(src, slot(zz, c), up_send.at[d], z_recv.at[zz], here.up)

        def to_down(src, zz, d):
            return remote(src, slot(zz, c), down_send.at[d], z_recv.at[zz], here.down)

        def to_y(src, zz):
            return remote(src, slot(zz, c), y_send.at[zz], y_recv.at[zz], here.over_y)

        def to_core(src, zz, cc, half):
            k = half * ROWS + zz
            return remote(src, slot(zz, cc), c_send.at[k], c_recv.at[k], here.over_core)

        def arrived(zz, cc, sem):
            remote(slot(zz, cc), slot(zz, cc), y_send.at[0], sem, here.over_y).wait_recv()

        top, low = z < ROWS - 1, z > 0
        if use_z:
            pl.when(top)(lambda: to_up(x_ref, z, 0).start())
            pl.when(low)(lambda: to_down(x_ref, z, 0).start())
        if use_c:
            to_y(x_ref, z).start()
            to_core(x_ref, z, c, 0).start()
        if with_stat:
            st_ref, so_ref = ins[1], outs[1]
            s_send, s_recv = sems[7:]
            me = z * COLS + c
            for k, zz, cc in here.peers():
                remote(
                    st_ref, so_ref.at[me], s_send.at[k], s_recv.at[me], (here.dp, zz, cc)
                ).start()
            so_ref[me] = st_ref[...]
        mine = place(z, c)

        def keep(r, step):
            o_ref[at(mine, r, step)] = x_ref[pl.ds(r, step), :]

        chunked(n, keep)
        yield

        def from_y(zz):
            arrived(zz, here.c_y, y_recv.at[zz])
            to_core(slot(zz, here.c_y), zz, here.c_y, 1).start()

        if use_z:
            for d in range(1, ROWS):
                below, above = z - d, z + d

                def step_below(below=below, d=d):
                    arrived(below, c, z_recv.at[below])
                    pl.when(top)(lambda: to_up(slot(below, c), below, d).start())
                    if use_c:
                        to_y(slot(below, c), below).start()
                        to_core(slot(below, c), below, c, 0).start()

                def step_above(above=above, d=d):
                    arrived(above, c, z_recv.at[above])
                    pl.when(low)(lambda: to_down(slot(above, c), above, d).start())
                    if use_c:
                        to_y(slot(above, c), above).start()
                        to_core(slot(above, c), above, c, 0).start()

                pl.when(below >= 0)(step_below)
                pl.when(above < ROWS)(step_above)
                yield
                if use_c:
                    if d == 1:
                        from_y(z)
                    else:
                        pl.when(z - (d - 1) >= 0)(lambda d=d: from_y(z - (d - 1)))
                        pl.when(z + (d - 1) < ROWS)(lambda d=d: from_y(z + (d - 1)))
                    yield
            if use_c:
                pl.when(z - (ROWS - 1) >= 0)(lambda: from_y(z - (ROWS - 1)))
                pl.when(z + (ROWS - 1) < ROWS)(lambda: from_y(z + (ROWS - 1)))
                yield
        else:
            from_y(z)
            yield

        if use_z:
            pl.when(top)(lambda: to_up(x_ref, z, 0).wait_send())
            pl.when(low)(lambda: to_down(x_ref, z, 0).wait_send())
            for d in range(1, ROWS):
                below, above = z - d, z + d
                pl.when((below >= 0) & top)(
                    lambda below=below, d=d: to_up(slot(below, c), below, d).wait_send()
                )
                pl.when((above < ROWS) & low)(
                    lambda above=above, d=d: to_down(slot(above, c), above, d).wait_send()
                )
        if use_c:
            for d in range(ROWS if use_z else 1):
                zz = (z + d) % ROWS
                to_y(slot(zz, c), zz).wait_send()
                to_core(slot(zz, c), zz, c, 0).wait_send()
                to_core(slot(zz, here.c_y), zz, here.c_y, 1).wait_send()
                arrived(zz, here.c_core, c_recv.at[zz])
                arrived(zz, (here.c_core + 2) % COLS, c_recv.at[ROWS + zz])
        if with_stat:
            for k, zz, cc in here.peers():
                source = zz * COLS + cc
                copy = remote(
                    st_ref, so_ref.at[source], s_send.at[k], s_recv.at[source], (here.dp, zz, cc)
                )
                copy.wait_send()
                copy.wait_recv()

    return Part(args, outs, scratch, kinds, steps)


def row_stats(here):
    sends = [(0, here.z, None, here.z, True)]
    sends += [(d, here.z, here.row(zz), zz, None) for d, zz, _ in here.others()]
    return sends, [(zz, None) for _, zz, _ in here.others()]


def plane_stats(here):
    me = here.z * COLS + here.c
    sends = [(0, me, None, here.c, True)]
    sends += [(k, me, (here.dp, zz, cc), cc, None) for k, zz, cc in here.peers()]
    return sends, [(zz * COLS + cc, None) for _, zz, cc in here.peers()]


def owner_stats(here):
    own = here.c == here.z
    sends = [(0, here.c, (here.dp, here.z, here.z), 0, own)]
    sends += [(d, here.c, (here.dp, zz, here.z), 0, None) for d, zz, _ in here.others()]
    receives = [(here.c, own)] + [((here.c + d) % COLS, None) for d in range(1, COLS)]
    return sends, receives


def send_stats(stat, stat_to):
    count = ROWS * COLS if stat_to is plane_stats else ROWS
    outs = [jax.ShapeDtypeStruct((count,) + stat.shape[1:], stat.dtype)]

    def steps(here, ins, outs, sems):
        (st_ref,), (so_ref,), (s_send, s_recv) = ins, outs, sems
        sends, receives = stat_to(here)

        def copy(k, slot, device, block):
            return remote(
                st_ref.at[block], so_ref.at[slot], s_send.at[k], s_recv.at[slot], device
            )

        for k, slot, device, block, own in sends:

            def keep(block=block, slot=slot):
                so_ref[slot] = st_ref[block]

            def go(k=k, slot=slot, device=device, block=block):
                copy(k, slot, device, block).start()

            if own is None:
                go()
            elif own is True:
                keep()
            else:
                pl.when(own)(keep)
                pl.when(jnp.logical_not(own))(go)
        yield
        for k, slot, device, block, own in sends:
            if own is not True:
                done = functools.partial(copy, k, slot, device, block)
                if own is None:
                    done().wait_send()
                else:
                    pl.when(jnp.logical_not(own))(lambda done=done: done().wait_send())
        for slot, own in receives:
            got = functools.partial(copy, 0, slot, here.over_core, 0)
            if own is None:
                got().wait_recv()
            else:
                pl.when(jnp.logical_not(own))(lambda got=got: got().wait_recv())

    kinds = {"rows"} if stat_to is row_stats else {"plane"}
    return Part([stat], outs, [DMA((count,))] * 2, kinds, steps)


def scatter_sum(p, use_z, use_c, dtype=F32):
    rows, cols = p.shape
    if use_z and use_c:
        n, w = rows // COLS, cols // ROWS
        place = whole_plane(n, w)
    elif use_z:
        n, w = rows // ROWS, cols
        place = tokens_by_row(n)
    else:
        n, w = rows // COLS, cols
        place = tokens_by_col(n)
    blocks = ROWS if use_z else 1
    scratch = []
    if use_c:
        scratch += [VMEM((2 * blocks, n, w), BF16), VMEM((blocks, n, w), BF16)]
        scratch += [VMEM((blocks, n, w), BF16)]
        scratch += [DMA((2 * blocks,))] * 2 + [DMA((blocks,))] * 2
    if use_z:
        scratch += [VMEM((ROWS - 1, n, w), BF16)] + [VMEM((ROWS, n, w), BF16)] * 2
        scratch += [DMA((ROWS,))] * 3
    kinds = ({"line"} if use_z else set()) | ({"col"} if use_c else set())

    def steps(here, ins, outs, refs):
        z, c = here.z, here.c
        (p_ref,), (o_ref,) = ins, outs
        if use_c:
            c_buf, t_buf, y_buf, c_send, c_recv, y_send, y_recv, *refs = refs
        if use_z:
            z_out, z_up, z_down, z_send, up_recv, down_recv = refs
        mirrored = z // 2

        def dest(i):
            if not use_z:
                return z
            ends, middle = (3, 2, 1, 0)[i], (3, 0, 2, 1)[i]
            g = ends + here.inner * (middle - ends)
            return g + mirrored * (3 - 2 * g)

        def core_copy(j, i):
            other = here.c_core
            cc = (other + 2) % COLS if j == 0 else other
            k = j * blocks + i
            return remote(
                p_ref.at[place(dest(i), cc)],
                c_buf.at[k],
                c_send.at[k],
                c_recv.at[k],
                here.over_core,
            )

        def y_copy(i):
            return remote(t_buf.at[i], y_buf.at[i], y_send.at[i], y_recv.at[i], here.over_y)

        if use_c:
            for j in range(2):
                for i in range(blocks):
                    core_copy(j, i).start()
            yield
            for i in range(blocks):
                core_copy(0, i).wait_recv()
                far = place(dest(i), here.c_y)

                def add_core(r, step, i=i, far=far):
                    s = pl.ds(r, step)
                    t_buf[i, s, :] = (
                        p_ref[at(far, r, step)].astype(F32) + c_buf[i, s, :].astype(F32)
                    ).astype(BF16)

                chunked(n, add_core)
                y_copy(i).start()
            yield

        def up_copy(i, zz):
            return remote(z_out.at[i], z_up.at[zz], z_send.at[i], up_recv.at[zz], here.up)

        def down_copy(i, zz):
            return remote(z_out.at[i], z_down.at[zz], z_send.at[i], down_recv.at[zz], here.down)

        for i in range(blocks):
            zz = dest(i)
            near = place(zz, c)
            if use_c:
                core_copy(1, i).wait_recv()
                y_copy(i).wait_recv()

            def local(r, step, i=i, near=near):
                total = p_ref[at(near, r, step)].astype(F32)
                if use_c:
                    s = pl.ds(r, step)
                    total = total + c_buf[blocks + i, s, :].astype(F32)
                    total = total + y_buf[i, s, :].astype(F32)
                return total

            if not use_z:

                def store(r, step, local=local):
                    o_ref[pl.ds(r, step), :] = local(r, step).astype(o_ref.dtype)

                chunked(n, store)
            elif i < ROWS - 1:

                def send(copy, buf, first, i=i, zz=zz, local=local):
                    @pl.when(first)
                    def _():
                        def put(r, step):
                            z_out[i, pl.ds(r, step), :] = local(r, step).astype(BF16)

                        chunked(n, put)

                    @pl.when(jnp.logical_not(first))
                    def _():
                        copy(i, zz).wait_recv()

                        def put(r, step):
                            s = pl.ds(r, step)
                            z_out[i, s, :] = (
                                local(r, step) + buf[zz, s, :].astype(F32)
                            ).astype(BF16)

                        chunked(n, put)

                    copy(i, zz).start()

                pl.when(zz > z)(functools.partial(send, up_copy, z_up, z == 0))
                pl.when(zz < z)(functools.partial(send, down_copy, z_down, z == ROWS - 1))
            else:

                def final(bufs, local=local):
                    def put(r, step):
                        s = pl.ds(r, step)
                        total = local(r, step)
                        for buf in bufs:
                            total = total + buf[z, s, :].astype(F32)
                        o_ref[s, :] = total.astype(o_ref.dtype)

                    chunked(n, put)

                pl.when(z > 0)(lambda: up_copy(0, z).wait_recv())
                pl.when(z < ROWS - 1)(lambda: down_copy(0, z).wait_recv())
                pl.when(z == 0)(lambda: final([z_down]))
                pl.when(z == ROWS - 1)(lambda: final([z_up]))
                pl.when(here.inner == 1)(lambda: final([z_up, z_down]))
            yield

        if use_c:
            for i in range(blocks):
                core_copy(0, i).wait_send()
                core_copy(1, i).wait_send()
                y_copy(i).wait_send()
        if use_z:
            for i in range(ROWS - 1):
                up_copy(i, 0).wait_send()

    return Part([p], [jax.ShapeDtypeStruct((n, w), dtype)], scratch, kinds, steps)


def pull_weights(weights, axes, dp):
    outs, shapes = [], []
    for w, axis in zip(weights, axes):
        shape = list(w.shape)
        shape[axis] //= ROWS
        shape[1 - axis] *= ROWS
        outs.append(jax.ShapeDtypeStruct(tuple(shape), w.dtype))
        shapes.append((w.shape[0] // (ROWS if axis == 0 else 1), w.shape[1] // (ROWS if axis else 1)))
    count = len(weights)
    shared = dp == 2
    kinds = {"rows"} | ({"dp"} if shared else set())

    def steps(here, ins, outs, sems):
        send, recv, dp_send, dp_recv = sems

        def source(m, zz, half):
            n, w = shapes[m]
            first = zz * n if axes[m] == 0 else 0
            rows = n // 2 if half else n
            first = first + here.dp * rows if half else first
            cols = slice(None) if axes[m] == 0 else pl.ds(pl.multiple_of(zz * w, w), w)
            return pl.ds(pl.multiple_of(first, rows), rows), cols

        def target(m, zz, half):
            n, w = shapes[m]
            first = zz * n if axes[m] == 1 else 0
            rows = n // 2 if half else n
            first = first + here.dp * rows if half else first
            cols = slice(None) if axes[m] == 1 else pl.ds(pl.multiple_of(zz * w, w), w)
            return pl.ds(pl.multiple_of(first, rows), rows), cols

        def copy(m, zz, landing):
            return remote(
                ins[m].at[source(m, zz, shared)],
                outs[m].at[target(m, landing, shared)],
                send.at[m * ROWS + zz],
                recv.at[m * ROWS + landing],
                here.row(zz),
            )

        def pass_on(m, zz):
            k = m * ROWS + zz
            region = outs[m].at[target(m, zz, True)]
            return remote(region, region, dp_send.at[k], dp_recv.at[k], here.over_dp)

        for m in range(count):
            for _, zz, _ in here.others():
                copy(m, zz, here.z).start()
        for m in range(count):
            from_place, to_place = source(m, here.z, False), target(m, here.z, False)

            def keep(r, step, m=m, from_place=from_place, to_place=to_place):
                outs[m][at(to_place, r, step)] = ins[m][at(from_place, r, step)]

            chunked(shapes[m][0], keep)
        yield
        yield
        yield
        for m in range(count):
            for d in (1, 3, 2):
                zz = (here.z - d + ROWS) % ROWS
                copy(m, here.z, zz).wait_recv()
                if shared:
                    pass_on(m, zz).start()
            yield
        for m in range(count):
            for _, zz, _ in here.others():
                copy(m, zz, here.z).wait_send()
                if shared:
                    pass_on(m, zz).wait_send()
                    pass_on(m, zz).wait_recv()

    sems = [DMA((count * ROWS,))] * 4
    return Part(list(weights), outs, sems, kinds, steps)


def swap_halves_sum(values, axes):
    outs, scratch = [], []
    for v, axis in zip(values, axes):
        n, w = v.shape
        outs.append(jax.ShapeDtypeStruct((n // 2, w), BF16))
        scratch.append(VMEM((n // 2, w), BF16))
    blocks = [ROWS if axis == 1 else 1 for axis in axes]
    total = sum(blocks)
    scratch += [DMA((total,))] * 2

    def steps(here, ins, outs, refs):
        bufs, send, recv = refs[: len(values)], refs[-2], refs[-1]
        work = []
        k = 0
        for m, v in enumerate(values):
            n = v.shape[0] // blocks[m]
            h = n // 2
            for b in range(blocks[m]):
                theirs = pl.ds(pl.multiple_of(b * n + (1 - here.dp) * h, h), h)
                copy = functools.partial(
                    remote,
                    ins[m].at[theirs],
                    bufs[m].at[pl.ds(b * h, h)],
                    send.at[k],
                    recv.at[k],
                    here.over_dp,
                )
                copy().start()
                work.append((m, b, h, n, copy))
                k += 1
        for _ in range(6):
            yield
        for m, b, h, n, copy in work:
            copy().wait_recv()

            def add(r, step, m=m, b=b, h=h, n=n):
                own = pl.ds(pl.multiple_of(b * n + here.dp * h + r, step), step)
                s = pl.ds(pl.multiple_of(b * h + r, step), step)
                outs[m][s, :] = (
                    ins[m][own, :].astype(F32) + bufs[m][s, :].astype(F32)
                ).astype(BF16)

            chunked(h, add)
        for m, b, h, n, copy in work:
            copy().wait_send()

    return Part(list(values), outs, scratch, {"dp"}, steps)


def push_gradients(values, axes, dp):
    shared = dp == 2
    halves = 2 if shared else 1
    outs, shapes = [], []
    for v, axis in zip(values, axes):
        n, w = v.shape
        if axis == 1:
            n = n // ROWS
            outs.append(jax.ShapeDtypeStruct((halves, n, w * ROWS), v.dtype))
        else:
            w = w // ROWS
            outs.append(jax.ShapeDtypeStruct((ROWS, halves, n, w), v.dtype))
        shapes.append((n, w))
    count = len(values)
    kinds = {"rows"} | ({"dp"} if shared else set())

    def steps(here, ins, outs, sems):
        send, recv, dp_send, dp_recv = sems
        half = here.dp if shared else 0

        def block(m, zz):
            n, w = shapes[m]
            if axes[m] == 1:
                return ins[m].at[pl.ds(pl.multiple_of(zz * n, n), n)]
            return ins[m].at[:, pl.ds(pl.multiple_of(zz * w, w), w)]

        def slot(m, zz):
            n, w = shapes[m]
            if axes[m] == 1:
                return outs[m].at[half, :, pl.ds(pl.multiple_of(zz * w, w), w)]
            return outs[m].at[zz, half]

        def copy(m, zz, landing):
            return remote(
                block(m, zz),
                slot(m, landing),
                send.at[m * ROWS + zz],
                recv.at[m * ROWS + landing],
                here.row(zz),
            )

        def pass_on(m, zz):
            k = m * ROWS + zz
            return remote(slot(m, zz), slot(m, zz), dp_send.at[k], dp_recv.at[k], here.over_dp)

        for m in range(count):
            for _, zz, _ in here.others():
                copy(m, zz, here.z).start()
        for m in range(count):

            def keep(r, step, m=m):
                s = pl.ds(r, step)
                slot(m, here.z)[s, :] = block(m, here.z)[s, :]

            chunked(shapes[m][0], keep)
            if shared:
                pass_on(m, here.z).start()
        for _ in range(4):
            yield
        for m in range(count):
            for d in (1, 3, 2):
                zz = (here.z - d + ROWS) % ROWS
                copy(m, here.z, zz).wait_recv()
                if shared:
                    pass_on(m, zz).start()
            yield
        for m in range(count):
            for _, zz, _ in here.others():
                copy(m, zz, here.z).wait_send()
            if shared:
                for zz in range(ROWS):
                    pass_on(m, zz).wait_send()
                    remote(
                        slot(m, zz), slot(m, zz), dp_send.at[0], dp_recv.at[m * ROWS + zz], here.over_dp
                    ).wait_recv()

    sems = [DMA((count * ROWS,))] * 4
    return Part(list(values), outs, sems, kinds, steps)


def swap(values):
    outs = [jax.ShapeDtypeStruct(v.shape, v.dtype) for v in values]

    def steps(here, ins, outs, sems):
        copies = [
            remote(i, o, sems[0].at[k], sems[1].at[k], here.over_dp)
            for k, (i, o) in enumerate(zip(ins, outs))
        ]
        for copy in copies:
            copy.start()
        for _ in range(20):
            yield
        for copy in copies:
            copy.wait()

    return Part(list(values), outs, [DMA((len(values),))] * 2, {"dp"}, steps)


def sum_gains(vector, n_dp):
    shape = vector.shape

    def steps(here, ins, outs, refs):
        (v_ref,), (o_ref,) = ins, outs
        buf, part, groups, send, recv, dp_send, dp_recv = refs
        me = here.z * COLS + here.c
        for k, zz, cc in here.peers():
            remote(v_ref, buf.at[me], send.at[k], recv.at[me], (here.dp, zz, cc)).start()
        buf[me] = v_ref[...]
        yield
        for k, zz, cc in here.peers():
            source = zz * COLS + cc
            copy = remote(
                v_ref, buf.at[source], send.at[k], recv.at[source], (here.dp, zz, cc)
            )
            copy.wait_send()
            copy.wait_recv()
        for zz in range(ROWS):
            part[zz] = buf[zz * COLS] + buf[zz * COLS + 1] + buf[zz * COLS + 2] + buf[zz * COLS + 3]
        groups[here.dp] = part[...]
        for d in range(1, n_dp):
            remote(
                part, groups.at[here.dp], dp_send.at[d], dp_recv.at[here.dp], here.group(d)
            ).start()
        yield
        for d in range(1, n_dp):
            source = (here.dp + d) % n_dp
            copy = remote(
                part, groups.at[source], dp_send.at[d], dp_recv.at[source], here.group(d)
            )
            copy.wait_send()
            copy.wait_recv()
        total = groups[0]
        for d in range(1, n_dp):
            total = total + groups[d]
        o_ref[...] = total

    scratch = [
        VMEM((ROWS * COLS,) + shape, F32),
        VMEM((ROWS,) + shape, F32),
        VMEM((n_dp, ROWS) + shape, F32),
        DMA((ROWS * COLS,)),
        DMA((ROWS * COLS,)),
        DMA((n_dp,)),
        DMA((n_dp,)),
    ]
    outs = [jax.ShapeDtypeStruct((ROWS,) + shape, F32)]
    return Part([vector], outs, scratch, {"plane", "dp"}, steps)


class Plan:
    def __init__(self):
        self.specs, self.kinds = [], set()

    def add(self, part):
        first = len(self.specs)
        self.specs += part.scratch
        self.kinds |= part.kinds
        return part, first

    def buffer(self, shape, dtype):
        self.specs.append(VMEM(shape, dtype))
        return len(self.specs) - 1

    def bind(self, here, refs):
        self.here, self.refs = here, refs

    def __getitem__(self, handle):
        return self.refs[handle]

    def start(self, handle, ins, outs):
        part, first = handle
        steps = part.steps(self.here, ins, outs, self.refs[first : first + len(part.scratch)])
        next(steps, None)
        return steps


def advance(steps, count=1):
    for _ in range(count):
        next(steps, None)


def finish(steps):
    for _ in steps:
        pass


def like(shape, dtype):
    return jax.ShapeDtypeStruct(shape, dtype)


def planned(n_dp, call, name, plan, args, outs, body):
    ins, out_list = vars(args), vars(outs)

    def kernel(*refs):
        here = Here(n_dp)
        i = SimpleNamespace(**dict(zip(ins, refs)))
        o = SimpleNamespace(**dict(zip(out_list, refs[len(ins) :])))
        plan.bind(here, refs[len(ins) + len(out_list) :])
        meet(here, plan.kinds)
        body(i, o)

    vmem = pl.BlockSpec(memory_space=VMEM)
    results = pl.pallas_call(
        kernel,
        out_shape=list(out_list.values()),
        in_specs=[vmem] * len(ins),
        out_specs=[vmem] * len(out_list),
        scratch_shapes=plan.specs,
        compiler_params=pltpu.CompilerParams(
            collective_id=call, has_side_effects=True, vmem_limit_bytes=63 << 20
        ),
        name=name,
    )(*ins.values())
    return SimpleNamespace(**dict(zip(out_list, results)))


def rows_times(o_ref, a_ref, terms, block=256):
    def body(i, _):
        s = pl.ds(pl.multiple_of(i * block, block), block)
        total = None
        for columns, b_ref, flipped in terms:
            term = dot(a_ref[s, columns], b_ref[...], flipped)
            total = term if total is None else total + term
        o_ref[s, :] = total.astype(o_ref.dtype)
        return 0

    lax.fori_loop(0, a_ref.shape[0] // block, body, 0)


def columns_times(o_ref, a_ref, b_ref, height=256, width=512):
    across = b_ref.shape[1] // width

    def body(i, _):
        m = pl.ds(pl.multiple_of(i // across * height, height), height)
        n = pl.ds(pl.multiple_of(i % across * width, width), width)
        o_ref[m, n] = weight_term(a_ref[:, m], b_ref[:, n]).astype(o_ref.dtype)
        return 0

    lax.fori_loop(0, a_ref.shape[1] // height * across, body, 0)


ALL = slice(None)


def swapped(field):
    return pltpu.roll(field, HEAD_SIZE // 2, 1)


def lane_major(column):
    return jnp.transpose(jnp.broadcast_to(column, (column.shape[0], HEAD_SIZE)))[:8]


def token_major(row):
    return jnp.transpose(jnp.broadcast_to(row, (HEAD_SIZE, row.shape[1])))


def head_at(ref, h):
    return ref[:, pl.ds(h * HEAD_SIZE, HEAD_SIZE)]


def make_tables(seg_ref, inverse_ref, sign_ref, o):
    row = seg_ref[...].astype(F32)
    n = row.shape[1]
    column = token_major(row)[:, 0:1]
    query = lax.broadcasted_iota(jnp.int32, (n, n), 0)
    key = lax.broadcasted_iota(jnp.int32, (n, n), 1)
    allowed = (column == row) & (key <= query)
    o.bias[...] = jnp.where(allowed, 0.0, -1e30)
    position = jnp.sum(jnp.where(allowed, 1.0, 0.0), axis=-1, keepdims=True) - 1.0
    angle = position * inverse_ref[...]
    o.cosine[...] = jnp.cos(angle)
    o.sine[...] = jnp.sin(angle) * sign_ref[...]


def attention_forward(i, o):
    heads, groups = o.q.shape[1] // HEAD_SIZE, o.k.shape[1] // HEAD_SIZE
    each = heads // groups
    scale = HEAD_SIZE ** (-0.5)
    lane = lax.broadcasted_iota(jnp.int32, o.lse.shape, 1)

    def turned(at_head, gain_ref):
        raw = head_at(o.joint, at_head)
        norm = lax.rsqrt(jnp.mean(raw * raw, axis=-1, keepdims=True) + EPSILON)
        field = raw * norm * gain_ref[...]
        return (field * o.cosine[...] + swapped(field) * o.sine[...]).astype(BF16)

    for g in range(groups):
        at_head = pl.ds(g * HEAD_SIZE, HEAD_SIZE)
        o.k[:, at_head] = turned(heads + g, i.key_gain)
        o.v[:, at_head] = head_at(o.joint, heads + groups + g).astype(BF16)
        for h in range(g * each, (g + 1) * each):
            query = turned(h, i.query_gain)
            o.q[:, pl.ds(h * HEAD_SIZE, HEAD_SIZE)] = query
            scores = dot(query, o.k[:, at_head], True) * scale + o.bias[...]
            top = jnp.max(scores, axis=-1, keepdims=True)
            weights = jnp.exp(scores - top)
            total = jnp.sum(weights, axis=-1, keepdims=True)
            probs = (weights / total).astype(BF16)
            o.mixed[:, pl.ds(h * HEAD_SIZE, HEAD_SIZE)] = dot(probs, o.v[:, at_head]).astype(BF16)
            log_total = jnp.broadcast_to(top + jnp.log(total), o.lse.shape)
            if h == 0:
                o.lse[...] = log_total
            else:
                o.lse[...] = jnp.where(lane == h, log_total, o.lse[...])
            yield


def forward(n_dp, call, a):
    length, feats = a.layer_input.shape
    query_width, key_width = a.w_query.shape[1], a.key_matrix.shape[1]
    wide = query_width + 2 * key_width
    tokens = length * COLS
    units = a.w_gate.shape[1] // ROWS
    plan = Plan()
    in_gather = plan.add(gather(a.layer_input, False, True))
    joint_sum = plan.add(scatter_sum(like((tokens, wide), BF16), True, False))
    in_stat = plan.add(send_stats(like((ROWS, 8, length), F32), row_stats))
    cot_gather = plan.add(gather(a.cotangent, True, True))
    mix_gather = plan.add(gather(like((length, query_width), BF16), True, False))
    out_sum = plan.add(scatter_sum(like((tokens, feats), BF16), False, True))
    mid_gather = plan.add(gather(like((length, feats), BF16), True, True, like((8, length), F32)))
    pulls = [
        pull_weights([a.w_down], [0], n_dp),
        pull_weights([a.w_gate], [1], n_dp),
        pull_weights([a.w_up], [1], n_dp),
    ]
    pull_low, pull_gate, pull_up = [plan.add(p) for p in pulls]
    in_rows = plan.buffer((tokens, feats), BF16)
    stats = plan.buffer((ROWS, 8, length), F32)
    got_stats = plan.buffer((ROWS, 8, length), F32)
    mid_stats = plan.buffer((ROWS * COLS, 8, length), F32)
    own_stat = plan.buffer((8, length), F32)
    p_joint = plan.buffer((tokens, wide), BF16)
    p_out = plan.buffer((tokens, feats), BF16)
    attn_out = plan.buffer((length, feats), F32)
    gained = plan.buffer((length, feats), BF16)
    outs = SimpleNamespace(
        in_gained=like((tokens, feats), BF16),
        joint=like((length, wide), F32),
        scale_in=like((length, HEAD_SIZE), F32),
        bias=like((length, length), F32),
        cosine=like((length, HEAD_SIZE), F32),
        sine=like((length, HEAD_SIZE), F32),
        q=like((length, query_width), BF16),
        k=like((length, key_width), BF16),
        v=like((length, key_width), BF16),
        mixed=like((length, query_width), BF16),
        lse=like((length, HEAD_SIZE), F32),
        mix_rows=like((tokens, query_width), BF16),
        hidden=like((length, feats), F32),
        mid_rows=like((tokens, MODEL_WIDTH), BF16),
        scale_mid=like((tokens, HEAD_SIZE), F32),
        cot_rows=like((tokens, MODEL_WIDTH), BF16),
        w_low=pulls[0].outs[0],
        w_gate_all=pulls[1].outs[0],
        w_up_all=pulls[2].outs[0],
        grad_active=like((tokens, units), F32),
    )

    def body(i, o):
        first = plan.start(in_gather, [i.layer_input], [plan[in_rows]])
        low = plan.start(pull_low, [i.w_down], [o.w_low])
        make_tables(i.segment, i.inverse, i.sign, o)
        finish(first)

        def normed(b, _):
            s = pl.ds(pl.multiple_of(b * length, length), length)
            field = plan[in_rows][s, :].astype(F32)
            o.in_gained[s, :] = (field * i.attn_gain[...]).astype(BF16)
            plan[stats][b] = lane_major(jnp.sum(field * field, axis=-1, keepdims=True))
            for columns, w_ref in (
                (pl.ds(0, query_width), i.w_query),
                (pl.ds(query_width, key_width), i.key_matrix),
                (pl.ds(query_width + key_width, key_width), i.value_matrix),
            ):
                plan[p_joint][s, columns] = dot(o.in_gained[s, :], w_ref[...]).astype(BF16)
            return 0

        lax.fori_loop(0, COLS, normed, 0)
        total = plan.start(joint_sum, [plan[p_joint]], [o.joint])
        stat = plan.start(in_stat, [plan[stats]], [plan[got_stats]])
        finish(total)
        finish(stat)
        cot = plan.start(cot_gather, [i.cotangent], [o.cot_rows])
        summed = plan[got_stats][0] + plan[got_stats][1] + plan[got_stats][2] + plan[got_stats][3]
        o.scale_in[...] = lax.rsqrt(token_major(summed[0:1]) / MODEL_WIDTH + EPSILON)

        def scaled(r, step):
            s = pl.ds(r, step)
            o.joint[s, :] = o.joint[s, :] * o.scale_in[s, 0:1]

        chunked(length, scaled)
        for _ in attention_forward(i, o):
            pass
        mix = plan.start(mix_gather, [o.mixed], [o.mix_rows])
        advance(cot, 2)
        advance(mix)
        advance(cot, 2)
        advance(mix)
        advance(cot, 2)
        finish(mix)
        gate = plan.start(pull_gate, [i.w_gate], [o.w_gate_all])
        rows_times(plan[p_out], o.mix_rows, [(ALL, i.w_output, False)])
        out = plan.start(out_sum, [plan[p_out]], [plan[attn_out]])
        finish(cot)
        finish(out)
        finish_low = low

        def add(r, step):
            s = pl.ds(r, step)
            field = i.layer_input[s, :].astype(F32) + plan[attn_out][s, :]
            o.hidden[s, :] = field
            plan[gained][s, :] = (field * i.mlp_gain[...]).astype(BF16)

        chunked(length, add)
        plan[own_stat][...] = lane_major(
            jnp.sum(o.hidden[...] * o.hidden[...], axis=-1, keepdims=True)
        )
        mid = plan.start(
            mid_gather, [plan[gained], plan[own_stat]], [o.mid_rows, plan[mid_stats]]
        )
        up = plan.start(pull_up, [i.w_up], [o.w_up_all])
        finish(finish_low)
        advance(mid, 2)
        rows_times(o.grad_active, o.cot_rows, [(ALL, o.w_low, True)])
        advance(mid, 2)
        advance(gate, 4)
        finish(mid)
        for b in range(COLS):
            summed = plan[mid_stats][b]
            for zz in range(1, ROWS):
                summed = summed + plan[mid_stats][zz * COLS + b]
            o.scale_mid[pl.ds(b * length, length), :] = lax.rsqrt(
                token_major(summed[0:1]) / MODEL_WIDTH + EPSILON
            )
        finish(gate)
        finish(up)

    return planned(n_dp, call, "forward", plan, a, outs, body)


def attention_back(i, grad_mixed, gj_ref, inner_ref, gains_ref, dk_ref, dv_ref):
    heads, groups = i.q.shape[1] // HEAD_SIZE, i.k.shape[1] // HEAD_SIZE
    each = heads // groups
    scale = HEAD_SIZE ** (-0.5)
    cosine, sine = i.cosine[...], i.sine[...]
    scale_in = i.scale_in[:, 0:1]
    inner = jnp.zeros((i.q.shape[0], HEAD_SIZE), F32)

    def norm_back(grad_rot, at_head, gain):
        grad = grad_rot * cosine - swapped(grad_rot) * sine
        raw = head_at(i.joint, at_head)
        norm = lax.rsqrt(jnp.mean(raw * raw, axis=-1, keepdims=True) + EPSILON)
        unit = raw * norm
        u = grad * gain
        back = norm * (u - unit * jnp.mean(u * unit, axis=-1, keepdims=True))
        out = (back * scale_in).astype(BF16)
        gj_ref[:, pl.ds(at_head * HEAD_SIZE, HEAD_SIZE)] = out
        return out.astype(F32) * raw, jnp.sum(grad * unit, axis=0, keepdims=True)

    gain_q = jnp.zeros((1, HEAD_SIZE), F32)
    gain_k = jnp.zeros((1, HEAD_SIZE), F32)
    for g in range(groups):
        key, value = head_at(i.k, g), head_at(i.v, g)
        for r in range(each):
            h = g * each + r
            query, grad = head_at(i.q, h), head_at(grad_mixed, h)
            scores = dot(query, key, True) * scale + i.bias[...]
            probs = jnp.exp(scores - i.lse[:, h : h + 1])
            term_v = weight_term(probs.astype(BF16), grad)
            delta = jnp.sum(
                grad.astype(F32) * head_at(i.mixed, h).astype(F32), axis=-1, keepdims=True
            )
            grad_scores = (probs * (dot(grad, value, True) - delta)).astype(BF16)
            term_k = weight_term(grad_scores, query) * scale
            if r == 0:
                dv_ref[...] = term_v
                dk_ref[...] = term_k
            else:
                dv_ref[...] += term_v
                dk_ref[...] += term_k
            term, gain = norm_back(dot(grad_scores, key) * scale, h, i.query_gain[...])
            inner = inner + term
            gain_q = gain_q + gain
        term, gain = norm_back(dk_ref[...], heads + g, i.key_gain[...])
        inner = inner + term
        gain_k = gain_k + gain
        at_head = heads + groups + g
        out = (dv_ref[...] * scale_in).astype(BF16)
        gj_ref[:, pl.ds(at_head * HEAD_SIZE, HEAD_SIZE)] = out
        inner = inner + out.astype(F32) * head_at(i.joint, at_head)
    gains_ref[8:9, :] = gain_q
    gains_ref[9:10, :] = gain_k
    inner_ref[0] = lane_major(jnp.sum(inner, axis=-1, keepdims=True) * scale_in)


def backward(n_dp, call, a):
    two = n_dp == 2
    length, feats = a.grad_attn.shape
    query_width, key_width = a.w_query.shape[1], a.key_matrix.shape[1]
    wide = query_width + 2 * key_width
    tokens = length * COLS
    plan = Plan()
    attn_gather = plan.add(gather(a.grad_attn, False, True))
    mixed_sum = plan.add(scatter_sum(like((tokens, feats), BF16), True, False, BF16))
    joint_gather = plan.add(gather(like((length, wide), BF16), True, False))
    in_sum = plan.add(scatter_sum(like((tokens, feats), BF16), False, True))
    in_stat = plan.add(send_stats(like((1, 8, length), F32), owner_stats))
    block_sum = plan.add(scatter_sum(like((tokens, MODEL_WIDTH), BF16), True, True))
    n, w = a.grad_gate.shape
    half = like((n // 2 if two else n, w), BF16)
    if two:
        gate_half = plan.add(swap_halves_sum([a.grad_gate], [1]))
        up_half = plan.add(swap_halves_sum([a.grad_up], [1]))
        gate_sum = plan.buffer(half.shape, BF16)
        up_sum = plan.buffer(half.shape, BF16)
    pushes = [
        push_gradients([half], [1], n_dp),
        push_gradients([half], [1], n_dp),
        push_gradients([a.grad_low], [0], n_dp),
    ]
    gate_push, up_push, low_push = [plan.add(p) for p in pushes]
    gain_sum = plan.add(sum_gains(like((16, HEAD_SIZE), F32), n_dp))
    d_output, d_joint = like((feats, feats), BF16), like((feats, wide), BF16)
    if two:
        output_swap = plan.add(swap([d_output]))
        joint_swap = plan.add(swap([d_joint]))
    attn_rows = plan.buffer((tokens, feats), BF16)
    p_mixed = plan.buffer((tokens, feats), BF16)
    grad_mixed = plan.buffer((length, feats), BF16)
    joint_in = plan.buffer((length, wide), BF16)
    joint_rows = plan.buffer((tokens, wide), BF16)
    p_in = plan.buffer((tokens, feats), BF16)
    p_block = plan.buffer((tokens, MODEL_WIDTH), BF16)
    inner = plan.buffer((1, 8, length), F32)
    gain_rows = plan.buffer((16, HEAD_SIZE), F32)
    dk, dv = [plan.buffer((length, HEAD_SIZE), F32) for _ in range(2)]
    outs = SimpleNamespace(
        grad_in=like((length, feats), F32),
        in_inners=like((COLS, 8, length), F32),
        block=like((length, feats), F32),
        grad_gate=pushes[0].outs[0],
        grad_up=pushes[1].outs[0],
        grad_low=pushes[2].outs[0],
        gains=like((ROWS, 16, HEAD_SIZE), F32),
        d_output=d_output,
        d_joint=d_joint,
    )
    if two:
        outs.d_output_other, outs.d_joint_other = d_output, d_joint

    def body(i, o):
        attn = plan.start(attn_gather, [i.grad_attn], [plan[attn_rows]])
        low = plan.start(low_push, [i.grad_low], [o.grad_low])
        if two:
            halves = [
                plan.start(gate_half, [i.grad_gate], [plan[gate_sum]]),
                plan.start(up_half, [i.grad_up], [plan[up_sum]]),
            ]
        rows_times(plan[p_block], i.active, [(ALL, i.w_low, False)])
        finish(attn)
        rows_times(plan[p_mixed], plan[attn_rows], [(ALL, i.w_output, True)])
        mixed = plan.start(mixed_sum, [plan[p_mixed]], [plan[grad_mixed]])
        block = plan.start(block_sum, [plan[p_block]], [o.block])
        columns_times(o.d_output, i.mix_rows, plan[attn_rows])
        if two:
            swap_output = plan.start(output_swap, [o.d_output], [o.d_output_other])
        finish(mixed)
        if two:
            finish(halves[0])
        gate = plan.start(gate_push, [plan[gate_sum] if two else i.grad_gate], [o.grad_gate])
        plan[gain_rows][...] = i.gain_mid[...]
        attention_back(
            i,
            plan[grad_mixed],
            plan[joint_in],
            plan[inner],
            plan[gain_rows],
            plan[dk],
            plan[dv],
        )
        joint = plan.start(joint_gather, [plan[joint_in]], [plan[joint_rows]])
        stat = plan.start(in_stat, [plan[inner]], [o.in_inners])
        finish(low)
        advance(block)
        if two:
            finish(halves[1])
        finish(joint)
        up = plan.start(up_push, [plan[up_sum] if two else i.grad_up], [o.grad_up])
        columns_times(o.d_joint, i.in_gained, plan[joint_rows])
        if two:
            swap_joint = plan.start(joint_swap, [o.d_joint], [o.d_joint_other])
        rows_times(
            plan[p_in],
            plan[joint_rows],
            [
                (pl.ds(0, query_width), i.w_query, True),
                (pl.ds(query_width, key_width), i.key_matrix, True),
                (pl.ds(query_width + key_width, key_width), i.value_matrix, True),
            ],
        )
        grad_in = plan.start(in_sum, [plan[p_in]], [o.grad_in])
        finish(gate)
        finish(grad_in)
        total = jnp.sum(o.grad_in[...] * i.layer_input[...].astype(F32), axis=0, keepdims=True)
        for k in range(feats // HEAD_SIZE):
            plan[gain_rows][k : k + 1, :] = total[:, k * HEAD_SIZE : (k + 1) * HEAD_SIZE]
        gains = plan.start(gain_sum, [plan[gain_rows]], [o.gains])
        finish(block)
        finish(gains)
        finish(stat)
        finish(up)
        if two:
            finish(swap_output)
            finish(swap_joint)

    return planned(n_dp, call, "backward", plan, a, outs, body)


def silu_parts(gate):
    sigma = jax.nn.sigmoid(gate)
    return (gate * sigma, sigma * (1.0 + gate * (1.0 - sigma)))


def dot(left, right, flipped=False):
    return lax.dot_general(
        left, right, (((1,), (1 if flipped else 0,)), ((), ())), preferred_element_type=F32
    )


def weight_term(left, right):
    return lax.dot_general(left, right, (((0,), (0,)), ((), ())), preferred_element_type=F32)


def per_device(
    dp,
    layer_input,
    cotangent,
    w_query,
    key_matrix,
    value_matrix,
    w_output,
    w_gate,
    w_up,
    w_down,
    attn_gain,
    mlp_gain,
    query_gain,
    key_gain,
    segment_ids,
):
    length, feats = layer_input.shape
    query_width, key_width = w_query.shape[1], key_matrix.shape[1]
    ff_local = w_gate.shape[1]
    two = dp == 2
    half = jnp.arange(HEAD_SIZE // 2, dtype=F32)
    inverse = jnp.power(THETA, -(half * (2.0 / HEAD_SIZE)))
    ones = jnp.ones_like(half)
    f = forward(
        dp,
        0,
        SimpleNamespace(
            layer_input=layer_input,
            cotangent=cotangent,
            w_query=w_query,
            key_matrix=key_matrix,
            value_matrix=value_matrix,
            w_output=w_output,
            w_gate=w_gate,
            w_up=w_up,
            w_down=w_down,
            attn_gain=attn_gain[None],
            mlp_gain=mlp_gain[None],
            query_gain=query_gain[None],
            key_gain=key_gain[None],
            segment=segment_ids,
            inverse=jnp.concatenate([inverse, inverse])[None],
            sign=jnp.concatenate([-ones, ones])[None],
        ),
    )
    scale_mid = f.scale_mid[:, 0:1]
    gate = dot(f.mid_rows, f.w_gate_all) * scale_mid
    upward = dot(f.mid_rows, f.w_up_all) * scale_mid
    silu, slope = silu_parts(gate)
    active = (silu * upward).astype(BF16)
    grad_gated = f.grad_active * scale_mid
    grad_gate_in = (grad_gated * upward * slope).astype(BF16)
    grad_up_in = (grad_gated * silu).astype(BF16)
    mid_inner = jnp.sum(
        grad_gate_in.astype(F32) * gate + grad_up_in.astype(F32) * upward, axis=-1, keepdims=True
    )
    grad_low = weight_term(active, f.cot_rows).astype(BF16)
    grad_mid_part = dot(grad_gate_in, f.w_gate_all, True) + dot(grad_up_in, f.w_up_all, True)
    parts = [
        scatter_sum(grad_mid_part.astype(BF16), True, True),
        send_stats((mid_inner * scale_mid).reshape(COLS, 2, HEAD_SIZE), plane_stats),
    ]
    if two:
        parts.append(swap_halves_sum([grad_low], [0]))
    else:
        grad_low = lax.psum(grad_low, "dp")
    (grad_mid,), (mid_inners,), *low = run_parts(dp, 1, *parts)
    if two:
        ((grad_low,),) = low
    grad_gate = weight_term(f.mid_rows, grad_gate_in).astype(BF16)
    grad_up = weight_term(f.mid_rows, grad_up_in).astype(BF16)
    mid_coef = jnp.sum(mid_inners, axis=0).reshape(length, 1) / MODEL_WIDTH
    gain_mid = jnp.sum(grad_mid * f.hidden, axis=0)
    grad_hidden = cotangent.astype(F32) + grad_mid * mlp_gain - f.hidden * mid_coef
    grad_attn = grad_hidden.astype(BF16)
    if not two:
        grad_gate, grad_up = lax.psum(grad_gate, "dp"), lax.psum(grad_up, "dp")
    b = backward(
        dp,
        2,
        SimpleNamespace(
            grad_attn=grad_attn,
            w_output=w_output,
            w_query=w_query,
            key_matrix=key_matrix,
            value_matrix=value_matrix,
            q=f.q,
            k=f.k,
            v=f.v,
            mixed=f.mixed,
            lse=f.lse,
            bias=f.bias,
            cosine=f.cosine,
            sine=f.sine,
            joint=f.joint,
            scale_in=f.scale_in,
            query_gain=query_gain[None],
            key_gain=key_gain[None],
            mix_rows=f.mix_rows,
            in_gained=f.in_gained,
            active=active,
            w_low=f.w_low,
            grad_gate=grad_gate,
            grad_up=grad_up,
            grad_low=grad_low,
            gain_mid=jnp.pad(gain_mid.reshape(-1, HEAD_SIZE), ((4, 8), (0, 0))),
            layer_input=layer_input,
        ),
    )
    if two:
        grad_output = b.d_output.astype(F32) + b.d_output_other.astype(F32)
        grad_joint = b.d_joint.astype(F32) + b.d_joint_other.astype(F32)
    else:
        grad_output, grad_joint = lax.psum((b.d_output, b.d_joint), "dp")
        grad_output, grad_joint = grad_output.astype(F32), grad_joint.astype(F32)
    in_coef = jnp.sum(b.in_inners[:, 0], axis=0).reshape(length, 1) / MODEL_WIDTH
    input_grad = grad_hidden + b.grad_in * attn_gain - layer_input.astype(F32) * in_coef
    return (
        (f.hidden + b.block).astype(BF16),
        input_grad,
        grad_joint[:, :query_width],
        grad_joint[:, query_width : query_width + key_width],
        grad_joint[:, query_width + key_width :],
        grad_output,
        b.grad_gate.reshape(feats, ff_local).astype(F32),
        b.grad_up.reshape(feats, ff_local).astype(F32),
        b.grad_low.reshape(ff_local, feats).astype(F32),
        b.gains[:, 0:4].reshape(MODEL_WIDTH),
        b.gains[:, 4:8].reshape(MODEL_WIDTH),
        jnp.sum(b.gains[:, 8], axis=0),
        jnp.sum(b.gains[:, 9], axis=0),
    )


def solution(mesh):
    tokens, weights, flipped = P(("dp", "col"), "row"), P("row", "col"), P("col", "row")
    features, copied = P("row"), P()
    return jax.shard_map(
        functools.partial(per_device, mesh.shape["dp"]),
        mesh=mesh,
        in_specs=(
            (tokens, tokens)
            + (weights,) * 3
            + (flipped, weights, weights, flipped)
            + (features, features, copied, copied, P(("dp", "row"), None))
        ),
        out_specs=(tokens, tokens)
        + (weights,) * 3
        + (flipped, weights, weights, flipped)
        + (copied,) * 4,
        check_vma=False,
    )
```

```python
import functools
from types import SimpleNamespace

import jax
import jax.numpy as jnp
from jax import lax
from jax.experimental import pallas as pl
from jax.experimental.pallas import tpu as pltpu
from jax.sharding import PartitionSpec as P

MODEL_WIDTH = 2048
HEAD_SIZE = 128
EPSILON = 1e-06
THETA = 1000000.0
ROWS = 4
COLS = 4
STEP = 32
MESH = pl.DeviceIdType.MESH
VMEM = pltpu.VMEM
DMA = pltpu.SemaphoreType.DMA
BF16 = jnp.bfloat16
F32 = jnp.float32


def remote(src, dst, send, recv, device):
    return pltpu.make_async_remote_copy(
        src_ref=src,
        dst_ref=dst,
        send_sem=send,
        recv_sem=recv,
        device_id=device,
        device_id_type=MESH,
    )


class Here:
    def __init__(self, n_dp):
        self.n_dp = n_dp
        self.dp = lax.axis_index("dp")
        self.z = lax.axis_index("row")
        self.c = lax.axis_index("col")
        self.core = self.c % 2
        self.c_core = self.c + 1 - 2 * self.core
        self.c_y = (self.c + 2) % COLS
        self.inner = (self.z % 3 + 2) // 3
        self.up = (self.dp, self.z + 1, self.c)
        self.down = (self.dp, self.z - 1, self.c)
        self.over_y = (self.dp, self.z, self.c_y)
        self.over_core = (self.dp, self.z, self.c_core)
        self.over_dp = (1 - self.dp, self.z, self.c)

    def group(self, d):
        return ((self.dp + d) % self.n_dp, self.z, self.c)

    def peers(self):
        for dz in range(ROWS):
            for dc in range(COLS):
                if dz or dc:
                    yield dz * COLS + dc, (self.z + dz) % ROWS, (self.c + dc) % COLS

    def others(self):
        for d in range(1, ROWS):
            yield d, (self.z + d) % ROWS, (self.z - d + ROWS) % ROWS

    def row(self, z):
        return (self.dp, z, self.c)


def meet(here, kinds):
    barrier = pltpu.get_barrier_semaphore()

    def signal(device):
        pl.semaphore_signal(barrier, inc=1, device_id=device, device_id_type=MESH)

    count = 0
    if "dp" in kinds:
        for d in range(1, here.n_dp):
            signal(here.group(d))
        count += here.n_dp - 1
    if "plane" in kinds:
        for _, z, c in here.peers():
            signal((here.dp, z, c))
        count += ROWS * COLS - 1
    else:
        if "col" in kinds:
            signal(here.over_y)
            signal(here.over_core)
            count += 2
        if "rows" in kinds:
            for _, z, _ in here.others():
                signal(here.row(z))
            count += ROWS - 1
        elif "line" in kinds:
            pl.when(here.z < ROWS - 1)(lambda: signal(here.up))
            pl.when(here.z > 0)(lambda: signal(here.down))
            count = count + 1 + here.inner
    pl.semaphore_wait(barrier, count)


class Part:
    def __init__(self, args, outs, scratch, kinds, steps):
        self.args, self.outs, self.scratch = args, outs, scratch
        self.kinds, self.steps = kinds, steps


def chunked(n, fn):
    step = min(STEP, n)

    def body(i, _):
        fn(pl.multiple_of(i * step, step), step)
        return 0

    lax.fori_loop(0, n // step, body, 0)


def at(place, r, step):
    rows, cols = place
    return pl.ds(rows.start + r, step), cols


def tokens_by_row(n):
    return lambda zz, cc: (pl.ds(pl.multiple_of(zz * n, n), n), slice(None))


def tokens_by_col(n):
    return lambda zz, cc: (pl.ds(pl.multiple_of(cc * n, n), n), slice(None))


def whole_plane(n, w):
    return lambda zz, cc: (
        pl.ds(pl.multiple_of(cc * n, n), n),
        pl.ds(pl.multiple_of(zz * w, w), w),
    )


def gather(x, use_z, use_c, stat=None):
    n, w = x.shape
    if use_z and use_c:
        place, shape = whole_plane(n, w), (n * COLS, w * ROWS)
    elif use_z:
        place, shape = tokens_by_row(n), (n * ROWS, w)
    else:
        place, shape = tokens_by_col(n), (n * COLS, w)
    with_stat = stat is not None
    args, outs = [x], [jax.ShapeDtypeStruct(shape, x.dtype)]
    scratch = [DMA((ROWS,))] * 5 + [DMA((2 * ROWS,))] * 2
    kinds = ({"line"} if use_z else set()) | ({"col"} if use_c else set())
    if with_stat:
        args.append(stat)
        outs.append(jax.ShapeDtypeStruct((ROWS * COLS,) + stat.shape, stat.dtype))
        scratch += [DMA((ROWS * COLS,))] * 2
        kinds.add("plane")

    def steps(here, ins, outs, sems):
        z, c = here.z, here.c
        x_ref, o_ref = ins[0], outs[0]
        up_send, down_send, z_recv, y_send, y_recv, c_send, c_recv = sems[:7]

        def slot(zz, cc):
            return o_ref.at[place(zz, cc)]

        def to_up(src, zz, d):
            return remote(src, slot(zz, c), up_send.at[d], z_recv.at[zz], here.up)

        def to_down(src, zz, d):
            return remote(src, slot(zz, c), down_send.at[d], z_recv.at[zz], here.down)

        def to_y(src, zz):
            return remote(src, slot(zz, c), y_send.at[zz], y_recv.at[zz], here.over_y)

        def to_core(src, zz, cc, half):
            k = half * ROWS + zz
            return remote(src, slot(zz, cc), c_send.at[k], c_recv.at[k], here.over_core)

        def arrived(zz, cc, sem):
            remote(slot(zz, cc), slot(zz, cc), y_send.at[0], sem, here.over_y).wait_recv()

        top, low = z < ROWS - 1, z > 0
        if use_z:
            pl.when(top)(lambda: to_up(x_ref, z, 0).start())
            pl.when(low)(lambda: to_down(x_ref, z, 0).start())
        if use_c:
            to_y(x_ref, z).start()
            to_core(x_ref, z, c, 0).start()
        if with_stat:
            st_ref, so_ref = ins[1], outs[1]
            s_send, s_recv = sems[7:]
            me = z * COLS + c
            for k, zz, cc in here.peers():
                remote(
                    st_ref, so_ref.at[me], s_send.at[k], s_recv.at[me], (here.dp, zz, cc)
                ).start()
            so_ref[me] = st_ref[...]
        mine = place(z, c)

        def keep(r, step):
            o_ref[at(mine, r, step)] = x_ref[pl.ds(r, step), :]

        chunked(n, keep)
        yield

        def from_y(zz):
            arrived(zz, here.c_y, y_recv.at[zz])
            to_core(slot(zz, here.c_y), zz, here.c_y, 1).start()

        if use_z:
            for d in range(1, ROWS):
                below, above = z - d, z + d

                def step_below(below=below, d=d):
                    arrived(below, c, z_recv.at[below])
                    pl.when(top)(lambda: to_up(slot(below, c), below, d).start())
                    if use_c:
                        to_y(slot(below, c), below).start()
                        to_core(slot(below, c), below, c, 0).start()

                def step_above(above=above, d=d):
                    arrived(above, c, z_recv.at[above])
                    pl.when(low)(lambda: to_down(slot(above, c), above, d).start())
                    if use_c:
                        to_y(slot(above, c), above).start()
                        to_core(slot(above, c), above, c, 0).start()

                pl.when(below >= 0)(step_below)
                pl.when(above < ROWS)(step_above)
                yield
                if use_c:
                    if d == 1:
                        from_y(z)
                    else:
                        pl.when(z - (d - 1) >= 0)(lambda d=d: from_y(z - (d - 1)))
                        pl.when(z + (d - 1) < ROWS)(lambda d=d: from_y(z + (d - 1)))
                    yield
            if use_c:
                pl.when(z - (ROWS - 1) >= 0)(lambda: from_y(z - (ROWS - 1)))
                pl.when(z + (ROWS - 1) < ROWS)(lambda: from_y(z + (ROWS - 1)))
                yield
        else:
            from_y(z)
            yield

        if use_z:
            pl.when(top)(lambda: to_up(x_ref, z, 0).wait_send())
            pl.when(low)(lambda: to_down(x_ref, z, 0).wait_send())
            for d in range(1, ROWS):
                below, above = z - d, z + d
                pl.when((below >= 0) & top)(
                    lambda below=below, d=d: to_up(slot(below, c), below, d).wait_send()
                )
                pl.when((above < ROWS) & low)(
                    lambda above=above, d=d: to_down(slot(above, c), above, d).wait_send()
                )
        if use_c:
            for d in range(ROWS if use_z else 1):
                zz = (z + d) % ROWS
                to_y(slot(zz, c), zz).wait_send()
                to_core(slot(zz, c), zz, c, 0).wait_send()
                to_core(slot(zz, here.c_y), zz, here.c_y, 1).wait_send()
                arrived(zz, here.c_core, c_recv.at[zz])
                arrived(zz, (here.c_core + 2) % COLS, c_recv.at[ROWS + zz])
        if with_stat:
            for k, zz, cc in here.peers():
                source = zz * COLS + cc
                copy = remote(
                    st_ref, so_ref.at[source], s_send.at[k], s_recv.at[source], (here.dp, zz, cc)
                )
                copy.wait_send()
                copy.wait_recv()

    return Part(args, outs, scratch, kinds, steps)


def row_stats(here):
    sends = [(0, here.z, None, here.z, True)]
    sends += [(d, here.z, here.row(zz), zz, None) for d, zz, _ in here.others()]
    return sends, [(zz, None) for _, zz, _ in here.others()]


def plane_stats(here):
    me = here.z * COLS + here.c
    sends = [(0, me, None, here.c, True)]
    sends += [(k, me, (here.dp, zz, cc), cc, None) for k, zz, cc in here.peers()]
    return sends, [(zz * COLS + cc, None) for _, zz, cc in here.peers()]


def owner_stats(here):
    own = here.c == here.z
    sends = [(0, here.c, (here.dp, here.z, here.z), 0, own)]
    sends += [(d, here.c, (here.dp, zz, here.z), 0, None) for d, zz, _ in here.others()]
    receives = [(here.c, own)] + [((here.c + d) % COLS, None) for d in range(1, COLS)]
    return sends, receives


def send_stats(stat, stat_to):
    count = ROWS * COLS if stat_to is plane_stats else ROWS
    outs = [jax.ShapeDtypeStruct((count,) + stat.shape[1:], stat.dtype)]

    def steps(here, ins, outs, sems):
        (st_ref,), (so_ref,), (s_send, s_recv) = ins, outs, sems
        sends, receives = stat_to(here)

        def copy(k, slot, device, block):
            return remote(
                st_ref.at[block], so_ref.at[slot], s_send.at[k], s_recv.at[slot], device
            )

        for k, slot, device, block, own in sends:

            def keep(block=block, slot=slot):
                so_ref[slot] = st_ref[block]

            def go(k=k, slot=slot, device=device, block=block):
                copy(k, slot, device, block).start()

            if own is None:
                go()
            elif own is True:
                keep()
            else:
                pl.when(own)(keep)
                pl.when(jnp.logical_not(own))(go)
        yield
        for k, slot, device, block, own in sends:
            if own is not True:
                done = functools.partial(copy, k, slot, device, block)
                if own is None:
                    done().wait_send()
                else:
                    pl.when(jnp.logical_not(own))(lambda done=done: done().wait_send())
        for slot, own in receives:
            got = functools.partial(copy, 0, slot, here.over_core, 0)
            if own is None:
                got().wait_recv()
            else:
                pl.when(jnp.logical_not(own))(lambda got=got: got().wait_recv())

    kinds = {"rows"} if stat_to is row_stats else {"plane"}
    return Part([stat], outs, [DMA((count,))] * 2, kinds, steps)


def scatter_sum(p, use_z, use_c, dtype=F32):
    rows, cols = p.shape
    if use_z and use_c:
        n, w = rows // COLS, cols // ROWS
        place = whole_plane(n, w)
    elif use_z:
        n, w = rows // ROWS, cols
        place = tokens_by_row(n)
    else:
        n, w = rows // COLS, cols
        place = tokens_by_col(n)
    blocks = ROWS if use_z else 1
    scratch = []
    if use_c:
        scratch += [VMEM((2 * blocks, n, w), BF16), VMEM((blocks, n, w), BF16)]
        scratch += [VMEM((blocks, n, w), BF16)]
        scratch += [DMA((2 * blocks,))] * 2 + [DMA((blocks,))] * 2
    if use_z:
        scratch += [VMEM((ROWS - 1, n, w), BF16)] + [VMEM((ROWS, n, w), BF16)] * 2
        scratch += [DMA((ROWS,))] * 3
    kinds = ({"line"} if use_z else set()) | ({"col"} if use_c else set())

    def steps(here, ins, outs, refs):
        z, c = here.z, here.c
        (p_ref,), (o_ref,) = ins, outs
        if use_c:
            c_buf, t_buf, y_buf, c_send, c_recv, y_send, y_recv, *refs = refs
        if use_z:
            z_out, z_up, z_down, z_send, up_recv, down_recv = refs
        mirrored = z // 2

        def dest(i):
            if not use_z:
                return z
            ends, middle = (3, 2, 1, 0)[i], (3, 0, 2, 1)[i]
            g = ends + here.inner * (middle - ends)
            return g + mirrored * (3 - 2 * g)

        def core_copy(j, i):
            other = here.c_core
            cc = (other + 2) % COLS if j == 0 else other
            k = j * blocks + i
            return remote(
                p_ref.at[place(dest(i), cc)],
                c_buf.at[k],
                c_send.at[k],
                c_recv.at[k],
                here.over_core,
            )

        def y_copy(i):
            return remote(t_buf.at[i], y_buf.at[i], y_send.at[i], y_recv.at[i], here.over_y)

        if use_c:
            for i in range(blocks):
                core_copy(0, i).start()
            yield
            for i in range(blocks):
                core_copy(0, i).wait_recv()
                far = place(dest(i), here.c_y)

                def add_core(r, step, i=i, far=far):
                    s = pl.ds(r, step)
                    t_buf[i, s, :] = (
                        p_ref[at(far, r, step)].astype(F32) + c_buf[i, s, :].astype(F32)
                    ).astype(BF16)

                chunked(n, add_core)
                y_copy(i).start()
            yield
            for i in range(blocks):
                core_copy(1, i).start()
            yield

        def up_copy(i, zz):
            return remote(z_out.at[i], z_up.at[zz], z_send.at[i], up_recv.at[zz], here.up)

        def down_copy(i, zz):
            return remote(z_out.at[i], z_down.at[zz], z_send.at[i], down_recv.at[zz], here.down)

        for i in range(blocks):
            zz = dest(i)
            near = place(zz, c)
            if use_c:
                core_copy(1, i).wait_recv()
                y_copy(i).wait_recv()

            def local(r, step, i=i, near=near):
                total = p_ref[at(near, r, step)].astype(F32)
                if use_c:
                    s = pl.ds(r, step)
                    total = total + c_buf[blocks + i, s, :].astype(F32)
                    total = total + y_buf[i, s, :].astype(F32)
                return total

            if not use_z:

                def store(r, step, local=local):
                    o_ref[pl.ds(r, step), :] = local(r, step).astype(o_ref.dtype)

                chunked(n, store)
            elif i < ROWS - 1:

                def send(copy, buf, first, i=i, zz=zz, local=local):
                    @pl.when(first)
                    def _():
                        def put(r, step):
                            z_out[i, pl.ds(r, step), :] = local(r, step).astype(BF16)

                        chunked(n, put)

                    @pl.when(jnp.logical_not(first))
                    def _():
                        copy(i, zz).wait_recv()

                        def put(r, step):
                            s = pl.ds(r, step)
                            z_out[i, s, :] = (
                                local(r, step) + buf[zz, s, :].astype(F32)
                            ).astype(BF16)

                        chunked(n, put)

                    copy(i, zz).start()

                pl.when(zz > z)(functools.partial(send, up_copy, z_up, z == 0))
                pl.when(zz < z)(functools.partial(send, down_copy, z_down, z == ROWS - 1))
            else:

                def final(bufs, local=local):
                    def put(r, step):
                        s = pl.ds(r, step)
                        total = local(r, step)
                        for buf in bufs:
                            total = total + buf[z, s, :].astype(F32)
                        o_ref[s, :] = total.astype(o_ref.dtype)

                    chunked(n, put)

                pl.when(z > 0)(lambda: up_copy(0, z).wait_recv())
                pl.when(z < ROWS - 1)(lambda: down_copy(0, z).wait_recv())
                pl.when(z == 0)(lambda: final([z_down]))
                pl.when(z == ROWS - 1)(lambda: final([z_up]))
                pl.when(here.inner == 1)(lambda: final([z_up, z_down]))
            yield

        if use_c:
            for i in range(blocks):
                core_copy(0, i).wait_send()
                core_copy(1, i).wait_send()
                y_copy(i).wait_send()
        if use_z:
            for i in range(ROWS - 1):
                up_copy(i, 0).wait_send()

    return Part([p], [jax.ShapeDtypeStruct((n, w), dtype)], scratch, kinds, steps)


def pull_weights(weights, axes, dp):
    outs, shapes = [], []
    for w, axis in zip(weights, axes):
        shape = list(w.shape)
        shape[axis] //= ROWS
        shape[1 - axis] *= ROWS
        outs.append(jax.ShapeDtypeStruct(tuple(shape), w.dtype))
        shapes.append((w.shape[0] // (ROWS if axis == 0 else 1), w.shape[1] // (ROWS if axis else 1)))
    count = len(weights)
    shared = dp == 2
    kinds = {"rows"} | ({"dp"} if shared else set())

    def steps(here, ins, outs, sems):
        send, recv, dp_send, dp_recv = sems

        def source(m, zz, half):
            n, w = shapes[m]
            first = zz * n if axes[m] == 0 else 0
            rows = n // 2 if half else n
            first = first + here.dp * rows if half else first
            cols = slice(None) if axes[m] == 0 else pl.ds(pl.multiple_of(zz * w, w), w)
            return pl.ds(pl.multiple_of(first, rows), rows), cols

        def target(m, zz, half):
            n, w = shapes[m]
            first = zz * n if axes[m] == 1 else 0
            rows = n // 2 if half else n
            first = first + here.dp * rows if half else first
            cols = slice(None) if axes[m] == 1 else pl.ds(pl.multiple_of(zz * w, w), w)
            return pl.ds(pl.multiple_of(first, rows), rows), cols

        def copy(m, zz, landing):
            return remote(
                ins[m].at[source(m, zz, shared)],
                outs[m].at[target(m, landing, shared)],
                send.at[m * ROWS + zz],
                recv.at[m * ROWS + landing],
                here.row(zz),
            )

        def pass_on(m, zz):
            k = m * ROWS + zz
            region = outs[m].at[target(m, zz, True)]
            return remote(region, region, dp_send.at[k], dp_recv.at[k], here.over_dp)

        for m in range(count):
            for _, zz, _ in here.others():
                copy(m, zz, here.z).start()
        for m in range(count):
            from_place, to_place = source(m, here.z, False), target(m, here.z, False)

            def keep(r, step, m=m, from_place=from_place, to_place=to_place):
                outs[m][at(to_place, r, step)] = ins[m][at(from_place, r, step)]

            chunked(shapes[m][0], keep)
        yield
        for m in range(count):
            for d in (1, 3, 2):
                zz = (here.z - d + ROWS) % ROWS
                copy(m, here.z, zz).wait_recv()
                if shared:
                    pass_on(m, zz).start()
        yield
        for m in range(count):
            for _, zz, _ in here.others():
                copy(m, zz, here.z).wait_send()
                if shared:
                    pass_on(m, zz).wait_send()
                    pass_on(m, zz).wait_recv()

    sems = [DMA((count * ROWS,))] * 4
    return Part(list(weights), outs, sems, kinds, steps)


def swap_halves_sum(values, axes):
    outs, scratch = [], []
    for v, axis in zip(values, axes):
        n, w = v.shape
        outs.append(jax.ShapeDtypeStruct((n // 2, w), BF16))
        scratch.append(VMEM((n // 2, w), BF16))
    blocks = [ROWS if axis == 1 else 1 for axis in axes]
    total = sum(blocks)
    scratch += [DMA((total,))] * 2

    def steps(here, ins, outs, refs):
        bufs, send, recv = refs[: len(values)], refs[-2], refs[-1]
        work = []
        k = 0
        for m, v in enumerate(values):
            n = v.shape[0] // blocks[m]
            h = n // 2
            for b in range(blocks[m]):
                theirs = pl.ds(pl.multiple_of(b * n + (1 - here.dp) * h, h), h)
                copy = functools.partial(
                    remote,
                    ins[m].at[theirs],
                    bufs[m].at[pl.ds(b * h, h)],
                    send.at[k],
                    recv.at[k],
                    here.over_dp,
                )
                copy().start()
                work.append((m, b, h, n, copy))
                k += 1
        yield
        for m, b, h, n, copy in work:
            copy().wait_recv()

            def add(r, step, m=m, b=b, h=h, n=n):
                own = pl.ds(pl.multiple_of(b * n + here.dp * h + r, step), step)
                s = pl.ds(pl.multiple_of(b * h + r, step), step)
                outs[m][s, :] = (
                    ins[m][own, :].astype(F32) + bufs[m][s, :].astype(F32)
                ).astype(BF16)

            chunked(h, add)
        yield
        for m, b, h, n, copy in work:
            copy().wait_send()

    return Part(list(values), outs, scratch, {"dp"}, steps)


def push_gradients(values, axes, dp):
    shared = dp == 2
    halves = 2 if shared else 1
    outs, shapes = [], []
    for v, axis in zip(values, axes):
        n, w = v.shape
        if axis == 1:
            n = n // ROWS
            outs.append(jax.ShapeDtypeStruct((halves, n, w * ROWS), v.dtype))
        else:
            w = w // ROWS
            outs.append(jax.ShapeDtypeStruct((ROWS, halves, n, w), v.dtype))
        shapes.append((n, w))
    count = len(values)
    kinds = {"rows"} | ({"dp"} if shared else set())

    def steps(here, ins, outs, sems):
        send, recv, dp_send, dp_recv = sems
        half = here.dp if shared else 0

        def block(m, zz):
            n, w = shapes[m]
            if axes[m] == 1:
                return ins[m].at[pl.ds(pl.multiple_of(zz * n, n), n)]
            return ins[m].at[:, pl.ds(pl.multiple_of(zz * w, w), w)]

        def slot(m, zz):
            n, w = shapes[m]
            if axes[m] == 1:
                return outs[m].at[half, :, pl.ds(pl.multiple_of(zz * w, w), w)]
            return outs[m].at[zz, half]

        def copy(m, zz, landing):
            return remote(
                block(m, zz),
                slot(m, landing),
                send.at[m * ROWS + zz],
                recv.at[m * ROWS + landing],
                here.row(zz),
            )

        def pass_on(m, zz):
            k = m * ROWS + zz
            return remote(slot(m, zz), slot(m, zz), dp_send.at[k], dp_recv.at[k], here.over_dp)

        for m in range(count):
            for _, zz, _ in here.others():
                copy(m, zz, here.z).start()
        for m in range(count):

            def keep(r, step, m=m):
                s = pl.ds(r, step)
                slot(m, here.z)[s, :] = block(m, here.z)[s, :]

            chunked(shapes[m][0], keep)
            if shared:
                pass_on(m, here.z).start()
        yield
        for m in range(count):
            for d in (1, 3, 2):
                zz = (here.z - d + ROWS) % ROWS
                copy(m, here.z, zz).wait_recv()
                if shared:
                    pass_on(m, zz).start()
        yield
        for m in range(count):
            for _, zz, _ in here.others():
                copy(m, zz, here.z).wait_send()
            if shared:
                for zz in range(ROWS):
                    pass_on(m, zz).wait_send()
                    remote(
                        slot(m, zz), slot(m, zz), dp_send.at[0], dp_recv.at[m * ROWS + zz], here.over_dp
                    ).wait_recv()

    sems = [DMA((count * ROWS,))] * 4
    return Part(list(values), outs, sems, kinds, steps)


def swap(values):
    outs = [jax.ShapeDtypeStruct(v.shape, v.dtype) for v in values]

    def steps(here, ins, outs, sems):
        copies = [
            remote(i, o, sems[0].at[k], sems[1].at[k], here.over_dp)
            for k, (i, o) in enumerate(zip(ins, outs))
        ]
        for copy in copies:
            copy.start()
        yield
        for copy in copies:
            copy.wait()

    return Part(list(values), outs, [DMA((len(values),))] * 2, {"dp"}, steps)


def sum_gains(vector, n_dp):
    shape = vector.shape

    def steps(here, ins, outs, refs):
        (v_ref,), (o_ref,) = ins, outs
        buf, part, groups, send, recv, dp_send, dp_recv = refs
        me = here.z * COLS + here.c
        for k, zz, cc in here.peers():
            remote(v_ref, buf.at[me], send.at[k], recv.at[me], (here.dp, zz, cc)).start()
        buf[me] = v_ref[...]
        yield
        for k, zz, cc in here.peers():
            source = zz * COLS + cc
            copy = remote(
                v_ref, buf.at[source], send.at[k], recv.at[source], (here.dp, zz, cc)
            )
            copy.wait_send()
            copy.wait_recv()
        for zz in range(ROWS):
            part[zz] = buf[zz * COLS] + buf[zz * COLS + 1] + buf[zz * COLS + 2] + buf[zz * COLS + 3]
        groups[here.dp] = part[...]
        for d in range(1, n_dp):
            remote(
                part, groups.at[here.dp], dp_send.at[d], dp_recv.at[here.dp], here.group(d)
            ).start()
        yield
        for d in range(1, n_dp):
            source = (here.dp + d) % n_dp
            copy = remote(
                part, groups.at[source], dp_send.at[d], dp_recv.at[source], here.group(d)
            )
            copy.wait_send()
            copy.wait_recv()
        total = groups[0]
        for d in range(1, n_dp):
            total = total + groups[d]
        o_ref[...] = total

    scratch = [
        VMEM((ROWS * COLS,) + shape, F32),
        VMEM((ROWS,) + shape, F32),
        VMEM((n_dp, ROWS) + shape, F32),
        DMA((ROWS * COLS,)),
        DMA((ROWS * COLS,)),
        DMA((n_dp,)),
        DMA((n_dp,)),
    ]
    outs = [jax.ShapeDtypeStruct((ROWS,) + shape, F32)]
    return Part([vector], outs, scratch, {"plane", "dp"}, steps)


class Plan:
    def __init__(self):
        self.specs, self.kinds = [], set()

    def add(self, part):
        first = len(self.specs)
        self.specs += part.scratch
        self.kinds |= part.kinds
        return part, first

    def buffer(self, shape, dtype):
        self.specs.append(VMEM(shape, dtype))
        return len(self.specs) - 1

    def bind(self, here, refs):
        self.here, self.refs = here, refs

    def __getitem__(self, handle):
        return self.refs[handle]

    def start(self, handle, ins, outs):
        part, first = handle
        steps = part.steps(self.here, ins, outs, self.refs[first : first + len(part.scratch)])
        next(steps, None)
        return steps


def advance(steps, count=1):
    for _ in range(count):
        next(steps, None)


def finish(steps):
    for _ in steps:
        pass


def like(shape, dtype):
    return jax.ShapeDtypeStruct(shape, dtype)


def planned(n_dp, call, name, plan, args, outs, body):
    ins, out_list = vars(args), vars(outs)

    def kernel(*refs):
        here = Here(n_dp)
        i = SimpleNamespace(**dict(zip(ins, refs)))
        o = SimpleNamespace(**dict(zip(out_list, refs[len(ins) :])))
        plan.bind(here, refs[len(ins) + len(out_list) :])
        meet(here, plan.kinds)
        body(i, o)

    vmem = pl.BlockSpec(memory_space=VMEM)
    results = pl.pallas_call(
        kernel,
        out_shape=list(out_list.values()),
        in_specs=[vmem] * len(ins),
        out_specs=[vmem] * len(out_list),
        scratch_shapes=plan.specs,
        compiler_params=pltpu.CompilerParams(
            collective_id=call, has_side_effects=True, vmem_limit_bytes=63 << 20
        ),
        name=name,
    )(*ins.values())
    return SimpleNamespace(**dict(zip(out_list, results)))


def rows_times(o_ref, a_ref, terms, block=256, first=0, last=None):
    def body(i, _):
        s = pl.ds(pl.multiple_of(i * block, block), block)
        total = None
        for columns, b_ref, flipped in terms:
            term = dot(a_ref[s, columns], b_ref[...], flipped)
            total = term if total is None else total + term
        o_ref[s, :] = total.astype(o_ref.dtype)
        return 0

    lax.fori_loop(first, last or a_ref.shape[0] // block, body, 0)


def columns_times(o_ref, a_ref, b_ref, height=256, width=512):
    across = b_ref.shape[1] // width

    def body(i, _):
        m = pl.ds(pl.multiple_of(i // across * height, height), height)
        n = pl.ds(pl.multiple_of(i % across * width, width), width)
        o_ref[m, n] = weight_term(a_ref[:, m], b_ref[:, n]).astype(o_ref.dtype)
        return 0

    lax.fori_loop(0, a_ref.shape[1] // height * across, body, 0)


ALL = slice(None)


def swapped(field):
    return pltpu.roll(field, HEAD_SIZE // 2, 1)


def lane_major(column):
    return jnp.transpose(jnp.broadcast_to(column, (column.shape[0], HEAD_SIZE)))[:8]


def token_major(row):
    return jnp.transpose(jnp.broadcast_to(row, (HEAD_SIZE, row.shape[1])))


def head_at(ref, h):
    return ref[:, pl.ds(h * HEAD_SIZE, HEAD_SIZE)]


def make_tables(seg_ref, inverse_ref, sign_ref, o):
    row = seg_ref[...].astype(F32)
    n = row.shape[1]
    column = token_major(row)[:, 0:1]
    query = lax.broadcasted_iota(jnp.int32, (n, n), 0)
    key = lax.broadcasted_iota(jnp.int32, (n, n), 1)
    allowed = (column == row) & (key <= query)
    o.bias[...] = jnp.where(allowed, 0.0, -1e30)
    position = jnp.sum(jnp.where(allowed, 1.0, 0.0), axis=-1, keepdims=True) - 1.0
    angle = position * inverse_ref[...]
    o.cosine[...] = jnp.cos(angle)
    o.sine[...] = jnp.sin(angle) * sign_ref[...]


def attention_forward(i, o):
    heads, groups = o.q.shape[1] // HEAD_SIZE, o.k.shape[1] // HEAD_SIZE
    each = heads // groups
    scale = HEAD_SIZE ** (-0.5)
    lane = lax.broadcasted_iota(jnp.int32, o.lse.shape, 1)

    def turned(at_head, gain_ref):
        raw = head_at(o.joint, at_head)
        norm = lax.rsqrt(jnp.mean(raw * raw, axis=-1, keepdims=True) + EPSILON)
        field = raw * norm * gain_ref[...]
        return (field * o.cosine[...] + swapped(field) * o.sine[...]).astype(BF16)

    for g in range(groups):
        at_head = pl.ds(g * HEAD_SIZE, HEAD_SIZE)
        o.k[:, at_head] = turned(heads + g, i.key_gain)
        o.v[:, at_head] = head_at(o.joint, heads + groups + g).astype(BF16)
        for h in range(g * each, (g + 1) * each):
            query = turned(h, i.query_gain)
            o.q[:, pl.ds(h * HEAD_SIZE, HEAD_SIZE)] = query
            scores = dot(query, o.k[:, at_head], True) * scale + o.bias[...]
            top = jnp.max(scores, axis=-1, keepdims=True)
            weights = jnp.exp(scores - top)
            total = jnp.sum(weights, axis=-1, keepdims=True)
            probs = (weights / total).astype(BF16)
            o.mixed[:, pl.ds(h * HEAD_SIZE, HEAD_SIZE)] = dot(probs, o.v[:, at_head]).astype(BF16)
            log_total = jnp.broadcast_to(top + jnp.log(total), o.lse.shape)
            if h == 0:
                o.lse[...] = log_total
            else:
                o.lse[...] = jnp.where(lane == h, log_total, o.lse[...])
            yield


def forward(n_dp, call, a):
    length, feats = a.layer_input.shape
    query_width, key_width = a.w_query.shape[1], a.key_matrix.shape[1]
    wide = query_width + 2 * key_width
    tokens = length * COLS
    units = a.w_gate.shape[1] // ROWS
    plan = Plan()
    in_gather = plan.add(gather(a.layer_input, False, True))
    joint_sum = plan.add(scatter_sum(like((tokens, wide), BF16), True, False))
    in_stat = plan.add(send_stats(like((ROWS, 8, length), F32), row_stats))
    cot_gather = plan.add(gather(a.cotangent, True, True))
    mix_gather = plan.add(gather(like((length, query_width), BF16), True, False))
    out_sum = plan.add(scatter_sum(like((tokens, feats), BF16), False, True))
    mid_gather = plan.add(gather(like((length, feats), BF16), True, True, like((8, length), F32)))
    pulls = [
        pull_weights([a.w_down], [0], n_dp),
        pull_weights([a.w_gate], [1], n_dp),
        pull_weights([a.w_up], [1], n_dp),
    ]
    pull_low, pull_gate, pull_up = [plan.add(p) for p in pulls]
    in_rows = plan.buffer((tokens, feats), BF16)
    stats = plan.buffer((ROWS, 8, length), F32)
    got_stats = plan.buffer((ROWS, 8, length), F32)
    mid_stats = plan.buffer((ROWS * COLS, 8, length), F32)
    own_stat = plan.buffer((8, length), F32)
    p_joint = plan.buffer((tokens, wide), BF16)
    p_out = plan.buffer((tokens, feats), BF16)
    attn_out = plan.buffer((length, feats), F32)
    gained = plan.buffer((length, feats), BF16)
    outs = SimpleNamespace(
        in_gained=like((tokens, feats), BF16),
        joint=like((length, wide), F32),
        scale_in=like((length, HEAD_SIZE), F32),
        bias=like((length, length), F32),
        cosine=like((length, HEAD_SIZE), F32),
        sine=like((length, HEAD_SIZE), F32),
        q=like((length, query_width), BF16),
        k=like((length, key_width), BF16),
        v=like((length, key_width), BF16),
        mixed=like((length, query_width), BF16),
        lse=like((length, HEAD_SIZE), F32),
        mix_rows=like((tokens, query_width), BF16),
        hidden=like((length, feats), F32),
        mid_rows=like((tokens, MODEL_WIDTH), BF16),
        scale_mid=like((tokens, HEAD_SIZE), F32),
        cot_rows=like((tokens, MODEL_WIDTH), BF16),
        w_low=pulls[0].outs[0],
        w_gate_all=pulls[1].outs[0],
        w_up_all=pulls[2].outs[0],
        grad_active=like((tokens, units), F32),
    )

    def body(i, o):
        first = plan.start(in_gather, [i.layer_input], [plan[in_rows]])
        low = plan.start(pull_low, [i.w_down], [o.w_low])
        make_tables(i.segment, i.inverse, i.sign, o)
        finish(first)
        cot = plan.start(cot_gather, [i.cotangent], [o.cot_rows])

        def normed(b, _):
            s = pl.ds(pl.multiple_of(b * length, length), length)
            field = plan[in_rows][s, :].astype(F32)
            o.in_gained[s, :] = (field * i.attn_gain[...]).astype(BF16)
            plan[stats][b] = lane_major(jnp.sum(field * field, axis=-1, keepdims=True))
            for columns, w_ref in (
                (pl.ds(0, query_width), i.w_query),
                (pl.ds(query_width, key_width), i.key_matrix),
                (pl.ds(query_width + key_width, key_width), i.value_matrix),
            ):
                plan[p_joint][s, columns] = dot(o.in_gained[s, :], w_ref[...]).astype(BF16)
            return 0

        lax.fori_loop(0, COLS, normed, 0)
        total = plan.start(joint_sum, [plan[p_joint]], [o.joint])
        stat = plan.start(in_stat, [plan[stats]], [plan[got_stats]])
        advance(low)
        advance(cot)
        advance(total)
        advance(cot, 2)
        advance(total)
        advance(cot, 2)
        finish(total)
        advance(cot)
        finish(stat)
        summed = plan[got_stats][0] + plan[got_stats][1] + plan[got_stats][2] + plan[got_stats][3]
        o.scale_in[...] = lax.rsqrt(token_major(summed[0:1]) / MODEL_WIDTH + EPSILON)

        def scaled(r, step):
            s = pl.ds(r, step)
            o.joint[s, :] = o.joint[s, :] * o.scale_in[s, 0:1]

        chunked(length, scaled)
        for _ in attention_forward(i, o):
            pass
        mix = plan.start(mix_gather, [o.mixed], [o.mix_rows])
        advance(mix, 2)
        gate = plan.start(pull_gate, [i.w_gate], [o.w_gate_all])
        finish(mix)
        finish(cot)
        finish(low)
        rows_times(plan[p_out], o.mix_rows, [(ALL, i.w_output, False)])
        out = plan.start(out_sum, [plan[p_out]], [plan[attn_out]])
        advance(out, 2)
        finish(out)

        def add(r, step):
            s = pl.ds(r, step)
            field = i.layer_input[s, :].astype(F32) + plan[attn_out][s, :]
            o.hidden[s, :] = field
            plan[gained][s, :] = (field * i.mlp_gain[...]).astype(BF16)

        chunked(length, add)
        plan[own_stat][...] = lane_major(
            jnp.sum(o.hidden[...] * o.hidden[...], axis=-1, keepdims=True)
        )
        mid = plan.start(
            mid_gather, [plan[gained], plan[own_stat]], [o.mid_rows, plan[mid_stats]]
        )
        advance(mid, 2)
        advance(gate)
        advance(mid)
        up = plan.start(pull_up, [i.w_up], [o.w_up_all])
        for k in range(4):
            rows_times(
                o.grad_active, o.cot_rows, [(ALL, o.w_low, True)], first=k, last=k + 1
            )
            advance(mid)
        advance(up)
        finish(mid)
        for b in range(COLS):
            summed = plan[mid_stats][b]
            for zz in range(1, ROWS):
                summed = summed + plan[mid_stats][zz * COLS + b]
            o.scale_mid[pl.ds(b * length, length), :] = lax.rsqrt(
                token_major(summed[0:1]) / MODEL_WIDTH + EPSILON
            )
        finish(gate)
        finish(up)

    return planned(n_dp, call, "forward", plan, a, outs, body)


def middle(n_dp, call, a):
    two = n_dp == 2
    length, feats = a.hidden.shape
    tokens, units = a.grad_active.shape
    plan = Plan()
    mid_sum = plan.add(scatter_sum(like((tokens, MODEL_WIDTH), BF16), True, True))
    inner_stat = plan.add(send_stats(like((COLS, 8, length), F32), plane_stats))
    d_low = like((units, MODEL_WIDTH), BF16)
    if two:
        low_half = plan.add(swap_halves_sum([d_low], [0]))
        low = plan.buffer(d_low.shape, BF16)
        d_low = like((units // 2, MODEL_WIDTH), BF16)
    p_mid = plan.buffer((tokens, MODEL_WIDTH), BF16)
    d_gate = plan.buffer((tokens, units), BF16)
    d_up = plan.buffer((tokens, units), BF16)
    inner = plan.buffer((COLS, 8, length), F32)
    inners = plan.buffer((ROWS * COLS, 8, length), F32)
    grad_mid = plan.buffer((length, feats), F32)
    outs = SimpleNamespace(
        grad_hidden=like((length, feats), F32),
        grad_attn=like((length, feats), BF16),
        gain_mid=like((16, HEAD_SIZE), F32),
        active=like((tokens, units), BF16),
        grad_low=d_low,
        grad_gate=like((MODEL_WIDTH, units), BF16),
        grad_up=like((MODEL_WIDTH, units), BF16),
    )

    def body(i, o):
        here = plan.here

        def tokens_of(b):
            s = pl.ds(pl.multiple_of(b * length, length), length)
            scale = i.scale_mid[s, 0:1]
            gate = dot(i.mid_rows[s, :], i.w_gate_all[...]) * scale
            upward = dot(i.mid_rows[s, :], i.w_up_all[...]) * scale
            silu, slope = silu_parts(gate)
            o.active[s, :] = (silu * upward).astype(BF16)
            grad = i.grad_active[s, :] * scale
            grad_gate = (grad * upward * slope).astype(BF16)
            grad_up = (grad * silu).astype(BF16)
            plan[d_gate][s, :] = grad_gate
            plan[d_up][s, :] = grad_up
            term = grad_gate.astype(F32) * gate + grad_up.astype(F32) * upward
            plan[inner][b] = lane_major(jnp.sum(term, axis=-1, keepdims=True) * scale)
            for k in range(ROWS):
                part = pl.ds(k * feats, feats)
                plan[p_mid][s, part] = (
                    dot(grad_gate, i.w_gate_all[part, :], True)
                    + dot(grad_up, i.w_up_all[part, :], True)
                ).astype(BF16)

        tokens_of((here.c_core + 2) % COLS)
        total = plan.start(mid_sum, [plan[p_mid]], [plan[grad_mid]])
        tokens_of(here.c_y)
        advance(total)
        tokens_of(here.c_core)
        advance(total)
        tokens_of(here.c)
        stat = plan.start(inner_stat, [plan[inner]], [plan[inners]])
        advance(total)
        low_ref = plan[low] if two else o.grad_low
        columns_times(low_ref, o.active, i.cot_rows, units)
        if two:
            low_sum = plan.start(low_half, [low_ref], [o.grad_low])
        advance(total)
        columns_times(o.grad_gate, i.mid_rows, plan[d_gate], width=units)
        advance(total)
        columns_times(o.grad_up, i.mid_rows, plan[d_up], width=units)
        finish(total)
        finish(stat)
        summed = plan[inners][0]
        for k in range(1, ROWS * COLS):
            summed = summed + plan[inners][k]
        coef = token_major(summed[0:1] / MODEL_WIDTH)[:, 0:1]
        grad = plan[grad_mid][...]
        hidden = i.hidden[...]
        total = jnp.sum(grad * hidden, axis=0, keepdims=True)
        o.gain_mid[...] = jnp.zeros((16, HEAD_SIZE), F32)
        for k in range(feats // HEAD_SIZE):
            o.gain_mid[4 + k : 5 + k, :] = total[:, k * HEAD_SIZE : (k + 1) * HEAD_SIZE]
        grad = i.cotangent[...].astype(F32) + grad * i.mlp_gain[...] - hidden * coef
        o.grad_hidden[...] = grad
        o.grad_attn[...] = grad.astype(BF16)
        if two:
            finish(low_sum)

    return planned(n_dp, call, "middle", plan, a, outs, body)


def attention_back(i, grad_mixed, gj_ref, inner_ref, gains_ref, dk_ref, dv_ref):
    heads, groups = i.q.shape[1] // HEAD_SIZE, i.k.shape[1] // HEAD_SIZE
    each = heads // groups
    scale = HEAD_SIZE ** (-0.5)
    cosine, sine = i.cosine[...], i.sine[...]
    scale_in = i.scale_in[:, 0:1]
    inner = jnp.zeros((i.q.shape[0], HEAD_SIZE), F32)

    def norm_back(grad_rot, at_head, gain):
        grad = grad_rot * cosine - swapped(grad_rot) * sine
        raw = head_at(i.joint, at_head)
        norm = lax.rsqrt(jnp.mean(raw * raw, axis=-1, keepdims=True) + EPSILON)
        unit = raw * norm
        u = grad * gain
        back = norm * (u - unit * jnp.mean(u * unit, axis=-1, keepdims=True))
        out = (back * scale_in).astype(BF16)
        gj_ref[:, pl.ds(at_head * HEAD_SIZE, HEAD_SIZE)] = out
        return out.astype(F32) * raw, jnp.sum(grad * unit, axis=0, keepdims=True)

    gain_q = jnp.zeros((1, HEAD_SIZE), F32)
    gain_k = jnp.zeros((1, HEAD_SIZE), F32)
    for g in range(groups):
        key, value = head_at(i.k, g), head_at(i.v, g)
        for r in range(each):
            h = g * each + r
            query, grad = head_at(i.q, h), head_at(grad_mixed, h)
            scores = dot(query, key, True) * scale + i.bias[...]
            probs = jnp.exp(scores - i.lse[:, h : h + 1])
            term_v = weight_term(probs.astype(BF16), grad)
            delta = jnp.sum(
                grad.astype(F32) * head_at(i.mixed, h).astype(F32), axis=-1, keepdims=True
            )
            grad_scores = (probs * (dot(grad, value, True) - delta)).astype(BF16)
            term_k = weight_term(grad_scores, query) * scale
            if r == 0:
                dv_ref[...] = term_v
                dk_ref[...] = term_k
            else:
                dv_ref[...] += term_v
                dk_ref[...] += term_k
            term, gain = norm_back(dot(grad_scores, key) * scale, h, i.query_gain[...])
            inner = inner + term
            gain_q = gain_q + gain
        term, gain = norm_back(dk_ref[...], heads + g, i.key_gain[...])
        inner = inner + term
        gain_k = gain_k + gain
        at_head = heads + groups + g
        out = (dv_ref[...] * scale_in).astype(BF16)
        gj_ref[:, pl.ds(at_head * HEAD_SIZE, HEAD_SIZE)] = out
        inner = inner + out.astype(F32) * head_at(i.joint, at_head)
    gains_ref[8:9, :] = gain_q
    gains_ref[9:10, :] = gain_k
    inner_ref[0] = lane_major(jnp.sum(inner, axis=-1, keepdims=True) * scale_in)


def backward(n_dp, call, a):
    two = n_dp == 2
    length, feats = a.grad_attn.shape
    query_width, key_width = a.w_query.shape[1], a.key_matrix.shape[1]
    wide = query_width + 2 * key_width
    tokens = length * COLS
    plan = Plan()
    attn_gather = plan.add(gather(a.grad_attn, False, True))
    mixed_sum = plan.add(scatter_sum(like((tokens, feats), BF16), True, False, BF16))
    joint_gather = plan.add(gather(like((length, wide), BF16), True, False))
    in_sum = plan.add(scatter_sum(like((tokens, feats), BF16), False, True))
    in_stat = plan.add(send_stats(like((1, 8, length), F32), owner_stats))
    block_sum = plan.add(scatter_sum(like((tokens, MODEL_WIDTH), BF16), True, True))
    n, w = a.grad_gate.shape
    half = like((n // 2 if two else n, w), BF16)
    if two:
        gate_half = plan.add(swap_halves_sum([a.grad_gate], [1]))
        up_half = plan.add(swap_halves_sum([a.grad_up], [1]))
        gate_sum = plan.buffer(half.shape, BF16)
        up_sum = plan.buffer(half.shape, BF16)
    pushes = [
        push_gradients([half], [1], n_dp),
        push_gradients([half], [1], n_dp),
        push_gradients([a.grad_low], [0], n_dp),
    ]
    gate_push, up_push, low_push = [plan.add(p) for p in pushes]
    gain_sum = plan.add(sum_gains(like((16, HEAD_SIZE), F32), n_dp))
    d_output, d_joint = like((feats, feats), BF16), like((feats, wide), BF16)
    if two:
        output_swap = plan.add(swap([d_output]))
        joint_swap = plan.add(swap([d_joint]))
    attn_rows = plan.buffer((tokens, feats), BF16)
    p_mixed = plan.buffer((tokens, feats), BF16)
    grad_mixed = plan.buffer((length, feats), BF16)
    joint_in = plan.buffer((length, wide), BF16)
    joint_rows = plan.buffer((tokens, wide), BF16)
    p_in = plan.buffer((tokens, feats), BF16)
    p_block = plan.buffer((tokens, MODEL_WIDTH), BF16)
    inner = plan.buffer((1, 8, length), F32)
    gain_rows = plan.buffer((16, HEAD_SIZE), F32)
    dk, dv = [plan.buffer((length, HEAD_SIZE), F32) for _ in range(2)]
    outs = SimpleNamespace(
        grad_in=like((length, feats), F32),
        in_inners=like((COLS, 8, length), F32),
        block=like((length, feats), F32),
        grad_gate=pushes[0].outs[0],
        grad_up=pushes[1].outs[0],
        grad_low=pushes[2].outs[0],
        gains=like((ROWS, 16, HEAD_SIZE), F32),
        d_output=d_output,
        d_joint=d_joint,
    )
    if two:
        outs.d_output_other, outs.d_joint_other = d_output, d_joint

    def body(i, o):
        attn = plan.start(attn_gather, [i.grad_attn], [plan[attn_rows]])
        low = plan.start(low_push, [i.grad_low], [o.grad_low])
        if two:
            gate_sums = plan.start(gate_half, [i.grad_gate], [plan[gate_sum]])
        rows_times(plan[p_block], i.active, [(ALL, i.w_low, False)], first=0, last=3)
        finish(attn)
        if two:
            up_sums = plan.start(up_half, [i.grad_up], [plan[up_sum]])
        rows_times(plan[p_mixed], plan[attn_rows], [(ALL, i.w_output, True)])
        mixed = plan.start(mixed_sum, [plan[p_mixed]], [plan[grad_mixed]])
        rows_times(plan[p_block], i.active, [(ALL, i.w_low, False)], first=3, last=4)
        block = plan.start(block_sum, [plan[p_block]], [o.block])
        advance(mixed)
        advance(low)
        advance(block, 2)
        if two:
            advance(gate_sums)
        advance(mixed)
        gate = plan.start(gate_push, [plan[gate_sum] if two else i.grad_gate], [o.grad_gate])
        finish(mixed)
        plan[gain_rows][...] = i.gain_mid[...]
        attention_back(
            i,
            plan[grad_mixed],
            plan[joint_in],
            plan[inner],
            plan[gain_rows],
            plan[dk],
            plan[dv],
        )
        joint = plan.start(joint_gather, [plan[joint_in]], [plan[joint_rows]])
        stat = plan.start(in_stat, [plan[inner]], [o.in_inners])
        columns_times(o.d_output, i.mix_rows, plan[attn_rows])
        if two:
            swap_output = plan.start(output_swap, [o.d_output], [o.d_output_other])
        advance(block)
        advance(joint)
        if two:
            advance(up_sums)
        advance(block)
        advance(gate)
        advance(joint)
        up = plan.start(up_push, [plan[up_sum] if two else i.grad_up], [o.grad_up])
        advance(block)
        finish(joint)
        columns_times(o.d_joint, i.in_gained, plan[joint_rows])
        if two:
            swap_joint = plan.start(joint_swap, [o.d_joint], [o.d_joint_other])
        rows_times(
            plan[p_in],
            plan[joint_rows],
            [
                (pl.ds(0, query_width), i.w_query, True),
                (pl.ds(query_width, key_width), i.key_matrix, True),
                (pl.ds(query_width + key_width, key_width), i.value_matrix, True),
            ],
        )
        grad_in = plan.start(in_sum, [plan[p_in]], [o.grad_in])
        advance(grad_in)
        advance(block)
        advance(up)
        finish(grad_in)
        total = jnp.sum(o.grad_in[...] * i.layer_input[...].astype(F32), axis=0, keepdims=True)
        for k in range(feats // HEAD_SIZE):
            plan[gain_rows][k : k + 1, :] = total[:, k * HEAD_SIZE : (k + 1) * HEAD_SIZE]
        gains = plan.start(gain_sum, [plan[gain_rows]], [o.gains])
        finish(block)
        finish(gains)
        finish(stat)
        finish(low)
        finish(gate)
        finish(up)
        if two:
            finish(gate_sums)
            finish(up_sums)
            finish(swap_output)
            finish(swap_joint)

    return planned(n_dp, call, "backward", plan, a, outs, body)


def silu_parts(gate):
    sigma = jax.nn.sigmoid(gate)
    return (gate * sigma, sigma * (1.0 + gate * (1.0 - sigma)))


def dot(left, right, flipped=False):
    return lax.dot_general(
        left, right, (((1,), (1 if flipped else 0,)), ((), ())), preferred_element_type=F32
    )


def weight_term(left, right):
    return lax.dot_general(left, right, (((0,), (0,)), ((), ())), preferred_element_type=F32)


def per_device(
    dp,
    layer_input,
    cotangent,
    w_query,
    key_matrix,
    value_matrix,
    w_output,
    w_gate,
    w_up,
    w_down,
    attn_gain,
    mlp_gain,
    query_gain,
    key_gain,
    segment_ids,
):
    length, feats = layer_input.shape
    query_width, key_width = w_query.shape[1], key_matrix.shape[1]
    ff_local = w_gate.shape[1]
    two = dp == 2
    half = jnp.arange(HEAD_SIZE // 2, dtype=F32)
    inverse = jnp.power(THETA, -(half * (2.0 / HEAD_SIZE)))
    ones = jnp.ones_like(half)
    f = forward(
        dp,
        0,
        SimpleNamespace(
            layer_input=layer_input,
            cotangent=cotangent,
            w_query=w_query,
            key_matrix=key_matrix,
            value_matrix=value_matrix,
            w_output=w_output,
            w_gate=w_gate,
            w_up=w_up,
            w_down=w_down,
            attn_gain=attn_gain[None],
            mlp_gain=mlp_gain[None],
            query_gain=query_gain[None],
            key_gain=key_gain[None],
            segment=segment_ids,
            inverse=jnp.concatenate([inverse, inverse])[None],
            sign=jnp.concatenate([-ones, ones])[None],
        ),
    )
    m = middle(
        dp,
        1,
        SimpleNamespace(
            mid_rows=f.mid_rows,
            cot_rows=f.cot_rows,
            grad_active=f.grad_active,
            scale_mid=f.scale_mid,
            w_gate_all=f.w_gate_all,
            w_up_all=f.w_up_all,
            hidden=f.hidden,
            cotangent=cotangent,
            mlp_gain=mlp_gain[None],
        ),
    )
    grad_low, grad_gate, grad_up = m.grad_low, m.grad_gate, m.grad_up
    if not two:
        grad_low, grad_gate, grad_up = lax.psum((grad_low, grad_gate, grad_up), "dp")
    b = backward(
        dp,
        2,
        SimpleNamespace(
            grad_attn=m.grad_attn,
            w_output=w_output,
            w_query=w_query,
            key_matrix=key_matrix,
            value_matrix=value_matrix,
            q=f.q,
            k=f.k,
            v=f.v,
            mixed=f.mixed,
            lse=f.lse,
            bias=f.bias,
            cosine=f.cosine,
            sine=f.sine,
            joint=f.joint,
            scale_in=f.scale_in,
            query_gain=query_gain[None],
            key_gain=key_gain[None],
            mix_rows=f.mix_rows,
            in_gained=f.in_gained,
            active=m.active,
            w_low=f.w_low,
            grad_gate=grad_gate,
            grad_up=grad_up,
            grad_low=grad_low,
            gain_mid=m.gain_mid,
            layer_input=layer_input,
        ),
    )
    if two:
        grad_output = b.d_output.astype(F32) + b.d_output_other.astype(F32)
        grad_joint = b.d_joint.astype(F32) + b.d_joint_other.astype(F32)
    else:
        grad_output, grad_joint = lax.psum((b.d_output, b.d_joint), "dp")
        grad_output, grad_joint = grad_output.astype(F32), grad_joint.astype(F32)
    in_coef = jnp.sum(b.in_inners[:, 0], axis=0).reshape(length, 1) / MODEL_WIDTH
    input_grad = m.grad_hidden + b.grad_in * attn_gain - layer_input.astype(F32) * in_coef
    return (
        (f.hidden + b.block).astype(BF16),
        input_grad,
        grad_joint[:, :query_width],
        grad_joint[:, query_width : query_width + key_width],
        grad_joint[:, query_width + key_width :],
        grad_output,
        b.grad_gate.reshape(feats, ff_local).astype(F32),
        b.grad_up.reshape(feats, ff_local).astype(F32),
        b.grad_low.reshape(ff_local, feats).astype(F32),
        b.gains[:, 0:4].reshape(MODEL_WIDTH),
        b.gains[:, 4:8].reshape(MODEL_WIDTH),
        jnp.sum(b.gains[:, 8], axis=0),
        jnp.sum(b.gains[:, 9], axis=0),
    )


def solution(mesh):
    tokens, weights, flipped = P(("dp", "col"), "row"), P("row", "col"), P("col", "row")
    features, copied = P("row"), P()
    return jax.shard_map(
        functools.partial(per_device, mesh.shape["dp"]),
        mesh=mesh,
        in_specs=(
            (tokens, tokens)
            + (weights,) * 3
            + (flipped, weights, weights, flipped)
            + (features, features, copied, copied, P(("dp", "row"), None))
        ),
        out_specs=(tokens, tokens)
        + (weights,) * 3
        + (flipped, weights, weights, flipped)
        + (copied,) * 4,
        check_vma=False,
    )
```

```python
import functools
from types import SimpleNamespace

import jax
import jax.numpy as jnp
from jax import lax
from jax.experimental import pallas as pl
from jax.experimental.pallas import tpu as pltpu
from jax.sharding import PartitionSpec as P

MODEL_WIDTH = 2048
HEAD_SIZE = 128
EPSILON = 1e-06
THETA = 1000000.0
ROWS = 4
COLS = 4
STEP = 32
MESH = pl.DeviceIdType.MESH
VMEM = pltpu.VMEM
DMA = pltpu.SemaphoreType.DMA
BF16 = jnp.bfloat16
F32 = jnp.float32


def remote(src, dst, send, recv, device):
    return pltpu.make_async_remote_copy(
        src_ref=src,
        dst_ref=dst,
        send_sem=send,
        recv_sem=recv,
        device_id=device,
        device_id_type=MESH,
    )


class Here:
    def __init__(self, n_dp):
        self.n_dp = n_dp
        self.dp = lax.axis_index("dp")
        self.z = lax.axis_index("row")
        self.c = lax.axis_index("col")
        self.core = self.c % 2
        self.c_core = self.c + 1 - 2 * self.core
        self.c_y = (self.c + 2) % COLS
        self.inner = (self.z % 3 + 2) // 3
        self.up = (self.dp, self.z + 1, self.c)
        self.down = (self.dp, self.z - 1, self.c)
        self.over_y = (self.dp, self.z, self.c_y)
        self.over_core = (self.dp, self.z, self.c_core)
        self.over_dp = (1 - self.dp, self.z, self.c)

    def group(self, d):
        return ((self.dp + d) % self.n_dp, self.z, self.c)

    def peers(self):
        for dz in range(ROWS):
            for dc in range(COLS):
                if dz or dc:
                    yield dz * COLS + dc, (self.z + dz) % ROWS, (self.c + dc) % COLS

    def others(self):
        for d in range(1, ROWS):
            yield d, (self.z + d) % ROWS, (self.z - d + ROWS) % ROWS

    def row(self, z):
        return (self.dp, z, self.c)


def meet(here, kinds):
    barrier = pltpu.get_barrier_semaphore()

    def signal(device):
        pl.semaphore_signal(barrier, inc=1, device_id=device, device_id_type=MESH)

    count = 0
    if "dp" in kinds:
        for d in range(1, here.n_dp):
            signal(here.group(d))
        count += here.n_dp - 1
    if "plane" in kinds:
        for _, z, c in here.peers():
            signal((here.dp, z, c))
        count += ROWS * COLS - 1
    else:
        if "col" in kinds:
            signal(here.over_y)
            signal(here.over_core)
            count += 2
        if "rows" in kinds:
            for _, z, _ in here.others():
                signal(here.row(z))
            count += ROWS - 1
        elif "line" in kinds:
            pl.when(here.z < ROWS - 1)(lambda: signal(here.up))
            pl.when(here.z > 0)(lambda: signal(here.down))
            count = count + 1 + here.inner
    pl.semaphore_wait(barrier, count)


class Part:
    def __init__(self, args, outs, scratch, kinds, steps):
        self.args, self.outs, self.scratch = args, outs, scratch
        self.kinds, self.steps = kinds, steps


def chunked(n, fn):
    step = min(STEP, n)

    def body(i, _):
        fn(pl.multiple_of(i * step, step), step)
        return 0

    lax.fori_loop(0, n // step, body, 0)


def at(place, r, step):
    rows, cols = place
    return pl.ds(rows.start + r, step), cols


def tokens_by_row(n):
    return lambda zz, cc: (pl.ds(pl.multiple_of(zz * n, n), n), slice(None))


def tokens_by_col(n):
    return lambda zz, cc: (pl.ds(pl.multiple_of(cc * n, n), n), slice(None))


def whole_plane(n, w):
    return lambda zz, cc: (
        pl.ds(pl.multiple_of(cc * n, n), n),
        pl.ds(pl.multiple_of(zz * w, w), w),
    )


def gather(x, use_z, use_c, stat=None):
    n, w = x.shape
    if use_z and use_c:
        place, shape = whole_plane(n, w), (n * COLS, w * ROWS)
    elif use_z:
        place, shape = tokens_by_row(n), (n * ROWS, w)
    else:
        place, shape = tokens_by_col(n), (n * COLS, w)
    with_stat = stat is not None
    args, outs = [x], [jax.ShapeDtypeStruct(shape, x.dtype)]
    scratch = [DMA((ROWS,))] * 5 + [DMA((2 * ROWS,))] * 2
    kinds = ({"line"} if use_z else set()) | ({"col"} if use_c else set())
    if with_stat:
        args.append(stat)
        outs.append(jax.ShapeDtypeStruct((ROWS * COLS,) + stat.shape, stat.dtype))
        scratch += [DMA((ROWS * COLS,))] * 2
        kinds.add("plane")

    def steps(here, ins, outs, sems):
        z, c = here.z, here.c
        x_ref, o_ref = ins[0], outs[0]
        up_send, down_send, z_recv, y_send, y_recv, c_send, c_recv = sems[:7]

        def slot(zz, cc):
            return o_ref.at[place(zz, cc)]

        def to_up(src, zz, d):
            return remote(src, slot(zz, c), up_send.at[d], z_recv.at[zz], here.up)

        def to_down(src, zz, d):
            return remote(src, slot(zz, c), down_send.at[d], z_recv.at[zz], here.down)

        def to_y(src, zz):
            return remote(src, slot(zz, c), y_send.at[zz], y_recv.at[zz], here.over_y)

        def to_core(src, zz, cc, half):
            k = half * ROWS + zz
            return remote(src, slot(zz, cc), c_send.at[k], c_recv.at[k], here.over_core)

        def arrived(zz, cc, sem):
            remote(slot(zz, cc), slot(zz, cc), y_send.at[0], sem, here.over_y).wait_recv()

        top, low = z < ROWS - 1, z > 0
        if use_z:
            pl.when(top)(lambda: to_up(x_ref, z, 0).start())
            pl.when(low)(lambda: to_down(x_ref, z, 0).start())
        if use_c:
            to_y(x_ref, z).start()
            to_core(x_ref, z, c, 0).start()
        if with_stat:
            st_ref, so_ref = ins[1], outs[1]
            s_send, s_recv = sems[7:]
            me = z * COLS + c
            for k, zz, cc in here.peers():
                remote(
                    st_ref, so_ref.at[me], s_send.at[k], s_recv.at[me], (here.dp, zz, cc)
                ).start()
            so_ref[me] = st_ref[...]
        mine = place(z, c)

        def keep(r, step):
            o_ref[at(mine, r, step)] = x_ref[pl.ds(r, step), :]

        chunked(n, keep)
        yield

        def from_y(zz):
            arrived(zz, here.c_y, y_recv.at[zz])
            to_core(slot(zz, here.c_y), zz, here.c_y, 1).start()

        if use_z:
            for d in range(1, ROWS):
                below, above = z - d, z + d

                def step_below(below=below, d=d):
                    arrived(below, c, z_recv.at[below])
                    pl.when(top)(lambda: to_up(slot(below, c), below, d).start())
                    if use_c:
                        to_y(slot(below, c), below).start()
                        to_core(slot(below, c), below, c, 0).start()

                def step_above(above=above, d=d):
                    arrived(above, c, z_recv.at[above])
                    pl.when(low)(lambda: to_down(slot(above, c), above, d).start())
                    if use_c:
                        to_y(slot(above, c), above).start()
                        to_core(slot(above, c), above, c, 0).start()

                pl.when(below >= 0)(step_below)
                pl.when(above < ROWS)(step_above)
                yield
                if use_c:
                    if d == 1:
                        from_y(z)
                    else:
                        pl.when(z - (d - 1) >= 0)(lambda d=d: from_y(z - (d - 1)))
                        pl.when(z + (d - 1) < ROWS)(lambda d=d: from_y(z + (d - 1)))
                    yield
            if use_c:
                pl.when(z - (ROWS - 1) >= 0)(lambda: from_y(z - (ROWS - 1)))
                pl.when(z + (ROWS - 1) < ROWS)(lambda: from_y(z + (ROWS - 1)))
                yield
        else:
            from_y(z)
            yield

        if use_z:
            pl.when(top)(lambda: to_up(x_ref, z, 0).wait_send())
            pl.when(low)(lambda: to_down(x_ref, z, 0).wait_send())
            for d in range(1, ROWS):
                below, above = z - d, z + d
                pl.when((below >= 0) & top)(
                    lambda below=below, d=d: to_up(slot(below, c), below, d).wait_send()
                )
                pl.when((above < ROWS) & low)(
                    lambda above=above, d=d: to_down(slot(above, c), above, d).wait_send()
                )
        if use_c:
            for d in range(ROWS if use_z else 1):
                zz = (z + d) % ROWS
                to_y(slot(zz, c), zz).wait_send()
                to_core(slot(zz, c), zz, c, 0).wait_send()
                to_core(slot(zz, here.c_y), zz, here.c_y, 1).wait_send()
                arrived(zz, here.c_core, c_recv.at[zz])
                arrived(zz, (here.c_core + 2) % COLS, c_recv.at[ROWS + zz])
        if with_stat:
            for k, zz, cc in here.peers():
                source = zz * COLS + cc
                copy = remote(
                    st_ref, so_ref.at[source], s_send.at[k], s_recv.at[source], (here.dp, zz, cc)
                )
                copy.wait_send()
                copy.wait_recv()

    return Part(args, outs, scratch, kinds, steps)


def row_stats(here):
    sends = [(0, here.z, None, here.z, True)]
    sends += [(d, here.z, here.row(zz), zz, None) for d, zz, _ in here.others()]
    return sends, [(zz, None) for _, zz, _ in here.others()]


def plane_stats(here):
    me = here.z * COLS + here.c
    sends = [(0, me, None, here.c, True)]
    sends += [(k, me, (here.dp, zz, cc), cc, None) for k, zz, cc in here.peers()]
    return sends, [(zz * COLS + cc, None) for _, zz, cc in here.peers()]


def owner_stats(here):
    own = here.c == here.z
    sends = [(0, here.c, (here.dp, here.z, here.z), 0, own)]
    sends += [(d, here.c, (here.dp, zz, here.z), 0, None) for d, zz, _ in here.others()]
    receives = [(here.c, own)] + [((here.c + d) % COLS, None) for d in range(1, COLS)]
    return sends, receives


def send_stats(stat, stat_to):
    count = ROWS * COLS if stat_to is plane_stats else ROWS
    outs = [jax.ShapeDtypeStruct((count,) + stat.shape[1:], stat.dtype)]

    def steps(here, ins, outs, sems):
        (st_ref,), (so_ref,), (s_send, s_recv) = ins, outs, sems
        sends, receives = stat_to(here)

        def copy(k, slot, device, block):
            return remote(
                st_ref.at[block], so_ref.at[slot], s_send.at[k], s_recv.at[slot], device
            )

        for k, slot, device, block, own in sends:

            def keep(block=block, slot=slot):
                so_ref[slot] = st_ref[block]

            def go(k=k, slot=slot, device=device, block=block):
                copy(k, slot, device, block).start()

            if own is None:
                go()
            elif own is True:
                keep()
            else:
                pl.when(own)(keep)
                pl.when(jnp.logical_not(own))(go)
        yield
        for k, slot, device, block, own in sends:
            if own is not True:
                done = functools.partial(copy, k, slot, device, block)
                if own is None:
                    done().wait_send()
                else:
                    pl.when(jnp.logical_not(own))(lambda done=done: done().wait_send())
        for slot, own in receives:
            got = functools.partial(copy, 0, slot, here.over_core, 0)
            if own is None:
                got().wait_recv()
            else:
                pl.when(jnp.logical_not(own))(lambda got=got: got().wait_recv())

    kinds = {"rows"} if stat_to is row_stats else {"plane"}
    return Part([stat], outs, [DMA((count,))] * 2, kinds, steps)


def scatter_sum(p, use_z, use_c, dtype=F32):
    rows, cols = p.shape
    if use_z and use_c:
        n, w = rows // COLS, cols // ROWS
        place = whole_plane(n, w)
    elif use_z:
        n, w = rows // ROWS, cols
        place = tokens_by_row(n)
    else:
        n, w = rows // COLS, cols
        place = tokens_by_col(n)
    blocks = ROWS if use_z else 1
    scratch = []
    if use_c:
        scratch += [VMEM((2 * blocks, n, w), BF16), VMEM((blocks, n, w), BF16)]
        scratch += [VMEM((blocks, n, w), BF16)]
        scratch += [DMA((2 * blocks,))] * 2 + [DMA((blocks,))] * 2
    if use_z:
        scratch += [VMEM((ROWS - 1, n, w), BF16)] + [VMEM((ROWS, n, w), BF16)] * 2
        scratch += [DMA((ROWS,))] * 3
    kinds = ({"line"} if use_z else set()) | ({"col"} if use_c else set())

    def steps(here, ins, outs, refs):
        z, c = here.z, here.c
        (p_ref,), (o_ref,) = ins, outs
        if use_c:
            c_buf, t_buf, y_buf, c_send, c_recv, y_send, y_recv, *refs = refs
        if use_z:
            z_out, z_up, z_down, z_send, up_recv, down_recv = refs
        mirrored = z // 2

        def dest(i):
            if not use_z:
                return z
            ends, middle = (3, 2, 1, 0)[i], (3, 0, 2, 1)[i]
            g = ends + here.inner * (middle - ends)
            return g + mirrored * (3 - 2 * g)

        def core_copy(j, i):
            other = here.c_core
            cc = (other + 2) % COLS if j == 0 else other
            k = j * blocks + i
            return remote(
                p_ref.at[place(dest(i), cc)],
                c_buf.at[k],
                c_send.at[k],
                c_recv.at[k],
                here.over_core,
            )

        def y_copy(i):
            return remote(t_buf.at[i], y_buf.at[i], y_send.at[i], y_recv.at[i], here.over_y)

        if use_c:
            for i in range(blocks):
                core_copy(0, i).start()
            yield
            for i in range(blocks):
                core_copy(0, i).wait_recv()
                far = place(dest(i), here.c_y)

                def add_core(r, step, i=i, far=far):
                    s = pl.ds(r, step)
                    t_buf[i, s, :] = (
                        p_ref[at(far, r, step)].astype(F32) + c_buf[i, s, :].astype(F32)
                    ).astype(BF16)

                chunked(n, add_core)
                y_copy(i).start()
            yield
            for i in range(blocks):
                core_copy(1, i).start()
            yield

        def up_copy(i, zz):
            return remote(z_out.at[i], z_up.at[zz], z_send.at[i], up_recv.at[zz], here.up)

        def down_copy(i, zz):
            return remote(z_out.at[i], z_down.at[zz], z_send.at[i], down_recv.at[zz], here.down)

        for i in range(blocks):
            zz = dest(i)
            near = place(zz, c)
            if use_c:
                core_copy(1, i).wait_recv()
                y_copy(i).wait_recv()

            def local(r, step, i=i, near=near):
                total = p_ref[at(near, r, step)].astype(F32)
                if use_c:
                    s = pl.ds(r, step)
                    total = total + c_buf[blocks + i, s, :].astype(F32)
                    total = total + y_buf[i, s, :].astype(F32)
                return total

            if not use_z:

                def store(r, step, local=local):
                    o_ref[pl.ds(r, step), :] = local(r, step).astype(o_ref.dtype)

                chunked(n, store)
            elif i < ROWS - 1:

                def send(copy, buf, first, i=i, zz=zz, local=local):
                    @pl.when(first)
                    def _():
                        def put(r, step):
                            z_out[i, pl.ds(r, step), :] = local(r, step).astype(BF16)

                        chunked(n, put)

                    @pl.when(jnp.logical_not(first))
                    def _():
                        copy(i, zz).wait_recv()

                        def put(r, step):
                            s = pl.ds(r, step)
                            z_out[i, s, :] = (
                                local(r, step) + buf[zz, s, :].astype(F32)
                            ).astype(BF16)

                        chunked(n, put)

                    copy(i, zz).start()

                pl.when(zz > z)(functools.partial(send, up_copy, z_up, z == 0))
                pl.when(zz < z)(functools.partial(send, down_copy, z_down, z == ROWS - 1))
            else:

                def final(bufs, local=local):
                    def put(r, step):
                        s = pl.ds(r, step)
                        total = local(r, step)
                        for buf in bufs:
                            total = total + buf[z, s, :].astype(F32)
                        o_ref[s, :] = total.astype(o_ref.dtype)

                    chunked(n, put)

                pl.when(z > 0)(lambda: up_copy(0, z).wait_recv())
                pl.when(z < ROWS - 1)(lambda: down_copy(0, z).wait_recv())
                pl.when(z == 0)(lambda: final([z_down]))
                pl.when(z == ROWS - 1)(lambda: final([z_up]))
                pl.when(here.inner == 1)(lambda: final([z_up, z_down]))
            yield

        if use_c:
            for i in range(blocks):
                core_copy(0, i).wait_send()
                core_copy(1, i).wait_send()
                y_copy(i).wait_send()
        if use_z:
            for i in range(ROWS - 1):
                up_copy(i, 0).wait_send()

    return Part([p], [jax.ShapeDtypeStruct((n, w), dtype)], scratch, kinds, steps)


def pull_weights(weights, axes, dp):
    outs, shapes = [], []
    for w, axis in zip(weights, axes):
        shape = list(w.shape)
        shape[axis] //= ROWS
        shape[1 - axis] *= ROWS
        outs.append(jax.ShapeDtypeStruct(tuple(shape), w.dtype))
        shapes.append((w.shape[0] // (ROWS if axis == 0 else 1), w.shape[1] // (ROWS if axis else 1)))
    count = len(weights)
    shared = dp == 2
    kinds = {"rows"} | ({"dp"} if shared else set())

    def steps(here, ins, outs, sems):
        send, recv, dp_send, dp_recv = sems

        def source(m, zz, half):
            n, w = shapes[m]
            first = zz * n if axes[m] == 0 else 0
            rows = n // 2 if half else n
            first = first + here.dp * rows if half else first
            cols = slice(None) if axes[m] == 0 else pl.ds(pl.multiple_of(zz * w, w), w)
            return pl.ds(pl.multiple_of(first, rows), rows), cols

        def target(m, zz, half):
            n, w = shapes[m]
            first = zz * n if axes[m] == 1 else 0
            rows = n // 2 if half else n
            first = first + here.dp * rows if half else first
            cols = slice(None) if axes[m] == 1 else pl.ds(pl.multiple_of(zz * w, w), w)
            return pl.ds(pl.multiple_of(first, rows), rows), cols

        def copy(m, zz, landing):
            return remote(
                ins[m].at[source(m, zz, shared)],
                outs[m].at[target(m, landing, shared)],
                send.at[m * ROWS + zz],
                recv.at[m * ROWS + landing],
                here.row(zz),
            )

        def pass_on(m, zz):
            k = m * ROWS + zz
            region = outs[m].at[target(m, zz, True)]
            return remote(region, region, dp_send.at[k], dp_recv.at[k], here.over_dp)

        for m in range(count):
            from_place, to_place = source(m, here.z, False), target(m, here.z, False)

            def keep(r, step, m=m, from_place=from_place, to_place=to_place):
                outs[m][at(to_place, r, step)] = ins[m][at(from_place, r, step)]

            chunked(shapes[m][0], keep)
        yield
        for d in (2, 1, 3):
            for m in range(count):
                copy(m, (here.z + d) % ROWS, here.z).start()
            yield
        for _, _, zz in here.others():
            for m in range(count):
                copy(m, here.z, zz).wait_recv()
                if shared:
                    pass_on(m, zz).start()
            yield
        for m in range(count):
            for _, zz, _ in here.others():
                copy(m, zz, here.z).wait_send()
                if shared:
                    pass_on(m, zz).wait_send()
                    pass_on(m, zz).wait_recv()

    sems = [DMA((count * ROWS,))] * 4
    return Part(list(weights), outs, sems, kinds, steps)


def swap_halves_sum(values, axes):
    outs, scratch = [], []
    for v, axis in zip(values, axes):
        n, w = v.shape
        outs.append(jax.ShapeDtypeStruct((n // 2, w), BF16))
        scratch.append(VMEM((n // 2, w), BF16))
    blocks = [ROWS if axis == 1 else 1 for axis in axes]
    total = sum(blocks)
    scratch += [DMA((total,))] * 2

    def steps(here, ins, outs, refs):
        bufs, send, recv = refs[: len(values)], refs[-2], refs[-1]
        work = []
        k = 0
        for m, v in enumerate(values):
            n = v.shape[0] // blocks[m]
            h = n // 2
            for b in range(blocks[m]):
                theirs = pl.ds(pl.multiple_of(b * n + (1 - here.dp) * h, h), h)
                copy = functools.partial(
                    remote,
                    ins[m].at[theirs],
                    bufs[m].at[pl.ds(b * h, h)],
                    send.at[k],
                    recv.at[k],
                    here.over_dp,
                )
                copy().start()
                work.append((m, b, h, n, copy))
                k += 1
        yield
        for m, b, h, n, copy in work:
            copy().wait_recv()

            def add(r, step, m=m, b=b, h=h, n=n):
                own = pl.ds(pl.multiple_of(b * n + here.dp * h + r, step), step)
                s = pl.ds(pl.multiple_of(b * h + r, step), step)
                outs[m][s, :] = (
                    ins[m][own, :].astype(F32) + bufs[m][s, :].astype(F32)
                ).astype(BF16)

            chunked(h, add)
        yield
        for m, b, h, n, copy in work:
            copy().wait_send()

    return Part(list(values), outs, scratch, {"dp"}, steps)


def push_gradients(values, axes, dp):
    shared = dp == 2
    halves = 2 if shared else 1
    outs, shapes = [], []
    for v, axis in zip(values, axes):
        n, w = v.shape
        if axis == 1:
            n = n // ROWS
            outs.append(jax.ShapeDtypeStruct((halves, n, w * ROWS), v.dtype))
        else:
            w = w // ROWS
            outs.append(jax.ShapeDtypeStruct((ROWS, halves, n, w), v.dtype))
        shapes.append((n, w))
    count = len(values)
    kinds = {"rows"} | ({"dp"} if shared else set())

    def steps(here, ins, outs, sems):
        send, recv, dp_send, dp_recv = sems
        half = here.dp if shared else 0

        def block(m, zz):
            n, w = shapes[m]
            if axes[m] == 1:
                return ins[m].at[pl.ds(pl.multiple_of(zz * n, n), n)]
            return ins[m].at[:, pl.ds(pl.multiple_of(zz * w, w), w)]

        def slot(m, zz):
            n, w = shapes[m]
            if axes[m] == 1:
                return outs[m].at[half, :, pl.ds(pl.multiple_of(zz * w, w), w)]
            return outs[m].at[zz, half]

        def copy(m, zz, landing):
            return remote(
                block(m, zz),
                slot(m, landing),
                send.at[m * ROWS + zz],
                recv.at[m * ROWS + landing],
                here.row(zz),
            )

        def pass_on(m, zz):
            k = m * ROWS + zz
            return remote(slot(m, zz), slot(m, zz), dp_send.at[k], dp_recv.at[k], here.over_dp)

        for m in range(count):
            for _, zz, _ in here.others():
                copy(m, zz, here.z).start()
        for m in range(count):

            def keep(r, step, m=m):
                s = pl.ds(r, step)
                slot(m, here.z)[s, :] = block(m, here.z)[s, :]

            chunked(shapes[m][0], keep)
            if shared:
                pass_on(m, here.z).start()
        yield
        for m in range(count):
            for d in (1, 3, 2):
                zz = (here.z - d + ROWS) % ROWS
                copy(m, here.z, zz).wait_recv()
                if shared:
                    pass_on(m, zz).start()
        yield
        for m in range(count):
            for _, zz, _ in here.others():
                copy(m, zz, here.z).wait_send()
            if shared:
                for zz in range(ROWS):
                    pass_on(m, zz).wait_send()
                    remote(
                        slot(m, zz), slot(m, zz), dp_send.at[0], dp_recv.at[m * ROWS + zz], here.over_dp
                    ).wait_recv()

    sems = [DMA((count * ROWS,))] * 4
    return Part(list(values), outs, sems, kinds, steps)


def swap(values):
    outs = [jax.ShapeDtypeStruct(v.shape, v.dtype) for v in values]

    def steps(here, ins, outs, sems):
        copies = [
            remote(i, o, sems[0].at[k], sems[1].at[k], here.over_dp)
            for k, (i, o) in enumerate(zip(ins, outs))
        ]
        for copy in copies:
            copy.start()
        yield
        for copy in copies:
            copy.wait()

    return Part(list(values), outs, [DMA((len(values),))] * 2, {"dp"}, steps)


def sum_gains(vector, n_dp):
    shape = vector.shape

    def steps(here, ins, outs, refs):
        (v_ref,), (o_ref,) = ins, outs
        buf, part, groups, send, recv, dp_send, dp_recv = refs
        me = here.z * COLS + here.c
        for k, zz, cc in here.peers():
            remote(v_ref, buf.at[me], send.at[k], recv.at[me], (here.dp, zz, cc)).start()
        buf[me] = v_ref[...]
        yield
        for k, zz, cc in here.peers():
            source = zz * COLS + cc
            copy = remote(
                v_ref, buf.at[source], send.at[k], recv.at[source], (here.dp, zz, cc)
            )
            copy.wait_send()
            copy.wait_recv()
        for zz in range(ROWS):
            part[zz] = buf[zz * COLS] + buf[zz * COLS + 1] + buf[zz * COLS + 2] + buf[zz * COLS + 3]
        groups[here.dp] = part[...]
        for d in range(1, n_dp):
            remote(
                part, groups.at[here.dp], dp_send.at[d], dp_recv.at[here.dp], here.group(d)
            ).start()
        yield
        for d in range(1, n_dp):
            source = (here.dp + d) % n_dp
            copy = remote(
                part, groups.at[source], dp_send.at[d], dp_recv.at[source], here.group(d)
            )
            copy.wait_send()
            copy.wait_recv()
        total = groups[0]
        for d in range(1, n_dp):
            total = total + groups[d]
        o_ref[...] = total

    scratch = [
        VMEM((ROWS * COLS,) + shape, F32),
        VMEM((ROWS,) + shape, F32),
        VMEM((n_dp, ROWS) + shape, F32),
        DMA((ROWS * COLS,)),
        DMA((ROWS * COLS,)),
        DMA((n_dp,)),
        DMA((n_dp,)),
    ]
    outs = [jax.ShapeDtypeStruct((ROWS,) + shape, F32)]
    return Part([vector], outs, scratch, {"plane", "dp"}, steps)


class Plan:
    def __init__(self):
        self.specs, self.kinds = [], set()

    def add(self, part):
        first = len(self.specs)
        self.specs += part.scratch
        self.kinds |= part.kinds
        return part, first

    def buffer(self, shape, dtype):
        self.specs.append(VMEM(shape, dtype))
        return len(self.specs) - 1

    def bind(self, here, refs):
        self.here, self.refs = here, refs

    def __getitem__(self, handle):
        return self.refs[handle]

    def start(self, handle, ins, outs):
        part, first = handle
        steps = part.steps(self.here, ins, outs, self.refs[first : first + len(part.scratch)])
        next(steps, None)
        return steps


def advance(steps, count=1):
    for _ in range(count):
        next(steps, None)


def finish(steps):
    for _ in steps:
        pass


def like(shape, dtype):
    return jax.ShapeDtypeStruct(shape, dtype)


def planned(n_dp, call, name, plan, args, outs, body):
    ins, out_list = vars(args), vars(outs)

    def kernel(*refs):
        here = Here(n_dp)
        i = SimpleNamespace(**dict(zip(ins, refs)))
        o = SimpleNamespace(**dict(zip(out_list, refs[len(ins) :])))
        plan.bind(here, refs[len(ins) + len(out_list) :])
        meet(here, plan.kinds)
        body(i, o)

    vmem = pl.BlockSpec(memory_space=VMEM)
    results = pl.pallas_call(
        kernel,
        out_shape=list(out_list.values()),
        in_specs=[vmem] * len(ins),
        out_specs=[vmem] * len(out_list),
        scratch_shapes=plan.specs,
        compiler_params=pltpu.CompilerParams(
            collective_id=call, has_side_effects=True, vmem_limit_bytes=63 << 20
        ),
        name=name,
    )(*ins.values())
    return SimpleNamespace(**dict(zip(out_list, results)))


def rows_times(o_ref, terms, block=256, first=0, last=None):
    def body(i, _):
        s = pl.ds(pl.multiple_of(i * block, block), block)
        total = None
        for a_ref, columns, b_ref, flipped in terms:
            term = dot(a_ref[s, columns], b_ref[...], flipped)
            total = term if total is None else total + term
        o_ref[s, :] = total.astype(o_ref.dtype)
        return 0

    lax.fori_loop(first, last or o_ref.shape[0] // block, body, 0)


def columns_times(o_ref, a_ref, b_ref, height=256, width=512):
    across = b_ref.shape[1] // width

    def body(i, _):
        m = pl.ds(pl.multiple_of(i // across * height, height), height)
        n = pl.ds(pl.multiple_of(i % across * width, width), width)
        o_ref[m, n] = weight_term(a_ref[:, m], b_ref[:, n]).astype(o_ref.dtype)
        return 0

    lax.fori_loop(0, a_ref.shape[1] // height * across, body, 0)


ALL = slice(None)


def swapped(field):
    return pltpu.roll(field, HEAD_SIZE // 2, 1)


def lane_major(column):
    return jnp.transpose(jnp.broadcast_to(column, (column.shape[0], HEAD_SIZE)))[:8]


def token_major(row):
    return jnp.transpose(jnp.broadcast_to(row, (HEAD_SIZE, row.shape[1])))


def head_at(ref, h):
    return ref[:, pl.ds(h * HEAD_SIZE, HEAD_SIZE)]


def make_tables(seg_ref, inverse_ref, sign_ref, o):
    row = seg_ref[...].astype(F32)
    n = row.shape[1]
    column = token_major(row)[:, 0:1]
    query = lax.broadcasted_iota(jnp.int32, (n, n), 0)
    key = lax.broadcasted_iota(jnp.int32, (n, n), 1)
    allowed = (column == row) & (key <= query)
    o.bias[...] = jnp.where(allowed, 0.0, -1e30)
    position = jnp.sum(jnp.where(allowed, 1.0, 0.0), axis=-1, keepdims=True) - 1.0
    angle = position * inverse_ref[...]
    o.cosine[...] = jnp.cos(angle)
    o.sine[...] = jnp.sin(angle) * sign_ref[...]


def attention_forward(i, o):
    heads, groups = o.q.shape[1] // HEAD_SIZE, o.k.shape[1] // HEAD_SIZE
    each = heads // groups
    scale = HEAD_SIZE ** (-0.5)
    lane = lax.broadcasted_iota(jnp.int32, o.lse.shape, 1)

    def turned(at_head, gain_ref):
        raw = head_at(o.joint, at_head)
        norm = lax.rsqrt(jnp.mean(raw * raw, axis=-1, keepdims=True) + EPSILON)
        field = raw * norm * gain_ref[...]
        return (field * o.cosine[...] + swapped(field) * o.sine[...]).astype(BF16)

    for g in range(groups):
        at_head = pl.ds(g * HEAD_SIZE, HEAD_SIZE)
        o.k[:, at_head] = turned(heads + g, i.key_gain)
        o.v[:, at_head] = head_at(o.joint, heads + groups + g).astype(BF16)
        for h in range(g * each, (g + 1) * each):
            query = turned(h, i.query_gain)
            o.q[:, pl.ds(h * HEAD_SIZE, HEAD_SIZE)] = query
            scores = dot(query, o.k[:, at_head], True) * scale + o.bias[...]
            top = jnp.max(scores, axis=-1, keepdims=True)
            weights = jnp.exp(scores - top)
            total = jnp.sum(weights, axis=-1, keepdims=True)
            probs = (weights / total).astype(BF16)
            o.mixed[:, pl.ds(h * HEAD_SIZE, HEAD_SIZE)] = dot(probs, o.v[:, at_head]).astype(BF16)
            log_total = jnp.broadcast_to(top + jnp.log(total), o.lse.shape)
            if h == 0:
                o.lse[...] = log_total
            else:
                o.lse[...] = jnp.where(lane == h, log_total, o.lse[...])
            yield


def forward(n_dp, call, a):
    length, feats = a.layer_input.shape
    query_width, key_width = a.w_query.shape[1], a.key_matrix.shape[1]
    wide = query_width + 2 * key_width
    tokens = length * COLS
    units = a.w_gate.shape[1] // ROWS
    plan = Plan()
    in_gather = plan.add(gather(a.layer_input, False, True))
    joint_sum = plan.add(scatter_sum(like((tokens, wide), BF16), True, False))
    in_stat = plan.add(send_stats(like((ROWS, 8, length), F32), row_stats))
    cot_gather = plan.add(gather(a.cotangent, True, True))
    mix_gather = plan.add(gather(like((length, query_width), BF16), True, False))
    out_sum = plan.add(scatter_sum(like((tokens, feats), BF16), False, True))
    mid_gather = plan.add(gather(like((length, feats), BF16), True, True, like((8, length), F32)))
    pulls = [
        pull_weights([a.w_down], [0], n_dp),
        pull_weights([a.w_gate], [1], n_dp),
        pull_weights([a.w_up], [1], n_dp),
    ]
    pull_low, pull_gate, pull_up = [plan.add(p) for p in pulls]
    in_rows = plan.buffer((tokens, feats), BF16)
    stats = plan.buffer((ROWS, 8, length), F32)
    got_stats = plan.buffer((ROWS, 8, length), F32)
    mid_stats = plan.buffer((ROWS * COLS, 8, length), F32)
    own_stat = plan.buffer((8, length), F32)
    p_joint = plan.buffer((tokens, wide), BF16)
    p_out = plan.buffer((tokens, feats), BF16)
    attn_out = plan.buffer((length, feats), F32)
    gained = plan.buffer((length, feats), BF16)
    outs = SimpleNamespace(
        in_gained=like((tokens, feats), BF16),
        joint=like((length, wide), F32),
        scale_in=like((length, HEAD_SIZE), F32),
        bias=like((length, length), F32),
        cosine=like((length, HEAD_SIZE), F32),
        sine=like((length, HEAD_SIZE), F32),
        q=like((length, query_width), BF16),
        k=like((length, key_width), BF16),
        v=like((length, key_width), BF16),
        mixed=like((length, query_width), BF16),
        lse=like((length, HEAD_SIZE), F32),
        mix_rows=like((tokens, query_width), BF16),
        hidden=like((length, feats), F32),
        mid_rows=like((tokens, MODEL_WIDTH), BF16),
        scale_mid=like((tokens, HEAD_SIZE), F32),
        cot_rows=like((tokens, MODEL_WIDTH), BF16),
        w_low=pulls[0].outs[0],
        w_gate_all=pulls[1].outs[0],
        w_up_all=pulls[2].outs[0],
        grad_active=like((tokens, units), F32),
    )

    def body(i, o):
        first = plan.start(in_gather, [i.layer_input], [plan[in_rows]])
        low = plan.start(pull_low, [i.w_down], [o.w_low])
        advance(low, 3)
        make_tables(i.segment, i.inverse, i.sign, o)
        finish(first)
        cot = plan.start(cot_gather, [i.cotangent], [o.cot_rows])

        def normed(b, _):
            s = pl.ds(pl.multiple_of(b * length, length), length)
            field = plan[in_rows][s, :].astype(F32)
            o.in_gained[s, :] = (field * i.attn_gain[...]).astype(BF16)
            plan[stats][b] = lane_major(jnp.sum(field * field, axis=-1, keepdims=True))
            for columns, w_ref in (
                (pl.ds(0, query_width), i.w_query),
                (pl.ds(query_width, key_width), i.key_matrix),
                (pl.ds(query_width + key_width, key_width), i.value_matrix),
            ):
                plan[p_joint][s, columns] = dot(o.in_gained[s, :], w_ref[...]).astype(BF16)
            return 0

        lax.fori_loop(0, COLS, normed, 0)
        total = plan.start(joint_sum, [plan[p_joint]], [o.joint])
        stat = plan.start(in_stat, [plan[stats]], [plan[got_stats]])
        advance(low, 3)
        advance(cot)
        advance(total)
        advance(cot, 2)
        advance(total)
        advance(cot, 2)
        finish(total)
        advance(cot)
        finish(stat)
        summed = plan[got_stats][0] + plan[got_stats][1] + plan[got_stats][2] + plan[got_stats][3]
        o.scale_in[...] = lax.rsqrt(token_major(summed[0:1]) / MODEL_WIDTH + EPSILON)

        def scaled(r, step):
            s = pl.ds(r, step)
            o.joint[s, :] = o.joint[s, :] * o.scale_in[s, 0:1]

        chunked(length, scaled)
        for _ in attention_forward(i, o):
            pass
        mix = plan.start(mix_gather, [o.mixed], [o.mix_rows])
        advance(mix, 2)
        gate = plan.start(pull_gate, [i.w_gate], [o.w_gate_all])
        advance(gate, 3)
        finish(mix)
        finish(cot)
        finish(low)
        rows_times(plan[p_out], [(o.mix_rows, ALL, i.w_output, False)])
        out = plan.start(out_sum, [plan[p_out]], [plan[attn_out]])
        advance(out, 2)
        finish(out)

        def add(r, step):
            s = pl.ds(r, step)
            field = i.layer_input[s, :].astype(F32) + plan[attn_out][s, :]
            o.hidden[s, :] = field
            plan[gained][s, :] = (field * i.mlp_gain[...]).astype(BF16)

        chunked(length, add)
        plan[own_stat][...] = lane_major(
            jnp.sum(o.hidden[...] * o.hidden[...], axis=-1, keepdims=True)
        )
        mid = plan.start(
            mid_gather, [plan[gained], plan[own_stat]], [o.mid_rows, plan[mid_stats]]
        )
        advance(mid, 2)
        advance(gate, 3)
        advance(mid)
        up = plan.start(pull_up, [i.w_up], [o.w_up_all])
        advance(up, 3)
        for k in range(4):
            rows_times(o.grad_active, [(o.cot_rows, ALL, o.w_low, True)], first=k, last=k + 1)
            advance(mid)
        advance(up, 3)
        finish(mid)
        for b in range(COLS):
            summed = plan[mid_stats][b]
            for zz in range(1, ROWS):
                summed = summed + plan[mid_stats][zz * COLS + b]
            o.scale_mid[pl.ds(b * length, length), :] = lax.rsqrt(
                token_major(summed[0:1]) / MODEL_WIDTH + EPSILON
            )
        finish(gate)
        finish(up)

    return planned(n_dp, call, "forward", plan, a, outs, body)


def middle(n_dp, call, a):
    two = n_dp == 2
    length, feats = a.hidden.shape
    tokens, units = a.grad_active.shape
    plan = Plan()
    mid_sum = plan.add(scatter_sum(like((tokens, MODEL_WIDTH), BF16), True, True))
    inner_stat = plan.add(send_stats(like((COLS, 8, length), F32), plane_stats))
    d_low = like((units, MODEL_WIDTH), BF16)
    if two:
        low_half = plan.add(swap_halves_sum([d_low], [0]))
        low = plan.buffer(d_low.shape, BF16)
        d_low = like((units // 2, MODEL_WIDTH), BF16)
    p_mid = plan.buffer((tokens, MODEL_WIDTH), BF16)
    d_gate = plan.buffer((tokens, units), BF16)
    d_up = plan.buffer((tokens, units), BF16)
    inner = plan.buffer((COLS, 8, length), F32)
    inners = plan.buffer((ROWS * COLS, 8, length), F32)
    grad_mid = plan.buffer((length, feats), F32)
    outs = SimpleNamespace(
        grad_hidden=like((length, feats), F32),
        grad_attn=like((length, feats), BF16),
        gain_mid=like((16, HEAD_SIZE), F32),
        active=like((tokens, units), BF16),
        grad_low=d_low,
        grad_gate=like((MODEL_WIDTH, units), BF16),
        grad_up=like((MODEL_WIDTH, units), BF16),
    )

    def body(i, o):
        here = plan.here

        def tokens_of(b):
            s = pl.ds(pl.multiple_of(b * length, length), length)
            scale = i.scale_mid[s, 0:1]
            gate = dot(i.mid_rows[s, :], i.w_gate_all[...]) * scale
            upward = dot(i.mid_rows[s, :], i.w_up_all[...]) * scale
            silu, slope = silu_parts(gate)
            o.active[s, :] = (silu * upward).astype(BF16)
            grad = i.grad_active[s, :] * scale
            grad_gate = (grad * upward * slope).astype(BF16)
            grad_up = (grad * silu).astype(BF16)
            plan[d_gate][s, :] = grad_gate
            plan[d_up][s, :] = grad_up
            term = grad_gate.astype(F32) * gate + grad_up.astype(F32) * upward
            plan[inner][b] = lane_major(jnp.sum(term, axis=-1, keepdims=True) * scale)
            for k in range(ROWS):
                part = pl.ds(k * feats, feats)
                plan[p_mid][s, part] = (
                    dot(grad_gate, i.w_gate_all[part, :], True)
                    + dot(grad_up, i.w_up_all[part, :], True)
                ).astype(BF16)

        tokens_of((here.c_core + 2) % COLS)
        total = plan.start(mid_sum, [plan[p_mid]], [plan[grad_mid]])
        tokens_of(here.c_y)
        advance(total)
        tokens_of(here.c_core)
        advance(total)
        tokens_of(here.c)
        stat = plan.start(inner_stat, [plan[inner]], [plan[inners]])
        advance(total)
        low_ref = plan[low] if two else o.grad_low
        columns_times(low_ref, o.active, i.cot_rows, units)
        if two:
            low_sum = plan.start(low_half, [low_ref], [o.grad_low])
        advance(total)
        columns_times(o.grad_gate, i.mid_rows, plan[d_gate], width=units)
        advance(total)
        columns_times(o.grad_up, i.mid_rows, plan[d_up], width=units)
        finish(total)
        finish(stat)
        summed = plan[inners][0]
        for k in range(1, ROWS * COLS):
            summed = summed + plan[inners][k]
        coef = token_major(summed[0:1] / MODEL_WIDTH)[:, 0:1]
        grad = plan[grad_mid][...]
        hidden = i.hidden[...]
        total = jnp.sum(grad * hidden, axis=0, keepdims=True)
        o.gain_mid[...] = jnp.zeros((16, HEAD_SIZE), F32)
        for k in range(feats // HEAD_SIZE):
            o.gain_mid[4 + k : 5 + k, :] = total[:, k * HEAD_SIZE : (k + 1) * HEAD_SIZE]
        grad = i.cotangent[...].astype(F32) + grad * i.mlp_gain[...] - hidden * coef
        o.grad_hidden[...] = grad
        o.grad_attn[...] = grad.astype(BF16)
        if two:
            finish(low_sum)

    return planned(n_dp, call, "middle", plan, a, outs, body)


def attention_back(i, grad_mixed, gq_ref, gkv_ref, inner_ref, gains_ref, dk_ref, dv_ref):
    heads, groups = i.q.shape[1] // HEAD_SIZE, i.k.shape[1] // HEAD_SIZE
    each = heads // groups
    scale = HEAD_SIZE ** (-0.5)
    cosine, sine = i.cosine[...], i.sine[...]
    scale_in = i.scale_in[:, 0:1]
    inner = jnp.zeros((i.q.shape[0], HEAD_SIZE), F32)

    def put(at_head, out):
        if at_head < heads:
            gq_ref[:, pl.ds(at_head * HEAD_SIZE, HEAD_SIZE)] = out
        else:
            gkv_ref[:, pl.ds((at_head - heads) * HEAD_SIZE, HEAD_SIZE)] = out

    def norm_back(grad_rot, at_head, gain):
        grad = grad_rot * cosine - swapped(grad_rot) * sine
        raw = head_at(i.joint, at_head)
        norm = lax.rsqrt(jnp.mean(raw * raw, axis=-1, keepdims=True) + EPSILON)
        unit = raw * norm
        u = grad * gain
        back = norm * (u - unit * jnp.mean(u * unit, axis=-1, keepdims=True))
        out = (back * scale_in).astype(BF16)
        put(at_head, out)
        return out.astype(F32) * raw, jnp.sum(grad * unit, axis=0, keepdims=True)

    gain_q = jnp.zeros((1, HEAD_SIZE), F32)
    gain_k = jnp.zeros((1, HEAD_SIZE), F32)
    for g in range(groups):
        key, value = head_at(i.k, g), head_at(i.v, g)
        for r in range(each):
            h = g * each + r
            query, grad = head_at(i.q, h), head_at(grad_mixed, h)
            scores = dot(query, key, True) * scale + i.bias[...]
            probs = jnp.exp(scores - i.lse[:, h : h + 1])
            term_v = weight_term(probs.astype(BF16), grad)
            delta = jnp.sum(
                grad.astype(F32) * head_at(i.mixed, h).astype(F32), axis=-1, keepdims=True
            )
            grad_scores = (probs * (dot(grad, value, True) - delta)).astype(BF16)
            term_k = weight_term(grad_scores, query) * scale
            if r == 0:
                dv_ref[...] = term_v
                dk_ref[...] = term_k
            else:
                dv_ref[...] += term_v
                dk_ref[...] += term_k
            term, gain = norm_back(dot(grad_scores, key) * scale, h, i.query_gain[...])
            inner = inner + term
            gain_q = gain_q + gain
        term, gain = norm_back(dk_ref[...], heads + g, i.key_gain[...])
        inner = inner + term
        gain_k = gain_k + gain
        at_head = heads + groups + g
        out = (dv_ref[...] * scale_in).astype(BF16)
        put(at_head, out)
        inner = inner + out.astype(F32) * head_at(i.joint, at_head)
    gains_ref[8:9, :] = gain_q
    gains_ref[9:10, :] = gain_k
    inner_ref[0] = lane_major(jnp.sum(inner, axis=-1, keepdims=True) * scale_in)


def backward(n_dp, call, a):
    two = n_dp == 2
    length, feats = a.grad_attn.shape
    query_width, key_width = a.w_query.shape[1], a.key_matrix.shape[1]
    tokens = length * COLS
    plan = Plan()
    attn_gather = plan.add(gather(a.grad_attn, False, True))
    mixed_sum = plan.add(scatter_sum(like((tokens, feats), BF16), True, False, BF16))
    q_gather = plan.add(gather(like((length, query_width), BF16), True, False))
    kv_gather = plan.add(gather(like((length, 2 * key_width), BF16), True, False))
    in_sum = plan.add(scatter_sum(like((tokens, feats), BF16), False, True))
    in_stat = plan.add(send_stats(like((1, 8, length), F32), owner_stats))
    block_sum = plan.add(scatter_sum(like((tokens, MODEL_WIDTH), BF16), True, True))
    n, w = a.grad_gate.shape
    half = like((n // 2 if two else n, w), BF16)
    if two:
        gate_half = plan.add(swap_halves_sum([a.grad_gate], [1]))
        up_half = plan.add(swap_halves_sum([a.grad_up], [1]))
        gate_sum = plan.buffer(half.shape, BF16)
        up_sum = plan.buffer(half.shape, BF16)
    pushes = [
        push_gradients([half], [1], n_dp),
        push_gradients([half], [1], n_dp),
        push_gradients([a.grad_low], [0], n_dp),
    ]
    gate_push, up_push, low_push = [plan.add(p) for p in pushes]
    gain_sum = plan.add(sum_gains(like((16, HEAD_SIZE), F32), n_dp))
    d_output, d_q = like((feats, feats), BF16), like((feats, query_width), BF16)
    d_kv = like((feats, 2 * key_width), BF16)
    if two:
        output_swap = plan.add(swap([d_output]))
        q_swap = plan.add(swap([d_q]))
        kv_swap = plan.add(swap([d_kv]))
    attn_rows = plan.buffer((tokens, feats), BF16)
    p_mixed = plan.buffer((tokens, feats), BF16)
    grad_mixed = plan.buffer((length, feats), BF16)
    q_in = plan.buffer((length, query_width), BF16)
    kv_in = plan.buffer((length, 2 * key_width), BF16)
    q_rows = plan.buffer((tokens, query_width), BF16)
    kv_rows = plan.buffer((tokens, 2 * key_width), BF16)
    p_in = plan.buffer((tokens, feats), BF16)
    p_block = plan.buffer((tokens, MODEL_WIDTH), BF16)
    inner = plan.buffer((1, 8, length), F32)
    gain_rows = plan.buffer((16, HEAD_SIZE), F32)
    dk, dv = [plan.buffer((length, HEAD_SIZE), F32) for _ in range(2)]
    outs = SimpleNamespace(
        grad_in=like((length, feats), F32),
        in_inners=like((COLS, 8, length), F32),
        block=like((length, feats), F32),
        grad_gate=pushes[0].outs[0],
        grad_up=pushes[1].outs[0],
        grad_low=pushes[2].outs[0],
        gains=like((ROWS, 16, HEAD_SIZE), F32),
        d_output=d_output,
        d_q=d_q,
        d_kv=d_kv,
    )
    if two:
        outs.d_output_other, outs.d_q_other, outs.d_kv_other = d_output, d_q, d_kv

    def body(i, o):
        attn = plan.start(attn_gather, [i.grad_attn], [plan[attn_rows]])
        low = plan.start(low_push, [i.grad_low], [o.grad_low])
        if two:
            gate_sums = plan.start(gate_half, [i.grad_gate], [plan[gate_sum]])
        rows_times(plan[p_block], [(i.active, ALL, i.w_low, False)], first=0, last=3)
        finish(attn)
        if two:
            up_sums = plan.start(up_half, [i.grad_up], [plan[up_sum]])
        rows_times(plan[p_mixed], [(plan[attn_rows], ALL, i.w_output, True)])
        mixed = plan.start(mixed_sum, [plan[p_mixed]], [plan[grad_mixed]])
        rows_times(plan[p_block], [(i.active, ALL, i.w_low, False)], first=3, last=4)
        block = plan.start(block_sum, [plan[p_block]], [o.block])
        advance(mixed)
        advance(block, 2)
        advance(low)
        if two:
            advance(gate_sums)
        advance(mixed)
        gate = plan.start(gate_push, [plan[gate_sum] if two else i.grad_gate], [o.grad_gate])
        finish(mixed)
        plan[gain_rows][...] = i.gain_mid[...]
        attention_back(
            i,
            plan[grad_mixed],
            plan[q_in],
            plan[kv_in],
            plan[inner],
            plan[gain_rows],
            plan[dk],
            plan[dv],
        )
        kv = plan.start(kv_gather, [plan[kv_in]], [plan[kv_rows]])
        q = plan.start(q_gather, [plan[q_in]], [plan[q_rows]])
        stat = plan.start(in_stat, [plan[inner]], [o.in_inners])
        if two:
            advance(up_sums)
        advance(kv)
        advance(gate)
        columns_times(o.d_output, i.mix_rows, plan[attn_rows])
        if two:
            swap_output = plan.start(output_swap, [o.d_output], [o.d_output_other])
        advance(q)
        advance(kv)
        advance(q)
        finish(kv)
        up = plan.start(up_push, [plan[up_sum] if two else i.grad_up], [o.grad_up])
        columns_times(o.d_kv, i.in_gained, plan[kv_rows])
        if two:
            swap_kv = plan.start(kv_swap, [o.d_kv], [o.d_kv_other])
        finish(q)
        columns_times(o.d_q, i.in_gained, plan[q_rows])
        if two:
            swap_q = plan.start(q_swap, [o.d_q], [o.d_q_other])
        rows_times(
            plan[p_in],
            [
                (plan[q_rows], ALL, i.w_query, True),
                (plan[kv_rows], pl.ds(0, key_width), i.key_matrix, True),
                (plan[kv_rows], pl.ds(key_width, key_width), i.value_matrix, True),
            ],
        )
        grad_in = plan.start(in_sum, [plan[p_in]], [o.grad_in])
        advance(grad_in)
        advance(block)
        advance(up)
        finish(grad_in)
        total = jnp.sum(o.grad_in[...] * i.layer_input[...].astype(F32), axis=0, keepdims=True)
        for k in range(feats // HEAD_SIZE):
            plan[gain_rows][k : k + 1, :] = total[:, k * HEAD_SIZE : (k + 1) * HEAD_SIZE]
        gains = plan.start(gain_sum, [plan[gain_rows]], [o.gains])
        finish(block)
        finish(gains)
        finish(stat)
        finish(low)
        finish(gate)
        finish(up)
        if two:
            finish(gate_sums)
            finish(up_sums)
            finish(swap_output)
            finish(swap_kv)
            finish(swap_q)

    return planned(n_dp, call, "backward", plan, a, outs, body)


def silu_parts(gate):
    sigma = jax.nn.sigmoid(gate)
    return (gate * sigma, sigma * (1.0 + gate * (1.0 - sigma)))


def dot(left, right, flipped=False):
    return lax.dot_general(
        left, right, (((1,), (1 if flipped else 0,)), ((), ())), preferred_element_type=F32
    )


def weight_term(left, right):
    return lax.dot_general(left, right, (((0,), (0,)), ((), ())), preferred_element_type=F32)


def per_device(
    dp,
    layer_input,
    cotangent,
    w_query,
    key_matrix,
    value_matrix,
    w_output,
    w_gate,
    w_up,
    w_down,
    attn_gain,
    mlp_gain,
    query_gain,
    key_gain,
    segment_ids,
):
    length, feats = layer_input.shape
    key_width = key_matrix.shape[1]
    ff_local = w_gate.shape[1]
    two = dp == 2
    half = jnp.arange(HEAD_SIZE // 2, dtype=F32)
    inverse = jnp.power(THETA, -(half * (2.0 / HEAD_SIZE)))
    ones = jnp.ones_like(half)
    f = forward(
        dp,
        0,
        SimpleNamespace(
            layer_input=layer_input,
            cotangent=cotangent,
            w_query=w_query,
            key_matrix=key_matrix,
            value_matrix=value_matrix,
            w_output=w_output,
            w_gate=w_gate,
            w_up=w_up,
            w_down=w_down,
            attn_gain=attn_gain[None],
            mlp_gain=mlp_gain[None],
            query_gain=query_gain[None],
            key_gain=key_gain[None],
            segment=segment_ids,
            inverse=jnp.concatenate([inverse, inverse])[None],
            sign=jnp.concatenate([-ones, ones])[None],
        ),
    )
    m = middle(
        dp,
        1,
        SimpleNamespace(
            mid_rows=f.mid_rows,
            cot_rows=f.cot_rows,
            grad_active=f.grad_active,
            scale_mid=f.scale_mid,
            w_gate_all=f.w_gate_all,
            w_up_all=f.w_up_all,
            hidden=f.hidden,
            cotangent=cotangent,
            mlp_gain=mlp_gain[None],
        ),
    )
    grad_low, grad_gate, grad_up = m.grad_low, m.grad_gate, m.grad_up
    if not two:
        grad_low, grad_gate, grad_up = lax.psum((grad_low, grad_gate, grad_up), "dp")
    b = backward(
        dp,
        2,
        SimpleNamespace(
            grad_attn=m.grad_attn,
            w_output=w_output,
            w_query=w_query,
            key_matrix=key_matrix,
            value_matrix=value_matrix,
            q=f.q,
            k=f.k,
            v=f.v,
            mixed=f.mixed,
            lse=f.lse,
            bias=f.bias,
            cosine=f.cosine,
            sine=f.sine,
            joint=f.joint,
            scale_in=f.scale_in,
            query_gain=query_gain[None],
            key_gain=key_gain[None],
            mix_rows=f.mix_rows,
            in_gained=f.in_gained,
            active=m.active,
            w_low=f.w_low,
            grad_gate=grad_gate,
            grad_up=grad_up,
            grad_low=grad_low,
            gain_mid=m.gain_mid,
            layer_input=layer_input,
        ),
    )
    if two:
        grad_output = b.d_output.astype(F32) + b.d_output_other.astype(F32)
        grad_query = b.d_q.astype(F32) + b.d_q_other.astype(F32)
        grad_kv = b.d_kv.astype(F32) + b.d_kv_other.astype(F32)
    else:
        sums = lax.psum((b.d_output, b.d_q, b.d_kv), "dp")
        grad_output, grad_query, grad_kv = [term.astype(F32) for term in sums]
    in_coef = jnp.sum(b.in_inners[:, 0], axis=0).reshape(length, 1) / MODEL_WIDTH
    input_grad = m.grad_hidden + b.grad_in * attn_gain - layer_input.astype(F32) * in_coef
    return (
        (f.hidden + b.block).astype(BF16),
        input_grad,
        grad_query,
        grad_kv[:, :key_width],
        grad_kv[:, key_width:],
        grad_output,
        b.grad_gate.reshape(feats, ff_local).astype(F32),
        b.grad_up.reshape(feats, ff_local).astype(F32),
        b.grad_low.reshape(ff_local, feats).astype(F32),
        b.gains[:, 0:4].reshape(MODEL_WIDTH),
        b.gains[:, 4:8].reshape(MODEL_WIDTH),
        jnp.sum(b.gains[:, 8], axis=0),
        jnp.sum(b.gains[:, 9], axis=0),
    )


def solution(mesh):
    tokens, weights, flipped = P(("dp", "col"), "row"), P("row", "col"), P("col", "row")
    features, copied = P("row"), P()
    return jax.shard_map(
        functools.partial(per_device, mesh.shape["dp"]),
        mesh=mesh,
        in_specs=(
            (tokens, tokens)
            + (weights,) * 3
            + (flipped, weights, weights, flipped)
            + (features, features, copied, copied, P(("dp", "row"), None))
        ),
        out_specs=(tokens, tokens)
        + (weights,) * 3
        + (flipped, weights, weights, flipped)
        + (copied,) * 4,
        check_vma=False,
    )
```

```python
import functools
from types import SimpleNamespace

import jax
import jax.numpy as jnp
from jax import lax
from jax.experimental import pallas as pl
from jax.experimental.pallas import tpu as pltpu
from jax.sharding import PartitionSpec as P

MODEL_WIDTH = 2048
HEAD_SIZE = 128
EPSILON = 1e-06
THETA = 1000000.0
ROWS = 4
COLS = 4
STEP = 32
MESH = pl.DeviceIdType.MESH
VMEM = pltpu.VMEM
DMA = pltpu.SemaphoreType.DMA
BF16 = jnp.bfloat16
F32 = jnp.float32


def remote(src, dst, send, recv, device):
    return pltpu.make_async_remote_copy(
        src_ref=src,
        dst_ref=dst,
        send_sem=send,
        recv_sem=recv,
        device_id=device,
        device_id_type=MESH,
    )


class Here:
    def __init__(self, n_dp):
        self.n_dp = n_dp
        self.dp = lax.axis_index("dp")
        self.z = lax.axis_index("row")
        self.c = lax.axis_index("col")
        self.core = self.c % 2
        self.c_core = self.c + 1 - 2 * self.core
        self.c_y = (self.c + 2) % COLS
        self.inner = (self.z % 3 + 2) // 3
        self.up = (self.dp, self.z + 1, self.c)
        self.down = (self.dp, self.z - 1, self.c)
        self.over_y = (self.dp, self.z, self.c_y)
        self.over_core = (self.dp, self.z, self.c_core)
        self.over_dp = (1 - self.dp, self.z, self.c)

    def group(self, d):
        return ((self.dp + d) % self.n_dp, self.z, self.c)

    def peers(self):
        for dz in range(ROWS):
            for dc in range(COLS):
                if dz or dc:
                    yield dz * COLS + dc, (self.z + dz) % ROWS, (self.c + dc) % COLS

    def others(self):
        for d in range(1, ROWS):
            yield d, (self.z + d) % ROWS, (self.z - d + ROWS) % ROWS

    def row(self, z):
        return (self.dp, z, self.c)


def meet(here, kinds):
    barrier = pltpu.get_barrier_semaphore()

    def signal(device):
        pl.semaphore_signal(barrier, inc=1, device_id=device, device_id_type=MESH)

    count = 0
    if "dp" in kinds:
        for d in range(1, here.n_dp):
            signal(here.group(d))
        count += here.n_dp - 1
    if "plane" in kinds:
        for _, z, c in here.peers():
            signal((here.dp, z, c))
        count += ROWS * COLS - 1
    else:
        if "col" in kinds:
            signal(here.over_y)
            signal(here.over_core)
            count += 2
        if "rows" in kinds:
            for _, z, _ in here.others():
                signal(here.row(z))
            count += ROWS - 1
        elif "line" in kinds:
            pl.when(here.z < ROWS - 1)(lambda: signal(here.up))
            pl.when(here.z > 0)(lambda: signal(here.down))
            count = count + 1 + here.inner
    pl.semaphore_wait(barrier, count)


class Part:
    def __init__(self, args, outs, scratch, kinds, steps):
        self.args, self.outs, self.scratch = args, outs, scratch
        self.kinds, self.steps = kinds, steps


def chunked(n, fn):
    step = min(STEP, n)

    def body(i, _):
        fn(pl.multiple_of(i * step, step), step)
        return 0

    lax.fori_loop(0, n // step, body, 0)


def at(place, r, step):
    rows, cols = place
    return pl.ds(rows.start + r, step), cols


def tokens_by_row(n):
    return lambda zz, cc: (pl.ds(pl.multiple_of(zz * n, n), n), slice(None))


def tokens_by_col(n):
    return lambda zz, cc: (pl.ds(pl.multiple_of(cc * n, n), n), slice(None))


def whole_plane(n, w):
    return lambda zz, cc: (
        pl.ds(pl.multiple_of(cc * n, n), n),
        pl.ds(pl.multiple_of(zz * w, w), w),
    )


def gather(x, use_z, use_c, stat=None):
    n, w = x.shape
    if use_z and use_c:
        place, shape = whole_plane(n, w), (n * COLS, w * ROWS)
    elif use_z:
        place, shape = tokens_by_row(n), (n * ROWS, w)
    else:
        place, shape = tokens_by_col(n), (n * COLS, w)
    with_stat = stat is not None
    args, outs = [x], [jax.ShapeDtypeStruct(shape, x.dtype)]
    scratch = [DMA((ROWS,))] * 5 + [DMA((2 * ROWS,))] * 2
    kinds = ({"line"} if use_z else set()) | ({"col"} if use_c else set())
    if with_stat:
        args.append(stat)
        outs.append(jax.ShapeDtypeStruct((ROWS * COLS,) + stat.shape, stat.dtype))
        scratch += [DMA((ROWS * COLS,))] * 2
        kinds.add("plane")

    def steps(here, ins, outs, sems):
        z, c = here.z, here.c
        x_ref, o_ref = ins[0], outs[0]
        up_send, down_send, z_recv, y_send, y_recv, c_send, c_recv = sems[:7]

        def slot(zz, cc):
            return o_ref.at[place(zz, cc)]

        def to_up(src, zz, d):
            return remote(src, slot(zz, c), up_send.at[d], z_recv.at[zz], here.up)

        def to_down(src, zz, d):
            return remote(src, slot(zz, c), down_send.at[d], z_recv.at[zz], here.down)

        def to_y(src, zz):
            return remote(src, slot(zz, c), y_send.at[zz], y_recv.at[zz], here.over_y)

        def to_core(src, zz, cc, half):
            k = half * ROWS + zz
            return remote(src, slot(zz, cc), c_send.at[k], c_recv.at[k], here.over_core)

        def arrived(zz, cc, sem):
            remote(slot(zz, cc), slot(zz, cc), y_send.at[0], sem, here.over_y).wait_recv()

        top, low = z < ROWS - 1, z > 0
        if use_z:
            pl.when(top)(lambda: to_up(x_ref, z, 0).start())
            pl.when(low)(lambda: to_down(x_ref, z, 0).start())
        if use_c:
            to_y(x_ref, z).start()
            to_core(x_ref, z, c, 0).start()
        if with_stat:
            st_ref, so_ref = ins[1], outs[1]
            s_send, s_recv = sems[7:]
            me = z * COLS + c
            for k, zz, cc in here.peers():
                remote(
                    st_ref, so_ref.at[me], s_send.at[k], s_recv.at[me], (here.dp, zz, cc)
                ).start()
            so_ref[me] = st_ref[...]
        mine = place(z, c)

        def keep(r, step):
            o_ref[at(mine, r, step)] = x_ref[pl.ds(r, step), :]

        chunked(n, keep)
        yield

        def from_y(zz):
            arrived(zz, here.c_y, y_recv.at[zz])
            to_core(slot(zz, here.c_y), zz, here.c_y, 1).start()

        if use_z:
            for d in range(1, ROWS):
                below, above = z - d, z + d

                def step_below(below=below, d=d):
                    arrived(below, c, z_recv.at[below])
                    pl.when(top)(lambda: to_up(slot(below, c), below, d).start())
                    if use_c:
                        to_y(slot(below, c), below).start()
                        to_core(slot(below, c), below, c, 0).start()

                def step_above(above=above, d=d):
                    arrived(above, c, z_recv.at[above])
                    pl.when(low)(lambda: to_down(slot(above, c), above, d).start())
                    if use_c:
                        to_y(slot(above, c), above).start()
                        to_core(slot(above, c), above, c, 0).start()

                pl.when(below >= 0)(step_below)
                pl.when(above < ROWS)(step_above)
                yield
                if use_c:
                    if d == 1:
                        from_y(z)
                    else:
                        pl.when(z - (d - 1) >= 0)(lambda d=d: from_y(z - (d - 1)))
                        pl.when(z + (d - 1) < ROWS)(lambda d=d: from_y(z + (d - 1)))
                    yield
            if use_c:
                pl.when(z - (ROWS - 1) >= 0)(lambda: from_y(z - (ROWS - 1)))
                pl.when(z + (ROWS - 1) < ROWS)(lambda: from_y(z + (ROWS - 1)))
                yield
        else:
            from_y(z)
            yield

        if use_z:
            pl.when(top)(lambda: to_up(x_ref, z, 0).wait_send())
            pl.when(low)(lambda: to_down(x_ref, z, 0).wait_send())
            for d in range(1, ROWS):
                below, above = z - d, z + d
                pl.when((below >= 0) & top)(
                    lambda below=below, d=d: to_up(slot(below, c), below, d).wait_send()
                )
                pl.when((above < ROWS) & low)(
                    lambda above=above, d=d: to_down(slot(above, c), above, d).wait_send()
                )
        if use_c:
            for d in range(ROWS if use_z else 1):
                zz = (z + d) % ROWS
                to_y(slot(zz, c), zz).wait_send()
                to_core(slot(zz, c), zz, c, 0).wait_send()
                to_core(slot(zz, here.c_y), zz, here.c_y, 1).wait_send()
                arrived(zz, here.c_core, c_recv.at[zz])
                arrived(zz, (here.c_core + 2) % COLS, c_recv.at[ROWS + zz])
        if with_stat:
            for k, zz, cc in here.peers():
                source = zz * COLS + cc
                copy = remote(
                    st_ref, so_ref.at[source], s_send.at[k], s_recv.at[source], (here.dp, zz, cc)
                )
                copy.wait_send()
                copy.wait_recv()

    return Part(args, outs, scratch, kinds, steps)


def row_stats(here):
    sends = [(0, here.z, None, here.z, True)]
    sends += [(d, here.z, here.row(zz), zz, None) for d, zz, _ in here.others()]
    return sends, [(zz, None) for _, zz, _ in here.others()]


def plane_stats(here):
    me = here.z * COLS + here.c
    sends = [(0, me, None, here.c, True)]
    sends += [(k, me, (here.dp, zz, cc), cc, None) for k, zz, cc in here.peers()]
    return sends, [(zz * COLS + cc, None) for _, zz, cc in here.peers()]


def owner_stats(here):
    own = here.c == here.z
    sends = [(0, here.c, (here.dp, here.z, here.z), 0, own)]
    sends += [(d, here.c, (here.dp, zz, here.z), 0, None) for d, zz, _ in here.others()]
    receives = [(here.c, own)] + [((here.c + d) % COLS, None) for d in range(1, COLS)]
    return sends, receives


def send_stats(stat, stat_to):
    count = ROWS * COLS if stat_to is plane_stats else ROWS
    outs = [jax.ShapeDtypeStruct((count,) + stat.shape[1:], stat.dtype)]

    def steps(here, ins, outs, sems):
        (st_ref,), (so_ref,), (s_send, s_recv) = ins, outs, sems
        sends, receives = stat_to(here)

        def copy(k, slot, device, block):
            return remote(
                st_ref.at[block], so_ref.at[slot], s_send.at[k], s_recv.at[slot], device
            )

        for k, slot, device, block, own in sends:

            def keep(block=block, slot=slot):
                so_ref[slot] = st_ref[block]

            def go(k=k, slot=slot, device=device, block=block):
                copy(k, slot, device, block).start()

            if own is None:
                go()
            elif own is True:
                keep()
            else:
                pl.when(own)(keep)
                pl.when(jnp.logical_not(own))(go)
        yield
        for k, slot, device, block, own in sends:
            if own is not True:
                done = functools.partial(copy, k, slot, device, block)
                if own is None:
                    done().wait_send()
                else:
                    pl.when(jnp.logical_not(own))(lambda done=done: done().wait_send())
        for slot, own in receives:
            got = functools.partial(copy, 0, slot, here.over_core, 0)
            if own is None:
                got().wait_recv()
            else:
                pl.when(jnp.logical_not(own))(lambda got=got: got().wait_recv())

    kinds = {"rows"} if stat_to is row_stats else {"plane"}
    return Part([stat], outs, [DMA((count,))] * 2, kinds, steps)


def scatter_sum(p, use_z, use_c, dtype=F32):
    rows, cols = p.shape
    if use_z and use_c:
        n, w = rows // COLS, cols // ROWS
        place = whole_plane(n, w)
    elif use_z:
        n, w = rows // ROWS, cols
        place = tokens_by_row(n)
    else:
        n, w = rows // COLS, cols
        place = tokens_by_col(n)
    blocks = ROWS if use_z else 1
    scratch = []
    if use_c:
        scratch += [VMEM((2 * blocks, n, w), BF16), VMEM((blocks, n, w), BF16)]
        scratch += [VMEM((blocks, n, w), BF16)]
        scratch += [DMA((2 * blocks,))] * 2 + [DMA((blocks,))] * 2
    if use_z:
        scratch += [VMEM((ROWS - 1, n, w), BF16)] + [VMEM((ROWS, n, w), BF16)] * 2
        scratch += [DMA((ROWS,))] * 3
    kinds = ({"line"} if use_z else set()) | ({"col"} if use_c else set())

    def steps(here, ins, outs, refs):
        z, c = here.z, here.c
        (p_ref,), (o_ref,) = ins, outs
        if use_c:
            c_buf, t_buf, y_buf, c_send, c_recv, y_send, y_recv, *refs = refs
        if use_z:
            z_out, z_up, z_down, z_send, up_recv, down_recv = refs
        mirrored = z // 2

        def dest(i):
            if not use_z:
                return z
            ends, middle = (3, 2, 1, 0)[i], (3, 0, 2, 1)[i]
            g = ends + here.inner * (middle - ends)
            return g + mirrored * (3 - 2 * g)

        def core_copy(j, i):
            other = here.c_core
            cc = (other + 2) % COLS if j == 0 else other
            k = j * blocks + i
            return remote(
                p_ref.at[place(dest(i), cc)],
                c_buf.at[k],
                c_send.at[k],
                c_recv.at[k],
                here.over_core,
            )

        def y_copy(i):
            return remote(t_buf.at[i], y_buf.at[i], y_send.at[i], y_recv.at[i], here.over_y)

        if use_c:
            for i in range(blocks):
                core_copy(0, i).start()
            yield
            for i in range(blocks):
                core_copy(0, i).wait_recv()
                far = place(dest(i), here.c_y)

                def add_core(r, step, i=i, far=far):
                    s = pl.ds(r, step)
                    t_buf[i, s, :] = (
                        p_ref[at(far, r, step)].astype(F32) + c_buf[i, s, :].astype(F32)
                    ).astype(BF16)

                chunked(n, add_core)
                y_copy(i).start()
            yield
            for i in range(blocks):
                core_copy(1, i).start()
            yield

        def up_copy(i, zz):
            return remote(z_out.at[i], z_up.at[zz], z_send.at[i], up_recv.at[zz], here.up)

        def down_copy(i, zz):
            return remote(z_out.at[i], z_down.at[zz], z_send.at[i], down_recv.at[zz], here.down)

        for i in range(blocks):
            zz = dest(i)
            near = place(zz, c)
            if use_c:
                core_copy(1, i).wait_recv()
                y_copy(i).wait_recv()

            def local(r, step, i=i, near=near):
                total = p_ref[at(near, r, step)].astype(F32)
                if use_c:
                    s = pl.ds(r, step)
                    total = total + c_buf[blocks + i, s, :].astype(F32)
                    total = total + y_buf[i, s, :].astype(F32)
                return total

            if not use_z:

                def store(r, step, local=local):
                    o_ref[pl.ds(r, step), :] = local(r, step).astype(o_ref.dtype)

                chunked(n, store)
            elif i < ROWS - 1:

                def send(copy, buf, first, i=i, zz=zz, local=local):
                    @pl.when(first)
                    def _():
                        def put(r, step):
                            z_out[i, pl.ds(r, step), :] = local(r, step).astype(BF16)

                        chunked(n, put)

                    @pl.when(jnp.logical_not(first))
                    def _():
                        copy(i, zz).wait_recv()

                        def put(r, step):
                            s = pl.ds(r, step)
                            z_out[i, s, :] = (
                                local(r, step) + buf[zz, s, :].astype(F32)
                            ).astype(BF16)

                        chunked(n, put)

                    copy(i, zz).start()

                pl.when(zz > z)(functools.partial(send, up_copy, z_up, z == 0))
                pl.when(zz < z)(functools.partial(send, down_copy, z_down, z == ROWS - 1))
            else:

                def final(bufs, local=local):
                    def put(r, step):
                        s = pl.ds(r, step)
                        total = local(r, step)
                        for buf in bufs:
                            total = total + buf[z, s, :].astype(F32)
                        o_ref[s, :] = total.astype(o_ref.dtype)

                    chunked(n, put)

                pl.when(z > 0)(lambda: up_copy(0, z).wait_recv())
                pl.when(z < ROWS - 1)(lambda: down_copy(0, z).wait_recv())
                pl.when(z == 0)(lambda: final([z_down]))
                pl.when(z == ROWS - 1)(lambda: final([z_up]))
                pl.when(here.inner == 1)(lambda: final([z_up, z_down]))
            yield

        if use_c:
            for i in range(blocks):
                core_copy(0, i).wait_send()
                core_copy(1, i).wait_send()
                y_copy(i).wait_send()
        if use_z:
            for i in range(ROWS - 1):
                up_copy(i, 0).wait_send()

    return Part([p], [jax.ShapeDtypeStruct((n, w), dtype)], scratch, kinds, steps)


def pull_weights(weights, axes, dp):
    outs, shapes = [], []
    for w, axis in zip(weights, axes):
        shape = list(w.shape)
        shape[axis] //= ROWS
        shape[1 - axis] *= ROWS
        outs.append(jax.ShapeDtypeStruct(tuple(shape), w.dtype))
        shapes.append((w.shape[0] // (ROWS if axis == 0 else 1), w.shape[1] // (ROWS if axis else 1)))
    count = len(weights)
    shared = dp == 2
    kinds = {"rows"} | ({"dp"} if shared else set())

    def steps(here, ins, outs, sems):
        send, recv, dp_send, dp_recv = sems

        def source(m, zz, half):
            n, w = shapes[m]
            first = zz * n if axes[m] == 0 else 0
            rows = n // 2 if half else n
            first = first + here.dp * rows if half else first
            cols = slice(None) if axes[m] == 0 else pl.ds(pl.multiple_of(zz * w, w), w)
            return pl.ds(pl.multiple_of(first, rows), rows), cols

        def target(m, zz, half):
            n, w = shapes[m]
            first = zz * n if axes[m] == 1 else 0
            rows = n // 2 if half else n
            first = first + here.dp * rows if half else first
            cols = slice(None) if axes[m] == 1 else pl.ds(pl.multiple_of(zz * w, w), w)
            return pl.ds(pl.multiple_of(first, rows), rows), cols

        def copy(m, zz, landing):
            return remote(
                ins[m].at[source(m, zz, shared)],
                outs[m].at[target(m, landing, shared)],
                send.at[m * ROWS + zz],
                recv.at[m * ROWS + landing],
                here.row(zz),
            )

        def pass_on(m, zz):
            k = m * ROWS + zz
            region = outs[m].at[target(m, zz, True)]
            return remote(region, region, dp_send.at[k], dp_recv.at[k], here.over_dp)

        for m in range(count):
            from_place, to_place = source(m, here.z, False), target(m, here.z, False)

            def keep(r, step, m=m, from_place=from_place, to_place=to_place):
                outs[m][at(to_place, r, step)] = ins[m][at(from_place, r, step)]

            chunked(shapes[m][0], keep)
        yield
        for d in (2, 1, 3):
            for m in range(count):
                copy(m, (here.z + d) % ROWS, here.z).start()
            yield
        for _, _, zz in here.others():
            for m in range(count):
                copy(m, here.z, zz).wait_recv()
                if shared:
                    pass_on(m, zz).start()
            yield
        for m in range(count):
            for _, zz, _ in here.others():
                copy(m, zz, here.z).wait_send()
                if shared:
                    pass_on(m, zz).wait_send()
                    pass_on(m, zz).wait_recv()

    sems = [DMA((count * ROWS,))] * 4
    return Part(list(weights), outs, sems, kinds, steps)


def swap_halves_sum(values, axes):
    outs, scratch = [], []
    for v, axis in zip(values, axes):
        n, w = v.shape
        outs.append(jax.ShapeDtypeStruct((n // 2, w), BF16))
        scratch.append(VMEM((n // 2, w), BF16))
    blocks = [ROWS if axis == 1 else 1 for axis in axes]
    total = sum(blocks)
    scratch += [DMA((total,))] * 2

    def steps(here, ins, outs, refs):
        bufs, send, recv = refs[: len(values)], refs[-2], refs[-1]
        work = []
        k = 0
        for m, v in enumerate(values):
            n = v.shape[0] // blocks[m]
            h = n // 2
            for b in range(blocks[m]):
                theirs = pl.ds(pl.multiple_of(b * n + (1 - here.dp) * h, h), h)
                copy = functools.partial(
                    remote,
                    ins[m].at[theirs],
                    bufs[m].at[pl.ds(b * h, h)],
                    send.at[k],
                    recv.at[k],
                    here.over_dp,
                )
                copy().start()
                work.append((m, b, h, n, copy))
                k += 1
        yield
        for m, b, h, n, copy in work:
            copy().wait_recv()

            def add(r, step, m=m, b=b, h=h, n=n):
                own = pl.ds(pl.multiple_of(b * n + here.dp * h + r, step), step)
                s = pl.ds(pl.multiple_of(b * h + r, step), step)
                outs[m][s, :] = (
                    ins[m][own, :].astype(F32) + bufs[m][s, :].astype(F32)
                ).astype(BF16)

            chunked(h, add)
        yield
        for m, b, h, n, copy in work:
            copy().wait_send()

    return Part(list(values), outs, scratch, {"dp"}, steps)


def push_gradients(values, axes, dp):
    shared = dp == 2
    halves = 2 if shared else 1
    outs, shapes = [], []
    for v, axis in zip(values, axes):
        n, w = v.shape
        if axis == 1:
            n = n // ROWS
            outs.append(jax.ShapeDtypeStruct((halves, n, w * ROWS), v.dtype))
        else:
            w = w // ROWS
            outs.append(jax.ShapeDtypeStruct((ROWS, halves, n, w), v.dtype))
        shapes.append((n, w))
    count = len(values)
    kinds = {"rows"} | ({"dp"} if shared else set())

    def steps(here, ins, outs, sems):
        send, recv, dp_send, dp_recv = sems
        half = here.dp if shared else 0

        def block(m, zz):
            n, w = shapes[m]
            if axes[m] == 1:
                return ins[m].at[pl.ds(pl.multiple_of(zz * n, n), n)]
            return ins[m].at[:, pl.ds(pl.multiple_of(zz * w, w), w)]

        def slot(m, zz):
            n, w = shapes[m]
            if axes[m] == 1:
                return outs[m].at[half, :, pl.ds(pl.multiple_of(zz * w, w), w)]
            return outs[m].at[zz, half]

        def copy(m, zz, landing):
            return remote(
                block(m, zz),
                slot(m, landing),
                send.at[m * ROWS + zz],
                recv.at[m * ROWS + landing],
                here.row(zz),
            )

        def pass_on(m, zz):
            k = m * ROWS + zz
            return remote(slot(m, zz), slot(m, zz), dp_send.at[k], dp_recv.at[k], here.over_dp)

        for m in range(count):
            for _, zz, _ in here.others():
                copy(m, zz, here.z).start()
        for m in range(count):

            def keep(r, step, m=m):
                s = pl.ds(r, step)
                slot(m, here.z)[s, :] = block(m, here.z)[s, :]

            chunked(shapes[m][0], keep)
            if shared:
                pass_on(m, here.z).start()
        yield
        for m in range(count):
            for d in (1, 3, 2):
                zz = (here.z - d + ROWS) % ROWS
                copy(m, here.z, zz).wait_recv()
                if shared:
                    pass_on(m, zz).start()
        yield
        for m in range(count):
            for _, zz, _ in here.others():
                copy(m, zz, here.z).wait_send()
            if shared:
                for zz in range(ROWS):
                    pass_on(m, zz).wait_send()
                    remote(
                        slot(m, zz), slot(m, zz), dp_send.at[0], dp_recv.at[m * ROWS + zz], here.over_dp
                    ).wait_recv()

    sems = [DMA((count * ROWS,))] * 4
    return Part(list(values), outs, sems, kinds, steps)


def swap(values):
    outs = [jax.ShapeDtypeStruct(v.shape, v.dtype) for v in values]

    def steps(here, ins, outs, sems):
        copies = [
            remote(i, o, sems[0].at[k], sems[1].at[k], here.over_dp)
            for k, (i, o) in enumerate(zip(ins, outs))
        ]
        for copy in copies:
            copy.start()
        yield
        for copy in copies:
            copy.wait()

    return Part(list(values), outs, [DMA((len(values),))] * 2, {"dp"}, steps)


def sum_gains(vector, n_dp):
    shape = vector.shape

    def steps(here, ins, outs, refs):
        (v_ref,), (o_ref,) = ins, outs
        buf, part, groups, send, recv, dp_send, dp_recv = refs
        me = here.z * COLS + here.c
        for k, zz, cc in here.peers():
            remote(v_ref, buf.at[me], send.at[k], recv.at[me], (here.dp, zz, cc)).start()
        buf[me] = v_ref[...]
        yield
        for k, zz, cc in here.peers():
            source = zz * COLS + cc
            copy = remote(
                v_ref, buf.at[source], send.at[k], recv.at[source], (here.dp, zz, cc)
            )
            copy.wait_send()
            copy.wait_recv()
        for zz in range(ROWS):
            part[zz] = buf[zz * COLS] + buf[zz * COLS + 1] + buf[zz * COLS + 2] + buf[zz * COLS + 3]
        groups[here.dp] = part[...]
        for d in range(1, n_dp):
            remote(
                part, groups.at[here.dp], dp_send.at[d], dp_recv.at[here.dp], here.group(d)
            ).start()
        yield
        for d in range(1, n_dp):
            source = (here.dp + d) % n_dp
            copy = remote(
                part, groups.at[source], dp_send.at[d], dp_recv.at[source], here.group(d)
            )
            copy.wait_send()
            copy.wait_recv()
        total = groups[0]
        for d in range(1, n_dp):
            total = total + groups[d]
        o_ref[...] = total

    scratch = [
        VMEM((ROWS * COLS,) + shape, F32),
        VMEM((ROWS,) + shape, F32),
        VMEM((n_dp, ROWS) + shape, F32),
        DMA((ROWS * COLS,)),
        DMA((ROWS * COLS,)),
        DMA((n_dp,)),
        DMA((n_dp,)),
    ]
    outs = [jax.ShapeDtypeStruct((ROWS,) + shape, F32)]
    return Part([vector], outs, scratch, {"plane", "dp"}, steps)


class Plan:
    def __init__(self):
        self.specs, self.kinds = [], set()

    def add(self, part):
        first = len(self.specs)
        self.specs += part.scratch
        self.kinds |= part.kinds
        return part, first

    def buffer(self, shape, dtype):
        self.specs.append(VMEM(shape, dtype))
        return len(self.specs) - 1

    def bind(self, here, refs):
        self.here, self.refs = here, refs

    def __getitem__(self, handle):
        return self.refs[handle]

    def start(self, handle, ins, outs):
        part, first = handle
        steps = part.steps(self.here, ins, outs, self.refs[first : first + len(part.scratch)])
        next(steps, None)
        return steps


def advance(steps, count=1):
    for _ in range(count):
        next(steps, None)


def finish(steps):
    for _ in steps:
        pass


def like(shape, dtype):
    return jax.ShapeDtypeStruct(shape, dtype)


def planned(n_dp, call, name, plan, args, outs, body):
    ins, out_list = vars(args), vars(outs)

    def kernel(*refs):
        here = Here(n_dp)
        i = SimpleNamespace(**dict(zip(ins, refs)))
        o = SimpleNamespace(**dict(zip(out_list, refs[len(ins) :])))
        plan.bind(here, refs[len(ins) + len(out_list) :])
        meet(here, plan.kinds)
        body(i, o)

    vmem = pl.BlockSpec(memory_space=VMEM)
    results = pl.pallas_call(
        kernel,
        out_shape=list(out_list.values()),
        in_specs=[vmem] * len(ins),
        out_specs=[vmem] * len(out_list),
        scratch_shapes=plan.specs,
        compiler_params=pltpu.CompilerParams(
            collective_id=call, has_side_effects=True, vmem_limit_bytes=63 << 20
        ),
        name=name,
    )(*ins.values())
    return SimpleNamespace(**dict(zip(out_list, results)))


def rows_times(o_ref, terms, block=256, first=0, last=None):
    def body(i, _):
        s = pl.ds(pl.multiple_of(i * block, block), block)
        total = None
        for a_ref, columns, b_ref, flipped in terms:
            term = dot(a_ref[s, columns], b_ref[...], flipped)
            total = term if total is None else total + term
        o_ref[s, :] = total.astype(o_ref.dtype)
        return 0

    lax.fori_loop(first, last or o_ref.shape[0] // block, body, 0)


def columns_times(o_ref, a_ref, b_ref, height=256, width=512):
    across = b_ref.shape[1] // width

    def body(i, _):
        m = pl.ds(pl.multiple_of(i // across * height, height), height)
        n = pl.ds(pl.multiple_of(i % across * width, width), width)
        o_ref[m, n] = weight_term(a_ref[:, m], b_ref[:, n]).astype(o_ref.dtype)
        return 0

    lax.fori_loop(0, a_ref.shape[1] // height * across, body, 0)


ALL = slice(None)


def swapped(field):
    return pltpu.roll(field, HEAD_SIZE // 2, 1)


def lane_major(column):
    return jnp.transpose(jnp.broadcast_to(column, (column.shape[0], HEAD_SIZE)))[:8]


def token_major(row):
    return jnp.transpose(jnp.broadcast_to(row, (HEAD_SIZE, row.shape[1])))


def head_at(ref, h):
    return ref[:, pl.ds(h * HEAD_SIZE, HEAD_SIZE)]


def make_tables(seg_ref, inverse_ref, sign_ref, o):
    row = seg_ref[...].astype(F32)
    n = row.shape[1]
    column = token_major(row)[:, 0:1]
    query = lax.broadcasted_iota(jnp.int32, (n, n), 0)
    key = lax.broadcasted_iota(jnp.int32, (n, n), 1)
    allowed = (column == row) & (key <= query)
    o.bias[...] = jnp.where(allowed, 0.0, -1e30)
    position = jnp.sum(jnp.where(allowed, 1.0, 0.0), axis=-1, keepdims=True) - 1.0
    angle = position * inverse_ref[...]
    o.cosine[...] = jnp.cos(angle)
    o.sine[...] = jnp.sin(angle) * sign_ref[...]


def attention_forward(i, o):
    heads, groups = o.q.shape[1] // HEAD_SIZE, o.k.shape[1] // HEAD_SIZE
    each = heads // groups
    scale = HEAD_SIZE ** (-0.5)
    lane = lax.broadcasted_iota(jnp.int32, o.lse.shape, 1)

    def turned(at_head, gain_ref):
        raw = head_at(o.joint, at_head)
        norm = lax.rsqrt(jnp.mean(raw * raw, axis=-1, keepdims=True) + EPSILON)
        field = raw * norm * gain_ref[...]
        return (field * o.cosine[...] + swapped(field) * o.sine[...]).astype(BF16)

    for g in range(groups):
        at_head = pl.ds(g * HEAD_SIZE, HEAD_SIZE)
        o.k[:, at_head] = turned(heads + g, i.key_gain)
        o.v[:, at_head] = head_at(o.joint, heads + groups + g).astype(BF16)
        for h in range(g * each, (g + 1) * each):
            query = turned(h, i.query_gain)
            o.q[:, pl.ds(h * HEAD_SIZE, HEAD_SIZE)] = query
            scores = dot(query, o.k[:, at_head], True) * scale + o.bias[...]
            top = jnp.max(scores, axis=-1, keepdims=True)
            weights = jnp.exp(scores - top)
            total = jnp.sum(weights, axis=-1, keepdims=True)
            probs = (weights / total).astype(BF16)
            o.mixed[:, pl.ds(h * HEAD_SIZE, HEAD_SIZE)] = dot(probs, o.v[:, at_head]).astype(BF16)
            log_total = jnp.broadcast_to(top + jnp.log(total), o.lse.shape)
            if h == 0:
                o.lse[...] = log_total
            else:
                o.lse[...] = jnp.where(lane == h, log_total, o.lse[...])
            yield


def forward(n_dp, call, a):
    length, feats = a.layer_input.shape
    query_width, key_width = a.w_query.shape[1], a.key_matrix.shape[1]
    wide = query_width + 2 * key_width
    tokens = length * COLS
    units = a.w_gate.shape[1] // ROWS
    plan = Plan()
    in_gather = plan.add(gather(a.layer_input, False, True))
    joint_sum = plan.add(scatter_sum(like((tokens, wide), BF16), True, False))
    in_stat = plan.add(send_stats(like((ROWS, 8, length), F32), row_stats))
    cot_gather = plan.add(gather(a.cotangent, True, True))
    mix_gather = plan.add(gather(like((length, query_width), BF16), True, False))
    out_sum = plan.add(scatter_sum(like((tokens, feats), BF16), False, True))
    mid_gather = plan.add(gather(like((length, feats), BF16), True, True, like((8, length), F32)))
    pulls = [
        pull_weights([a.w_down], [0], n_dp),
        pull_weights([a.w_gate], [1], n_dp),
        pull_weights([a.w_up], [1], n_dp),
    ]
    pull_low, pull_gate, pull_up = [plan.add(p) for p in pulls]
    in_rows = plan.buffer((tokens, feats), BF16)
    stats = plan.buffer((ROWS, 8, length), F32)
    got_stats = plan.buffer((ROWS, 8, length), F32)
    mid_stats = plan.buffer((ROWS * COLS, 8, length), F32)
    own_stat = plan.buffer((8, length), F32)
    p_joint = plan.buffer((tokens, wide), BF16)
    p_out = plan.buffer((tokens, feats), BF16)
    attn_out = plan.buffer((length, feats), F32)
    gained = plan.buffer((length, feats), BF16)
    outs = SimpleNamespace(
        in_gained=like((tokens, feats), BF16),
        joint=like((length, wide), F32),
        scale_in=like((length, HEAD_SIZE), F32),
        bias=like((length, length), F32),
        cosine=like((length, HEAD_SIZE), F32),
        sine=like((length, HEAD_SIZE), F32),
        q=like((length, query_width), BF16),
        k=like((length, key_width), BF16),
        v=like((length, key_width), BF16),
        mixed=like((length, query_width), BF16),
        lse=like((length, HEAD_SIZE), F32),
        mix_rows=like((tokens, query_width), BF16),
        hidden=like((length, feats), F32),
        mid_rows=like((tokens, MODEL_WIDTH), BF16),
        scale_mid=like((tokens, HEAD_SIZE), F32),
        cot_rows=like((tokens, MODEL_WIDTH), BF16),
        w_low=pulls[0].outs[0],
        w_gate_all=pulls[1].outs[0],
        w_up_all=pulls[2].outs[0],
        grad_active=like((tokens, units), F32),
    )

    def body(i, o):
        first = plan.start(in_gather, [i.layer_input], [plan[in_rows]])
        low = plan.start(pull_low, [i.w_down], [o.w_low])
        advance(low, 3)
        make_tables(i.segment, i.inverse, i.sign, o)
        finish(first)
        cot = plan.start(cot_gather, [i.cotangent], [o.cot_rows])

        def normed(b, _):
            s = pl.ds(pl.multiple_of(b * length, length), length)
            field = plan[in_rows][s, :].astype(F32)
            o.in_gained[s, :] = (field * i.attn_gain[...]).astype(BF16)
            plan[stats][b] = lane_major(jnp.sum(field * field, axis=-1, keepdims=True))
            for columns, w_ref in (
                (pl.ds(0, query_width), i.w_query),
                (pl.ds(query_width, key_width), i.key_matrix),
                (pl.ds(query_width + key_width, key_width), i.value_matrix),
            ):
                plan[p_joint][s, columns] = dot(o.in_gained[s, :], w_ref[...]).astype(BF16)
            return 0

        lax.fori_loop(0, COLS, normed, 0)
        total = plan.start(joint_sum, [plan[p_joint]], [o.joint])
        stat = plan.start(in_stat, [plan[stats]], [plan[got_stats]])
        advance(low, 3)
        advance(cot)
        advance(total)
        advance(cot, 2)
        advance(total)
        advance(cot, 2)
        finish(total)
        advance(cot)
        finish(stat)
        summed = plan[got_stats][0] + plan[got_stats][1] + plan[got_stats][2] + plan[got_stats][3]
        o.scale_in[...] = lax.rsqrt(token_major(summed[0:1]) / MODEL_WIDTH + EPSILON)

        def scaled(r, step):
            s = pl.ds(r, step)
            o.joint[s, :] = o.joint[s, :] * o.scale_in[s, 0:1]

        chunked(length, scaled)
        for _ in attention_forward(i, o):
            pass
        mix = plan.start(mix_gather, [o.mixed], [o.mix_rows])
        advance(mix, 2)
        gate = plan.start(pull_gate, [i.w_gate], [o.w_gate_all])
        advance(gate, 3)
        finish(mix)
        finish(cot)
        finish(low)
        rows_times(plan[p_out], [(o.mix_rows, ALL, i.w_output, False)])
        out = plan.start(out_sum, [plan[p_out]], [plan[attn_out]])
        advance(out, 2)
        finish(out)

        def add(r, step):
            s = pl.ds(r, step)
            field = i.layer_input[s, :].astype(F32) + plan[attn_out][s, :]
            o.hidden[s, :] = field
            plan[gained][s, :] = (field * i.mlp_gain[...]).astype(BF16)

        chunked(length, add)
        plan[own_stat][...] = lane_major(
            jnp.sum(o.hidden[...] * o.hidden[...], axis=-1, keepdims=True)
        )
        mid = plan.start(
            mid_gather, [plan[gained], plan[own_stat]], [o.mid_rows, plan[mid_stats]]
        )
        advance(mid, 2)
        advance(gate, 3)
        advance(mid)
        up = plan.start(pull_up, [i.w_up], [o.w_up_all])
        advance(up, 3)
        for k in range(4):
            rows_times(o.grad_active, [(o.cot_rows, ALL, o.w_low, True)], first=k, last=k + 1)
            advance(mid)
        advance(up, 3)
        finish(mid)
        for b in range(COLS):
            summed = plan[mid_stats][b]
            for zz in range(1, ROWS):
                summed = summed + plan[mid_stats][zz * COLS + b]
            o.scale_mid[pl.ds(b * length, length), :] = lax.rsqrt(
                token_major(summed[0:1]) / MODEL_WIDTH + EPSILON
            )
        finish(gate)
        finish(up)

    return planned(n_dp, call, "forward", plan, a, outs, body)


def middle(n_dp, call, a):
    two = n_dp == 2
    length, feats = a.hidden.shape
    tokens, units = a.grad_active.shape
    plan = Plan()
    mid_sum = plan.add(scatter_sum(like((tokens, MODEL_WIDTH), BF16), True, True))
    inner_stat = plan.add(send_stats(like((COLS, 8, length), F32), plane_stats))
    d_low = like((units, MODEL_WIDTH), BF16)
    if two:
        low_half = plan.add(swap_halves_sum([d_low], [0]))
        low = plan.buffer(d_low.shape, BF16)
        d_low = like((units // 2, MODEL_WIDTH), BF16)
    p_mid = plan.buffer((tokens, MODEL_WIDTH), BF16)
    d_gate = plan.buffer((tokens, units), BF16)
    d_up = plan.buffer((tokens, units), BF16)
    inner = plan.buffer((COLS, 8, length), F32)
    inners = plan.buffer((ROWS * COLS, 8, length), F32)
    grad_mid = plan.buffer((length, feats), F32)
    outs = SimpleNamespace(
        grad_hidden=like((length, feats), F32),
        grad_attn=like((length, feats), BF16),
        gain_mid=like((16, HEAD_SIZE), F32),
        active=like((tokens, units), BF16),
        grad_low=d_low,
        grad_gate=like((MODEL_WIDTH, units), BF16),
        grad_up=like((MODEL_WIDTH, units), BF16),
    )

    def body(i, o):
        here = plan.here

        def tokens_of(b):
            s = pl.ds(pl.multiple_of(b * length, length), length)
            scale = i.scale_mid[s, 0:1]
            gate = dot(i.mid_rows[s, :], i.w_gate_all[...]) * scale
            upward = dot(i.mid_rows[s, :], i.w_up_all[...]) * scale
            silu, slope = silu_parts(gate)
            o.active[s, :] = (silu * upward).astype(BF16)
            grad = i.grad_active[s, :] * scale
            grad_gate = (grad * upward * slope).astype(BF16)
            grad_up = (grad * silu).astype(BF16)
            plan[d_gate][s, :] = grad_gate
            plan[d_up][s, :] = grad_up
            term = grad_gate.astype(F32) * gate + grad_up.astype(F32) * upward
            plan[inner][b] = lane_major(jnp.sum(term, axis=-1, keepdims=True) * scale)
            for k in range(ROWS):
                part = pl.ds(k * feats, feats)
                plan[p_mid][s, part] = (
                    dot(grad_gate, i.w_gate_all[part, :], True)
                    + dot(grad_up, i.w_up_all[part, :], True)
                ).astype(BF16)

        tokens_of((here.c_core + 2) % COLS)
        total = plan.start(mid_sum, [plan[p_mid]], [plan[grad_mid]])
        tokens_of(here.c_y)
        advance(total)
        tokens_of(here.c_core)
        advance(total)
        tokens_of(here.c)
        stat = plan.start(inner_stat, [plan[inner]], [plan[inners]])
        advance(total)
        low_ref = plan[low] if two else o.grad_low
        columns_times(low_ref, o.active, i.cot_rows, units)
        if two:
            low_sum = plan.start(low_half, [low_ref], [o.grad_low])
        advance(total)
        columns_times(o.grad_gate, i.mid_rows, plan[d_gate], width=units)
        advance(total)
        columns_times(o.grad_up, i.mid_rows, plan[d_up], width=units)
        finish(total)
        finish(stat)
        summed = plan[inners][0]
        for k in range(1, ROWS * COLS):
            summed = summed + plan[inners][k]
        coef = token_major(summed[0:1] / MODEL_WIDTH)[:, 0:1]
        grad = plan[grad_mid][...]
        hidden = i.hidden[...]
        total = jnp.sum(grad * hidden, axis=0, keepdims=True)
        o.gain_mid[...] = jnp.zeros((16, HEAD_SIZE), F32)
        for k in range(feats // HEAD_SIZE):
            o.gain_mid[4 + k : 5 + k, :] = total[:, k * HEAD_SIZE : (k + 1) * HEAD_SIZE]
        grad = i.cotangent[...].astype(F32) + grad * i.mlp_gain[...] - hidden * coef
        o.grad_hidden[...] = grad
        o.grad_attn[...] = grad.astype(BF16)
        if two:
            finish(low_sum)

    return planned(n_dp, call, "middle", plan, a, outs, body)


def attention_back(i, grad_mixed, gq_ref, gkv_ref, inner_ref, gains_ref, dk_ref, dv_ref):
    heads, groups = i.q.shape[1] // HEAD_SIZE, i.k.shape[1] // HEAD_SIZE
    each = heads // groups
    scale = HEAD_SIZE ** (-0.5)
    cosine, sine = i.cosine[...], i.sine[...]
    scale_in = i.scale_in[:, 0:1]
    inner = jnp.zeros((i.q.shape[0], HEAD_SIZE), F32)

    def put(at_head, out):
        if at_head < heads:
            gq_ref[:, pl.ds(at_head * HEAD_SIZE, HEAD_SIZE)] = out
        else:
            gkv_ref[:, pl.ds((at_head - heads) * HEAD_SIZE, HEAD_SIZE)] = out

    def norm_back(grad_rot, at_head, gain):
        grad = grad_rot * cosine - swapped(grad_rot) * sine
        raw = head_at(i.joint, at_head)
        norm = lax.rsqrt(jnp.mean(raw * raw, axis=-1, keepdims=True) + EPSILON)
        unit = raw * norm
        u = grad * gain
        back = norm * (u - unit * jnp.mean(u * unit, axis=-1, keepdims=True))
        out = (back * scale_in).astype(BF16)
        put(at_head, out)
        return out.astype(F32) * raw, jnp.sum(grad * unit, axis=0, keepdims=True)

    gain_q = jnp.zeros((1, HEAD_SIZE), F32)
    gain_k = jnp.zeros((1, HEAD_SIZE), F32)
    for g in range(groups):
        key, value = head_at(i.k, g), head_at(i.v, g)
        for r in range(each):
            h = g * each + r
            query, grad = head_at(i.q, h), head_at(grad_mixed, h)
            scores = dot(query, key, True) * scale + i.bias[...]
            probs = jnp.exp(scores - i.lse[:, h : h + 1])
            term_v = weight_term(probs.astype(BF16), grad)
            delta = jnp.sum(
                grad.astype(F32) * head_at(i.mixed, h).astype(F32), axis=-1, keepdims=True
            )
            grad_scores = (probs * (dot(grad, value, True) - delta)).astype(BF16)
            term_k = weight_term(grad_scores, query) * scale
            if r == 0:
                dv_ref[...] = term_v
                dk_ref[...] = term_k
            else:
                dv_ref[...] += term_v
                dk_ref[...] += term_k
            term, gain = norm_back(dot(grad_scores, key) * scale, h, i.query_gain[...])
            inner = inner + term
            gain_q = gain_q + gain
        term, gain = norm_back(dk_ref[...], heads + g, i.key_gain[...])
        inner = inner + term
        gain_k = gain_k + gain
        at_head = heads + groups + g
        out = (dv_ref[...] * scale_in).astype(BF16)
        put(at_head, out)
        inner = inner + out.astype(F32) * head_at(i.joint, at_head)
    gains_ref[8:9, :] = gain_q
    gains_ref[9:10, :] = gain_k
    inner_ref[0] = lane_major(jnp.sum(inner, axis=-1, keepdims=True) * scale_in)


def backward(n_dp, call, a):
    two = n_dp == 2
    length, feats = a.grad_attn.shape
    query_width, key_width = a.w_query.shape[1], a.key_matrix.shape[1]
    tokens = length * COLS
    plan = Plan()
    attn_gather = plan.add(gather(a.grad_attn, False, True))
    mixed_sum = plan.add(scatter_sum(like((tokens, feats), BF16), True, False, BF16))
    q_gather = plan.add(gather(like((length, query_width), BF16), True, False))
    kv_gather = plan.add(gather(like((length, 2 * key_width), BF16), True, False))
    in_sum = plan.add(scatter_sum(like((tokens, feats), BF16), False, True))
    in_stat = plan.add(send_stats(like((1, 8, length), F32), owner_stats))
    block_sum = plan.add(scatter_sum(like((tokens, MODEL_WIDTH), BF16), True, True))
    n, w = a.grad_gate.shape
    half = like((n // 2 if two else n, w), BF16)
    if two:
        gate_half = plan.add(swap_halves_sum([a.grad_gate], [1]))
        up_half = plan.add(swap_halves_sum([a.grad_up], [1]))
        gate_sum = plan.buffer(half.shape, BF16)
        up_sum = plan.buffer(half.shape, BF16)
    pushes = [
        push_gradients([half], [1], n_dp),
        push_gradients([half], [1], n_dp),
        push_gradients([a.grad_low], [0], n_dp),
    ]
    gate_push, up_push, low_push = [plan.add(p) for p in pushes]
    gain_sum = plan.add(sum_gains(like((16, HEAD_SIZE), F32), n_dp))
    d_output, d_q = like((feats, feats), BF16), like((feats, query_width), BF16)
    d_kv = like((feats, 2 * key_width), BF16)
    if two:
        output_swap = plan.add(swap([d_output]))
        q_swap = plan.add(swap([d_q]))
        kv_swap = plan.add(swap([d_kv]))
    attn_rows = plan.buffer((tokens, feats), BF16)
    p_mixed = plan.buffer((tokens, feats), BF16)
    grad_mixed = plan.buffer((length, feats), BF16)
    q_in = plan.buffer((length, query_width), BF16)
    kv_in = plan.buffer((length, 2 * key_width), BF16)
    q_rows = plan.buffer((tokens, query_width), BF16)
    kv_rows = plan.buffer((tokens, 2 * key_width), BF16)
    p_in = plan.buffer((tokens, feats), BF16)
    p_block = plan.buffer((tokens, MODEL_WIDTH), BF16)
    inner = plan.buffer((1, 8, length), F32)
    gain_rows = plan.buffer((16, HEAD_SIZE), F32)
    dk, dv = [plan.buffer((length, HEAD_SIZE), F32) for _ in range(2)]
    outs = SimpleNamespace(
        grad_in=like((length, feats), F32),
        in_inners=like((COLS, 8, length), F32),
        block=like((length, feats), F32),
        grad_gate=pushes[0].outs[0],
        grad_up=pushes[1].outs[0],
        grad_low=pushes[2].outs[0],
        gains=like((ROWS, 16, HEAD_SIZE), F32),
        d_output=d_output,
        d_q=d_q,
        d_kv=d_kv,
    )
    if two:
        outs.d_output_other, outs.d_q_other, outs.d_kv_other = d_output, d_q, d_kv

    def body(i, o):
        attn = plan.start(attn_gather, [i.grad_attn], [plan[attn_rows]])
        low = plan.start(low_push, [i.grad_low], [o.grad_low])
        if two:
            gate_sums = plan.start(gate_half, [i.grad_gate], [plan[gate_sum]])
        rows_times(plan[p_block], [(i.active, ALL, i.w_low, False)], first=0, last=3)
        finish(attn)
        if two:
            up_sums = plan.start(up_half, [i.grad_up], [plan[up_sum]])
        rows_times(plan[p_mixed], [(plan[attn_rows], ALL, i.w_output, True)])
        mixed = plan.start(mixed_sum, [plan[p_mixed]], [plan[grad_mixed]])
        rows_times(plan[p_block], [(i.active, ALL, i.w_low, False)], first=3, last=4)
        block = plan.start(block_sum, [plan[p_block]], [o.block])
        advance(mixed)
        advance(block, 2)
        advance(low)
        if two:
            advance(gate_sums)
        advance(mixed)
        finish(mixed)
        plan[gain_rows][...] = i.gain_mid[...]
        attention_back(
            i,
            plan[grad_mixed],
            plan[q_in],
            plan[kv_in],
            plan[inner],
            plan[gain_rows],
            plan[dk],
            plan[dv],
        )
        kv = plan.start(kv_gather, [plan[kv_in]], [plan[kv_rows]])
        q = plan.start(q_gather, [plan[q_in]], [plan[q_rows]])
        stat = plan.start(in_stat, [plan[inner]], [o.in_inners])
        if two:
            advance(up_sums)
        advance(kv)
        gate = plan.start(gate_push, [plan[gate_sum] if two else i.grad_gate], [o.grad_gate])
        columns_times(o.d_output, i.mix_rows, plan[attn_rows])
        if two:
            swap_output = plan.start(output_swap, [o.d_output], [o.d_output_other])
        advance(q)
        advance(kv)
        advance(q)
        finish(kv)
        advance(gate)
        up = plan.start(up_push, [plan[up_sum] if two else i.grad_up], [o.grad_up])
        columns_times(o.d_kv, i.in_gained, plan[kv_rows])
        if two:
            swap_kv = plan.start(kv_swap, [o.d_kv], [o.d_kv_other])
        finish(q)
        columns_times(o.d_q, i.in_gained, plan[q_rows])
        if two:
            swap_q = plan.start(q_swap, [o.d_q], [o.d_q_other])
        rows_times(
            plan[p_in],
            [
                (plan[q_rows], ALL, i.w_query, True),
                (plan[kv_rows], pl.ds(0, key_width), i.key_matrix, True),
                (plan[kv_rows], pl.ds(key_width, key_width), i.value_matrix, True),
            ],
        )
        grad_in = plan.start(in_sum, [plan[p_in]], [o.grad_in])
        advance(grad_in)
        advance(block)
        advance(up)
        finish(grad_in)
        total = jnp.sum(o.grad_in[...] * i.layer_input[...].astype(F32), axis=0, keepdims=True)
        for k in range(feats // HEAD_SIZE):
            plan[gain_rows][k : k + 1, :] = total[:, k * HEAD_SIZE : (k + 1) * HEAD_SIZE]
        gains = plan.start(gain_sum, [plan[gain_rows]], [o.gains])
        finish(block)
        finish(gains)
        finish(stat)
        finish(low)
        finish(gate)
        finish(up)
        if two:
            finish(gate_sums)
            finish(up_sums)
            finish(swap_output)
            finish(swap_kv)
            finish(swap_q)

    return planned(n_dp, call, "backward", plan, a, outs, body)


def silu_parts(gate):
    sigma = jax.nn.sigmoid(gate)
    return (gate * sigma, sigma * (1.0 + gate * (1.0 - sigma)))


def dot(left, right, flipped=False):
    return lax.dot_general(
        left, right, (((1,), (1 if flipped else 0,)), ((), ())), preferred_element_type=F32
    )


def weight_term(left, right):
    return lax.dot_general(left, right, (((0,), (0,)), ((), ())), preferred_element_type=F32)


def per_device(
    dp,
    layer_input,
    cotangent,
    w_query,
    key_matrix,
    value_matrix,
    w_output,
    w_gate,
    w_up,
    w_down,
    attn_gain,
    mlp_gain,
    query_gain,
    key_gain,
    segment_ids,
):
    length, feats = layer_input.shape
    key_width = key_matrix.shape[1]
    ff_local = w_gate.shape[1]
    two = dp == 2
    half = jnp.arange(HEAD_SIZE // 2, dtype=F32)
    inverse = jnp.power(THETA, -(half * (2.0 / HEAD_SIZE)))
    ones = jnp.ones_like(half)
    f = forward(
        dp,
        0,
        SimpleNamespace(
            layer_input=layer_input,
            cotangent=cotangent,
            w_query=w_query,
            key_matrix=key_matrix,
            value_matrix=value_matrix,
            w_output=w_output,
            w_gate=w_gate,
            w_up=w_up,
            w_down=w_down,
            attn_gain=attn_gain[None],
            mlp_gain=mlp_gain[None],
            query_gain=query_gain[None],
            key_gain=key_gain[None],
            segment=segment_ids,
            inverse=jnp.concatenate([inverse, inverse])[None],
            sign=jnp.concatenate([-ones, ones])[None],
        ),
    )
    m = middle(
        dp,
        1,
        SimpleNamespace(
            mid_rows=f.mid_rows,
            cot_rows=f.cot_rows,
            grad_active=f.grad_active,
            scale_mid=f.scale_mid,
            w_gate_all=f.w_gate_all,
            w_up_all=f.w_up_all,
            hidden=f.hidden,
            cotangent=cotangent,
            mlp_gain=mlp_gain[None],
        ),
    )
    grad_low, grad_gate, grad_up = m.grad_low, m.grad_gate, m.grad_up
    if not two:
        grad_low, grad_gate, grad_up = lax.psum((grad_low, grad_gate, grad_up), "dp")
    b = backward(
        dp,
        2,
        SimpleNamespace(
            grad_attn=m.grad_attn,
            w_output=w_output,
            w_query=w_query,
            key_matrix=key_matrix,
            value_matrix=value_matrix,
            q=f.q,
            k=f.k,
            v=f.v,
            mixed=f.mixed,
            lse=f.lse,
            bias=f.bias,
            cosine=f.cosine,
            sine=f.sine,
            joint=f.joint,
            scale_in=f.scale_in,
            query_gain=query_gain[None],
            key_gain=key_gain[None],
            mix_rows=f.mix_rows,
            in_gained=f.in_gained,
            active=m.active,
            w_low=f.w_low,
            grad_gate=grad_gate,
            grad_up=grad_up,
            grad_low=grad_low,
            gain_mid=m.gain_mid,
            layer_input=layer_input,
        ),
    )
    if two:
        grad_output = b.d_output.astype(F32) + b.d_output_other.astype(F32)
        grad_query = b.d_q.astype(F32) + b.d_q_other.astype(F32)
        grad_kv = b.d_kv.astype(F32) + b.d_kv_other.astype(F32)
    else:
        sums = lax.psum((b.d_output, b.d_q, b.d_kv), "dp")
        grad_output, grad_query, grad_kv = [term.astype(F32) for term in sums]
    in_coef = jnp.sum(b.in_inners[:, 0], axis=0).reshape(length, 1) / MODEL_WIDTH
    input_grad = m.grad_hidden + b.grad_in * attn_gain - layer_input.astype(F32) * in_coef
    return (
        (f.hidden + b.block).astype(BF16),
        input_grad,
        grad_query,
        grad_kv[:, :key_width],
        grad_kv[:, key_width:],
        grad_output,
        b.grad_gate.reshape(feats, ff_local).astype(F32),
        b.grad_up.reshape(feats, ff_local).astype(F32),
        b.grad_low.reshape(ff_local, feats).astype(F32),
        b.gains[:, 0:4].reshape(MODEL_WIDTH),
        b.gains[:, 4:8].reshape(MODEL_WIDTH),
        jnp.sum(b.gains[:, 8], axis=0),
        jnp.sum(b.gains[:, 9], axis=0),
    )


def solution(mesh):
    tokens, weights, flipped = P(("dp", "col"), "row"), P("row", "col"), P("col", "row")
    features, copied = P("row"), P()
    return jax.shard_map(
        functools.partial(per_device, mesh.shape["dp"]),
        mesh=mesh,
        in_specs=(
            (tokens, tokens)
            + (weights,) * 3
            + (flipped, weights, weights, flipped)
            + (features, features, copied, copied, P(("dp", "row"), None))
        ),
        out_specs=(tokens, tokens)
        + (weights,) * 3
        + (flipped, weights, weights, flipped)
        + (copied,) * 4,
        check_vma=False,
    )
```
